256 devices in a mesh: gx: 32 (over y, z), gz: 8 (over x, core).
Axes of the slice: x: 4, y: 4, z: 8, core: 2. Of those that a mesh axis runs over, the one named last changes fastest.
Arguments:
- flow_state: float32 [4, 512, 256, 128], P(None, 'gx', 'gz'), may hold values from -6 to 6
- slot_ids: int32 [2048], P(('gx', 'gz')), may hold values from -1 to 1023, as said below
- corners: int32 [3, 2048], P(None, ('gx', 'gz')), may hold values from 0 to 511, as said below
- marker_cells: int32 [3, 2048, 512], P(None, ('gx', 'gz')), may hold values from 1 to 21
- marker_frac: float32 [3, 2048, 512], P(None, ('gx', 'gz')), may hold values from 0 to 1
- particle_velocity: float32 [3, 1024], replicated, may hold values from -4 to 4
- particle_spin: float32 [3, 1024], replicated, may hold values from -0.6 to 0.6
Outputs:
- velocity: float32 [3, 512, 256, 128], P(None, 'gx', 'gz')
- source: float32 [2, 128, 256, 512], P(None, 'gz', 'gx')
The draws below stay inside these ranges and needn't reach their ends.
Inputs may be any that keep to these rules, and one draw needn't show every extreme that they name: `slot_ids`: the ids of the particles that a tile's device owns stand in its 8 slots and -1 in each empty slot; every id 0 to 1023 stands in exactly one slot; some device has all of its slots full. corners[:, s] is the first cell of the box of slot s; the box's x and z ranges wrap around the grid; the cells (corners[0, s] + 12) mod 512 and (corners[2, s] + 12) mod 256 lie in the x and z ranges of the tile whose device holds slot s, and corners[1, s] <= 104.
All inputs are finite; a program needn't handle non-finite values.
Results may differ from the reference program's by a relative error of at most 0.0003.
Values sent between devices are 32-bit elements; how exact they have to be, the bound alone decides.
A program may use at most 64 MiB of HBM per device.

```python
import math
import jax
import jax.numpy as jnp
from jax import lax

CX = 16
CZ = 32
CY = 128
BOX = 24
NM = 512
MAXB = 8
HALF = 12
NX = 512
NZ = 256
SLOTS = 2048
NP = 1024


def draw_slot_ids(key, part):
    devices = SLOTS // MAXB
    half_load = MAXB // 2
    order_key, count_key, ident_key = jax.random.split(jax.random.fold_in(key, 11), 3)
    pairing = jax.random.permutation(order_key, devices)
    surplus = jax.random.randint(count_key, (devices // 2,), 0, half_load + 1, dtype=jnp.int32)
    surplus = surplus.at[0].set(half_load)
    counts = jnp.zeros((devices,), jnp.int32)
    counts = counts.at[pairing[0::2]].set(half_load + surplus)
    counts = counts.at[pairing[1::2]].set(half_load - surplus)
    occupied = jnp.arange(MAXB, dtype=jnp.int32)[None, :] < counts[:, None]
    flat_live = occupied.reshape(-1).astype(jnp.int32)
    rank_index = jnp.clip(jnp.cumsum(flat_live) - 1, 0, NP - 1)
    particle_ids = jax.random.permutation(ident_key, NP).astype(jnp.int32)
    return jnp.where(flat_live > 0, particle_ids[rank_index], -1).astype(jnp.int32)


def draw_corners(key, part):
    tiles_z = NZ // CZ
    owner_index = jnp.arange(SLOTS, dtype=jnp.int32) // MAXB
    tile_x = owner_index // tiles_z
    tile_z = owner_index % tiles_z
    draw_keys = jax.random.split(jax.random.fold_in(key, 23), 3)
    centre_x = tile_x * CX + jax.random.randint(draw_keys[0], (SLOTS,), 0, CX, dtype=jnp.int32)
    centre_z = tile_z * CZ + jax.random.randint(draw_keys[2], (SLOTS,), 0, CZ, dtype=jnp.int32)
    first_y = jax.random.randint(draw_keys[1], (SLOTS,), 0, CY - BOX + 1, dtype=jnp.int32)
    first_x = (centre_x - BOX // 2) % NX
    first_z = (centre_z - BOX // 2) % NZ
    return jnp.stack([first_x, first_y, first_z]).astype(jnp.int32)


def with_ends(entries, stream_key, least, top_value):
    index_at = [jax.random.randint(jax.random.fold_in(stream_key, axis), (), 0, length) for axis, length in enumerate(entries.shape)]
    widest = entries.shape.index(max(entries.shape))
    neighbour = index_at[:widest] + [(index_at[widest] + 1) % entries.shape[widest]] + index_at[widest + 1:]
    return entries.at[tuple(index_at)].set(least).at[tuple(neighbour)].set(top_value)


def steps_of(rng, extent, cuts, least, high):
    gain, own = 1.0, jax.random.fold_in(rng, 6)
    for dim, blocks in cuts:
        heights = jnp.exp(jax.random.uniform(jax.random.fold_in(own, dim), (blocks,), jnp.float32, least / len(cuts), high / len(cuts)))
        gain = gain * jnp.repeat(heights, extent[dim] // blocks).reshape([-1 if axis == dim else 1 for axis in range(len(extent))])
    return gain


def gaussian(key, dims, scale, most, pieces=(), kind=jnp.bfloat16):
    result = scale * jax.random.normal(key, dims, jnp.float32)
    if pieces:
        result = result * steps_of(key, dims, pieces, -0.22, 0.18)
    return jnp.clip(result, -most, most).astype(kind)


def setup_inputs(seed: int = 0) -> dict:
    splits = jax.random.split(jax.random.key(seed), 8)
    flow_state = gaussian(splits[0], (4, NX, NZ, CY), 1.0, 6.0, ((1, 32), (2, 8)), jnp.float32)
    slot_ids = draw_slot_ids(jax.random.fold_in(splits[7], 71), 0)
    corners = draw_corners(jax.random.fold_in(splits[7], 71), 0)
    marker_cells = with_ends(jax.random.randint(splits[3], (3, SLOTS, NM), 1, BOX - 2), jax.random.fold_in(splits[3], 1), 1, (BOX - 2) - 1).astype(jnp.int32)
    marker_frac = jnp.clip(1.0 * jax.random.uniform(splits[4], (3, SLOTS, NM), jnp.float32) ** steps_of(splits[4], (3, SLOTS, NM), ((1, 256),), -0.2, 0.2), 0.0, 1.0)
    particle_velocity = gaussian(splits[5], (3, NP), 1.0, 4.0, (), jnp.float32)
    particle_spin = gaussian(splits[6], (3, NP), 0.15, 0.6, (), jnp.float32)
    return dict(flow_state=flow_state, slot_ids=slot_ids, corners=corners, marker_cells=marker_cells, marker_frac=marker_frac, particle_velocity=particle_velocity, particle_spin=particle_spin)


time_step = 0.1
viscosity = 0.2
drive_force = 1.0

def predict(padded):
    velocity = padded[:3]
    pressure = padded[3]
    wall_zeros = jnp.zeros(velocity.shape[:3] + (1,), jnp.float32)
    fields = jnp.concatenate([wall_zeros, velocity, wall_zeros], axis=3)
    pressure_y = jnp.concatenate([pressure[:, :, :1], pressure, pressure[:, :, -1:]], axis=2)
    centre = fields[:, 1:-1, 1:-1, 1:-1]
    x_plus = fields[:, 2:, 1:-1, 1:-1]
    x_minus = fields[:, :-2, 1:-1, 1:-1]
    z_plus = fields[:, 1:-1, 2:, 1:-1]
    z_minus = fields[:, 1:-1, :-2, 1:-1]
    y_plus = fields[:, 1:-1, 1:-1, 2:]
    y_minus = fields[:, 1:-1, 1:-1, :-2]
    laplace = x_plus + x_minus + z_plus + z_minus + y_plus + y_minus - 6.0 * centre
    advect = (centre[0:1] * (x_plus - x_minus) + centre[1:2] * (y_plus - y_minus) + centre[2:3] * (z_plus - z_minus)) * 0.5
    gradient_x = (pressure_y[2:, 1:-1, 1:-1] - pressure_y[:-2, 1:-1, 1:-1]) * 0.5
    gradient_y = (pressure_y[1:-1, 1:-1, 2:] - pressure_y[1:-1, 1:-1, :-2]) * 0.5
    gradient_z = (pressure_y[1:-1, 2:, 1:-1] - pressure_y[1:-1, :-2, 1:-1]) * 0.5
    gradient = jnp.stack([gradient_x - drive_force, gradient_y, gradient_z])
    return centre + time_step * (viscosity * laplace - advect - gradient)

def diverge(padded):
    along_x = (padded[0, 2:, 1:-1] - padded[0, :-2, 1:-1]) * 0.5
    along_z = (padded[2, 1:-1, 2:] - padded[2, 1:-1, :-2]) * 0.5
    normal = padded[1, 1:-1, 1:-1]
    wall_zeros = jnp.zeros(normal.shape[:2] + (1,), jnp.float32)
    normal = jnp.concatenate([wall_zeros, normal, wall_zeros], axis=2)
    along_y = (normal[:, :, 2:] - normal[:, :, :-2]) * 0.5
    return along_x + along_y + along_z

def rigid_target(velocity, angular, position):
    lever_arm = position - HALF
    rotation = jnp.stack([angular[1] * lever_arm[2] - angular[2] * lever_arm[1], angular[2] * lever_arm[0] - angular[0] * lever_arm[2], angular[0] * lever_arm[1] - angular[1] * lever_arm[0]])
    return velocity[:, None] + rotation

def reference(flow_state, slot_ids, corners, marker_cells, marker_frac, particle_velocity, particle_spin):
    wrapped = jnp.pad(flow_state, ((0, 0), (1, 1), (1, 1), (0, 0)), mode='wrap')
    predicted = predict(wrapped)
    tap_offsets = jnp.arange(4, dtype=jnp.int32) - 1
    tap_values = tap_offsets.astype(jnp.float32)

    def one_slot(spread, inputs):
        particle, corner, cell_offsets, fraction = inputs
        occupied = (particle >= 0).astype(jnp.float32)
        column = jnp.maximum(particle, 0).astype(jnp.int32)
        velocity = lax.dynamic_index_in_dim(particle_velocity, column, 1, keepdims=False)
        angular = lax.dynamic_index_in_dim(particle_spin, column, 1, keepdims=False)
        cell_index = corner[:, None, None] + cell_offsets[:, :, None] + tap_offsets[None, None, :]
        along_x = cell_index[0] % NX
        along_y = cell_index[1]
        along_z = cell_index[2] % NZ
        weight = 0.25 * (1.0 + jnp.cos(0.5 * math.pi * (tap_values[None, None, :] - fraction[:, :, None])))
        triple = weight[0][:, :, None, None] * weight[2][:, None, :, None] * weight[1][:, None, None, :]
        pick_x = along_x[:, :, None, None]
        pick_z = along_z[:, None, :, None]
        pick_y = along_y[:, None, None, :]
        values = predicted[:, pick_x, pick_z, pick_y]
        sampled = lax.optimization_barrier(jnp.sum(values * triple[None], axis=(2, 3, 4)))
        target = rigid_target(velocity, angular, cell_offsets.astype(jnp.float32) + fraction)
        pushing = occupied * (target - sampled)
        spread = spread.at[:, pick_x, pick_z, pick_y].add(pushing[:, :, None, None, None] * triple[None])
        return (spread, None)
    scanned = (slot_ids, jnp.transpose(corners), jnp.transpose(marker_cells, (1, 0, 2)), jnp.transpose(marker_frac, (1, 0, 2)))
    forcing = lax.scan(one_slot, jnp.zeros_like(predicted), scanned)[0]
    velocity = predicted + forcing
    divergence = diverge(jnp.pad(velocity, ((0, 0), (1, 1), (1, 1), (0, 0)), mode='wrap'))
    spectrum = jnp.fft.fft2(divergence, axes=(0, 1))
    spectrum = jnp.transpose(spectrum, (2, 1, 0)) / math.sqrt(NX * NZ)
    source = jnp.stack([jnp.real(spectrum), jnp.imag(spectrum)]).astype(jnp.float32)
    return (velocity, source)
```

```python
import functools
import math

import jax
import jax.numpy as jnp
from jax import lax
from jax.experimental import pallas as pl
from jax.experimental.pallas import tpu as pltpu
from jax.sharding import Mesh
from jax.sharding import PartitionSpec as P

BOX = 24
HALF = 12
BAND = 32
STEP = 8
GZ = ("gz_0", "gz_1")
GX_GZ = ("gx", "gz_0", "gz_1")


time_step = 0.1
viscosity = 0.2
drive_force = 1.0
highest = lax.Precision.HIGHEST


def padded_2(array, sides, width):
    for axis, dim in sides:
        devices, length = (lax.axis_size(axis), array.shape[dim])
        up = [(i, (i + 1) % devices) for i in range(devices)]
        down = [(j, i) for i, j in up]
        last = lax.slice_in_dim(array, length - width, length, axis=dim)
        first = lax.slice_in_dim(array, 0, width, axis=dim)
        before = lax.ppermute(last, axis, up)
        after = lax.ppermute(first, axis, down)
        array = jnp.concatenate([before, array, after], axis=dim)
    return array


def with_halo(array, sides, width):
    edges = {}
    for axis, dim in sides:
        devices, length = (lax.axis_size(axis), array.shape[dim])
        up = [(i, (i + 1) % devices) for i in range(devices)]
        last = lax.slice_in_dim(array, length - width, length, axis=dim)
        first = lax.slice_in_dim(array, 0, width, axis=dim)
        edges[dim] = (
            lax.ppermute(last, axis, up),
            lax.ppermute(first, axis, [(b, a) for a, b in up]),
        )
    done = []
    for _, dim in sides:
        low, high = edges[dim]
        around = [(width, width) if d in done else (0, 0) for d in range(array.ndim)]
        array = jnp.concatenate([jnp.pad(low, around), array, jnp.pad(high, around)], axis=dim)
        done.append(dim)
    return array


def cut_along(array, dim, devices):
    before, after = (array.shape[:dim], array.shape[dim + 1 :])
    return jnp.moveaxis(array.reshape(*before, devices, -1, *after), dim, 0)


def laid_out(blocks, dim):
    lengths = list(blocks.shape[1:])
    lengths[dim] *= blocks.shape[0]
    return jnp.moveaxis(blocks, 0, dim).reshape(lengths)


def moved_by_axis(blocks, axes, turns):
    inside = blocks.shape[1:]
    filled = blocks.reshape(*(lax.axis_size(a) for a in axes), *inside)
    for k in turns:
        filled = lax.all_to_all(filled, axes[k], k, k, tiled=True)
    return filled.reshape(-1, *inside)


def core_and_chips(array, groups, turns, split_dim, concat_dim):
    devices = lax.axis_size(groups[0]) * lax.axis_size(groups[1])
    blocks = cut_along(array, split_dim, devices)
    return laid_out(moved_by_axis(blocks, groups, turns), concat_dim)


def predict(padded):
    velocity = padded[:3]
    pressure = padded[3]
    wall_zeros = jnp.zeros(velocity.shape[:3] + (1,), jnp.float32)
    fields = jnp.concatenate([wall_zeros, velocity, wall_zeros], axis=3)
    pressure_y = jnp.concatenate([pressure[:, :, :1], pressure, pressure[:, :, -1:]], axis=2)
    centre = fields[:, 1:-1, 1:-1, 1:-1]
    x_plus = fields[:, 2:, 1:-1, 1:-1]
    x_minus = fields[:, :-2, 1:-1, 1:-1]
    z_plus = fields[:, 1:-1, 2:, 1:-1]
    z_minus = fields[:, 1:-1, :-2, 1:-1]
    y_plus = fields[:, 1:-1, 1:-1, 2:]
    y_minus = fields[:, 1:-1, 1:-1, :-2]
    laplace = x_plus + x_minus + z_plus + z_minus + y_plus + y_minus - 6.0 * centre
    advect = (
        centre[0:1] * (x_plus - x_minus)
        + centre[1:2] * (y_plus - y_minus)
        + centre[2:3] * (z_plus - z_minus)
    ) * 0.5
    gradient_x = (pressure_y[2:, 1:-1, 1:-1] - pressure_y[:-2, 1:-1, 1:-1]) * 0.5
    gradient_y = (pressure_y[1:-1, 1:-1, 2:] - pressure_y[1:-1, 1:-1, :-2]) * 0.5
    gradient_z = (pressure_y[1:-1, 2:, 1:-1] - pressure_y[1:-1, :-2, 1:-1]) * 0.5
    gradient = jnp.stack([gradient_x - drive_force, gradient_y, gradient_z])
    return centre + time_step * (viscosity * laplace - advect - gradient)


def diverge(padded):
    along_x = (padded[0, 2:, 1:-1] - padded[0, :-2, 1:-1]) * 0.5
    along_z = (padded[2, 1:-1, 2:] - padded[2, 1:-1, :-2]) * 0.5
    normal = padded[1, 1:-1, 1:-1]
    wall_zeros = jnp.zeros(normal.shape[:2] + (1,), jnp.float32)
    normal = jnp.concatenate([wall_zeros, normal, wall_zeros], axis=2)
    along_y = (normal[:, :, 2:] - normal[:, :, :-2]) * 0.5
    return along_x + along_y + along_z


def dft_tables(length):
    counter = jnp.arange(length, dtype=jnp.int32)
    product_index = counter[:, None] * counter[None, :] % length
    angles = product_index.astype(jnp.float32) * (2.0 * math.pi / length)
    return (jnp.cos(angles), jnp.sin(angles))


def parts(value):
    high = value.astype(jnp.bfloat16)
    return high, (value - high.astype(jnp.float32)).astype(jnp.bfloat16)


def tap_weights(length, first, taps):
    offset = lax.broadcasted_iota(jnp.int32, (length, first.shape[-1]), 0) - first
    weight = jnp.where(offset == 3, taps[3], 0.0)
    for t in (2, 1, 0):
        weight = jnp.where(offset == t, taps[t], weight)
    return weight


def dot(a, b, across):
    return lax.dot_general(
        a, b, (((1,), (across,)), ((), ())), preferred_element_type=jnp.float32
    )


def marker_kernel(
    ids, starts, moving, turning, cells, fracs, field, force, tap, cross, spread, way_y, load
):
    force[...] = jnp.zeros_like(force)
    half_pi = 0.5 * math.pi
    angle = fracs[...] * half_pi
    cosine, sine = jnp.cos(angle), jnp.sin(angle)
    tap[0] = 0.25 * (1.0 - sine)
    tap[1] = 0.25 * (1.0 + cosine)
    tap[2] = 0.25 * (1.0 + sine)
    tap[3] = 0.25 * (1.0 - cosine)
    markers = fracs.shape[2]
    wall = field.shape[3]

    def one_slot(s, carry):
        @pl.when(ids[s] >= 0)
        def _():
            n = ids[s]
            x0, y0, z0 = starts[0, s], starts[1, s], starts[2, s]
            zb = pl.multiple_of((z0 // 8) * 8, 8)
            cell = cells[s]
            frac = fracs[s]
            taps = [tap[t, s] for t in range(4)]

            def along(d):
                return [w[d : d + 1] for w in taps]

            weight_x = tap_weights(BOX, cell[0:1] - 1, along(0))
            weight_y = tap_weights(wall, cell[1:2] - 1 + y0, along(1))
            weight_z = tap_weights(BAND, cell[2:3] - 1 + (z0 - zb), along(2))
            for i in range(BOX):
                cross[i // STEP, i % STEP] = weight_x[i : i + 1] * weight_z
            spread[...] = weight_y
            y_high, y_low = parts(weight_y)
            way_y[0] = y_high
            way_y[1] = y_low

            def sample(t, total):
                window = field[:, pl.ds(x0 + t * STEP, STEP), pl.ds(zb, BAND), :]
                high, low = parts(window.reshape(3 * STEP * BAND, wall))
                value = dot(high, way_y[0], 0) + dot(low, way_y[0], 0) + dot(high, way_y[1], 0)
                value = value.reshape(3, STEP * BAND // 8, 8, markers)
                factor = cross[t].reshape(1, STEP * BAND // 8, 8, markers)
                return total + jnp.sum(value * factor, axis=1)

            total = lax.fori_loop(
                0, BOX // STEP, sample, jnp.zeros((3, 8, markers), jnp.float32)
            )
            sampled = jnp.sum(total, axis=1)
            lever = cell.astype(jnp.float32) + frac - float(HALF)
            spin = [turning[c, n] for c in range(3)]
            for c in range(3):
                a, b = (c + 1) % 3, (c + 2) % 3
                target = moving[c, n] + (spin[a] * lever[b : b + 1] - spin[b] * lever[a : a + 1])
                push = target - sampled[c : c + 1]
                high, low = parts(spread[...] * push)
                load[0, pl.ds(c * wall, wall), :] = high
                load[1, pl.ds(c * wall, wall), :] = low

            def scatter(t, carry):
                high, low = parts(cross[t].reshape(STEP * BAND, markers))
                value = dot(high, load[0], 1) + dot(low, load[0], 1) + dot(high, load[1], 1)
                for c in range(3):
                    force[c, pl.ds(x0 + t * STEP, STEP), pl.ds(zb, BAND), :] += value[
                        :, c * wall : (c + 1) * wall
                    ].reshape(STEP, BAND, wall)
                return carry

            lax.fori_loop(0, BOX // STEP, scatter, 0)

        return carry

    lax.fori_loop(0, ids.shape[0], one_slot, 0)


def spread_forces(extended, slot_ids, starts, cells, fracs, moving, turning):
    slots, _, markers = cells.shape
    wall = extended.shape[3]
    scalar = pl.BlockSpec(memory_space=pltpu.SMEM)
    vector = pl.BlockSpec(memory_space=pltpu.VMEM)
    return pl.pallas_call(
        marker_kernel,
        out_shape=jax.ShapeDtypeStruct(extended.shape, jnp.float32),
        in_specs=[scalar] * 4 + [vector] * 3,
        out_specs=vector,
        scratch_shapes=[
            pltpu.VMEM((4, slots, 3, markers), jnp.float32),
            pltpu.VMEM((BOX // STEP, STEP, BAND, markers), jnp.float32),
            pltpu.VMEM((wall, markers), jnp.float32),
            pltpu.VMEM((2, wall, markers), jnp.bfloat16),
            pltpu.VMEM((2, 3 * wall, markers), jnp.bfloat16),
        ],
        name="markers",
    )(slot_ids, starts, moving, turning, cells, fracs, extended)


def fold_along(packed, axis, dim):
    devices, length = lax.axis_size(axis), packed.shape[dim]
    up = [(i, (i + 1) % devices) for i in range(devices)]
    low = lax.slice_in_dim(packed, 0, HALF, axis=dim)
    high = lax.slice_in_dim(packed, length - HALF, length, axis=dim)
    from_below = lax.ppermute(high, axis, up)
    from_above = lax.ppermute(low, axis, [(b, a) for a, b in up])
    middle = lax.slice_in_dim(packed, HALF, length - HALF, axis=dim)
    rest = length - 3 * HALF
    after = [(0, rest) if d == dim else (0, 0) for d in range(packed.ndim)]
    before = [(rest, 0) if d == dim else (0, 0) for d in range(packed.ndim)]
    return middle + jnp.pad(from_below, after) + jnp.pad(from_above, before)


def on_device(
    flow_state, slot_ids, corners, marker_cells, marker_frac, particle_velocity, particle_spin
):
    tile_x = flow_state.shape[1]
    tile_z = flow_state.shape[2]
    ghosted = with_halo(flow_state, (("gx", 1), (GZ, 2)), 1)
    extended = padded_2(predict(ghosted), (("gx", 1), (GZ, 2)), HALF)
    starts = jnp.stack(
        [
            (corners[0] - lax.axis_index("gx") * tile_x + HALF) % (tile_x * lax.axis_size("gx")),
            corners[1],
            (corners[2] - lax.axis_index(GZ) * tile_z + HALF) % (tile_z * lax.axis_size(GZ)),
        ]
    )
    spread = spread_forces(
        extended,
        slot_ids,
        starts,
        jnp.transpose(marker_cells, (1, 0, 2)),
        jnp.transpose(marker_frac, (1, 0, 2)),
        particle_velocity,
        particle_spin,
    )
    predicted = extended[:, HALF : HALF + tile_x, HALF : HALF + tile_z]
    forcing = fold_along(fold_along(spread, GZ, 2), "gx", 1)
    velocity = predicted + forcing
    normal_faces = with_halo(jnp.stack([velocity[0], velocity[2]]), (("gx", 1), (GZ, 2)), 1)
    padded = jnp.stack(
        [normal_faces[0], jnp.pad(velocity[1], ((1, 1), (1, 1), (0, 0))), normal_faces[1]]
    )
    divergence = diverge(padded)
    planes = core_and_chips(divergence, ("gz_0", "gz_1"), (1, 0), 2, 1)
    length_z = planes.shape[1]
    cosine_z, sine_z = dft_tables(length_z)
    real_z = jnp.einsum("xzy,zk->ykx", planes, cosine_z, precision=highest)
    imag_z = -jnp.einsum("xzy,zk->ykx", planes, sine_z, precision=highest)
    real_z, imag_z = (
        lax.all_to_all(real_z, "gx", split_axis=1, concat_axis=2, tiled=True),
        lax.all_to_all(imag_z, "gx", split_axis=1, concat_axis=2, tiled=True),
    )
    length_x = real_z.shape[2]
    cosine_x, sine_x = dft_tables(length_x)
    normalise = 1.0 / math.sqrt(length_x * length_z)
    real_part = (
        jnp.einsum("ykx,xq->ykq", real_z, cosine_x, precision=highest)
        + jnp.einsum("ykx,xq->ykq", imag_z, sine_x, precision=highest)
    ) * normalise
    imag_part = (
        jnp.einsum("ykx,xq->ykq", imag_z, cosine_x, precision=highest)
        - jnp.einsum("ykx,xq->ykq", real_z, sine_x, precision=highest)
    ) * normalise
    return (velocity, jnp.stack([real_part, imag_part]))


def solution(mesh):
    finer = Mesh(mesh.devices.reshape(mesh.shape["gx"], 4, 2), ("gx", "gz_0", "gz_1"))
    placed = (
        P(None, "gx", GZ, None),
        P(GX_GZ),
        P(None, GX_GZ),
        P(None, GX_GZ, None),
        P(None, GX_GZ, None),
        P(),
        P(),
    )
    return jax.shard_map(
        on_device,
        mesh=finer,
        in_specs=placed,
        out_specs=(P(None, "gx", GZ, None), P(None, GZ, "gx", None)),
        check_vma=False,
    )
```

```python
import functools
import math

import jax
import jax.numpy as jnp
import numpy as np
from jax import lax
from jax.experimental import pallas as pl
from jax.experimental.pallas import tpu as pltpu
from jax.sharding import PartitionSpec as P

BOX = 24
HALF = 12
BAND = 32
STEP = 8
SIDE = 16
MESH = pl.DeviceIdType.MESH


time_step = 0.1
viscosity = 0.2
drive_force = 1.0


def padded_2(array, sides):
    for axis, dim, width in sides:
        devices, length = (lax.axis_size(axis), array.shape[dim])
        up = [(i, (i + 1) % devices) for i in range(devices)]
        down = [(j, i) for i, j in up]
        last = lax.slice_in_dim(array, length - width, length, axis=dim)
        first = lax.slice_in_dim(array, 0, width, axis=dim)
        before = lax.ppermute(last, axis, up)
        after = lax.ppermute(first, axis, down)
        array = jnp.concatenate([before, array, after], axis=dim)
    return array


def with_halo(array, sides, width):
    edges = {}
    for axis, dim in sides:
        devices, length = (lax.axis_size(axis), array.shape[dim])
        up = [(i, (i + 1) % devices) for i in range(devices)]
        last = lax.slice_in_dim(array, length - width, length, axis=dim)
        first = lax.slice_in_dim(array, 0, width, axis=dim)
        edges[dim] = (
            lax.ppermute(last, axis, up),
            lax.ppermute(first, axis, [(b, a) for a, b in up]),
        )
    done = []
    for _, dim in sides:
        low, high = edges[dim]
        around = [(width, width) if d in done else (0, 0) for d in range(array.ndim)]
        array = jnp.concatenate([jnp.pad(low, around), array, jnp.pad(high, around)], axis=dim)
        done.append(dim)
    return array


def predict(padded):
    velocity = padded[:3]
    pressure = padded[3]
    wall_zeros = jnp.zeros(velocity.shape[:3] + (1,), jnp.float32)
    fields = jnp.concatenate([wall_zeros, velocity, wall_zeros], axis=3)
    pressure_y = jnp.concatenate([pressure[:, :, :1], pressure, pressure[:, :, -1:]], axis=2)
    centre = fields[:, 1:-1, 1:-1, 1:-1]
    x_plus = fields[:, 2:, 1:-1, 1:-1]
    x_minus = fields[:, :-2, 1:-1, 1:-1]
    z_plus = fields[:, 1:-1, 2:, 1:-1]
    z_minus = fields[:, 1:-1, :-2, 1:-1]
    y_plus = fields[:, 1:-1, 1:-1, 2:]
    y_minus = fields[:, 1:-1, 1:-1, :-2]
    laplace = x_plus + x_minus + z_plus + z_minus + y_plus + y_minus - 6.0 * centre
    advect = (
        centre[0:1] * (x_plus - x_minus)
        + centre[1:2] * (y_plus - y_minus)
        + centre[2:3] * (z_plus - z_minus)
    ) * 0.5
    gradient_x = (pressure_y[2:, 1:-1, 1:-1] - pressure_y[:-2, 1:-1, 1:-1]) * 0.5
    gradient_y = (pressure_y[1:-1, 1:-1, 2:] - pressure_y[1:-1, 1:-1, :-2]) * 0.5
    gradient_z = (pressure_y[1:-1, 2:, 1:-1] - pressure_y[1:-1, :-2, 1:-1]) * 0.5
    gradient = jnp.stack([gradient_x - drive_force, gradient_y, gradient_z])
    return centre + time_step * (viscosity * laplace - advect - gradient)


def parts(value):
    high = value.astype(jnp.bfloat16)
    return high, (value - high.astype(jnp.float32)).astype(jnp.bfloat16)


def tap_weights(length, first, taps):
    offset = lax.broadcasted_iota(jnp.int32, (length, first.shape[-1]), 0) - first
    weight = jnp.where(offset == 3, taps[3], 0.0)
    for t in (2, 1, 0):
        weight = jnp.where(offset == t, taps[t], weight)
    return weight


def dot(a, b, across):
    return lax.dot_general(
        a, b, (((1,), (across,)), ((), ())), preferred_element_type=jnp.float32
    )


def marker_kernel(
    ids, starts, moving, turning, cells, fracs, field, force, tap, cross, spread, way_y, load
):
    force[...] = jnp.zeros_like(force)
    half_pi = 0.5 * math.pi
    angle = fracs[...] * half_pi
    cosine, sine = jnp.cos(angle), jnp.sin(angle)
    tap[0] = 0.25 * (1.0 - sine)
    tap[1] = 0.25 * (1.0 + cosine)
    tap[2] = 0.25 * (1.0 + sine)
    tap[3] = 0.25 * (1.0 - cosine)
    markers = fracs.shape[2]
    wall = field.shape[3]

    def one_slot(s, carry):
        @pl.when(ids[s] >= 0)
        def _():
            n = ids[s]
            x0, y0, z0 = starts[0, s], starts[1, s], starts[2, s]
            zb = pl.multiple_of((z0 // 8) * 8, 8)
            cell = cells[s]
            frac = fracs[s]
            taps = [tap[t, s] for t in range(4)]

            def along(d):
                return [w[d : d + 1] for w in taps]

            weight_x = tap_weights(BOX, cell[0:1] - 1, along(0))
            weight_y = tap_weights(wall, cell[1:2] - 1 + y0, along(1))
            weight_z = tap_weights(BAND, cell[2:3] - 1 + (z0 - zb), along(2))
            for i in range(BOX):
                cross[i // STEP, i % STEP] = weight_x[i : i + 1] * weight_z
            spread[...] = weight_y
            y_high, y_low = parts(weight_y)
            way_y[0] = y_high
            way_y[1] = y_low

            def sample(t, total):
                window = field[:, pl.ds(x0 + t * STEP, STEP), pl.ds(zb, BAND), :]
                high, low = parts(window.reshape(3 * STEP * BAND, wall))
                value = dot(high, way_y[0], 0) + dot(low, way_y[0], 0) + dot(high, way_y[1], 0)
                value = value.reshape(3, STEP * BAND // 8, 8, markers)
                factor = cross[t].reshape(1, STEP * BAND // 8, 8, markers)
                return total + jnp.sum(value * factor, axis=1)

            total = lax.fori_loop(
                0, BOX // STEP, sample, jnp.zeros((3, 8, markers), jnp.float32)
            )
            sampled = jnp.sum(total, axis=1)
            lever = cell.astype(jnp.float32) + frac - float(HALF)
            spin = [turning[c, n] for c in range(3)]
            for c in range(3):
                a, b = (c + 1) % 3, (c + 2) % 3
                target = moving[c, n] + (spin[a] * lever[b : b + 1] - spin[b] * lever[a : a + 1])
                push = target - sampled[c : c + 1]
                high, low = parts(spread[...] * push)
                load[0, pl.ds(c * wall, wall), :] = high
                load[1, pl.ds(c * wall, wall), :] = low

            def scatter(t, carry):
                high, low = parts(cross[t].reshape(STEP * BAND, markers))
                value = dot(high, load[0], 1) + dot(low, load[0], 1) + dot(high, load[1], 1)
                for c in range(3):
                    force[c, pl.ds(x0 + t * STEP, STEP), pl.ds(zb, BAND), :] += value[
                        :, c * wall : (c + 1) * wall
                    ].reshape(STEP, BAND, wall)
                return carry

            lax.fori_loop(0, BOX // STEP, scatter, 0)

        return carry

    lax.fori_loop(0, ids.shape[0], one_slot, 0)


def spread_forces(extended, slot_ids, starts, cells, fracs, moving, turning):
    slots, _, markers = cells.shape
    wall = extended.shape[3]
    scalar = pl.BlockSpec(memory_space=pltpu.SMEM)
    vector = pl.BlockSpec(memory_space=pltpu.VMEM)
    return pl.pallas_call(
        marker_kernel,
        out_shape=jax.ShapeDtypeStruct(extended.shape, jnp.float32),
        in_specs=[scalar] * 4 + [vector] * 3,
        out_specs=vector,
        scratch_shapes=[
            pltpu.VMEM((4, slots, 3, markers), jnp.float32),
            pltpu.VMEM((BOX // STEP, STEP, BAND, markers), jnp.float32),
            pltpu.VMEM((wall, markers), jnp.float32),
            pltpu.VMEM((2, wall, markers), jnp.bfloat16),
            pltpu.VMEM((2, 3 * wall, markers), jnp.bfloat16),
        ],
        name="markers",
    )(slot_ids, starts, moving, turning, cells, fracs, extended)


def dot3(high, low, other_high, other_low):
    return dot(high, other_high, 0) + dot(low, other_high, 0) + dot(high, other_low, 0)


def exchanged(rows, lane_bits):
    lane = lax.broadcasted_iota(jnp.int32, rows[0].shape, rows[0].ndim - 1)
    axis = rows[0].ndim - 1
    for bit, shift in enumerate(lane_bits):
        low = (lane & shift) == 0
        step = 1 << bit
        out = list(rows)
        for m in range(len(rows)):
            if m & step == 0:
                a, b = rows[m], rows[m + step]
                out[m] = jnp.where(low, a, pltpu.roll(b, shift, axis))
                out[m + step] = jnp.where(low, pltpu.roll(a, 128 - shift, axis), b)
        rows = out
    return rows


def remote(source, target, sems, slot, to):
    return pltpu.make_async_remote_copy(
        src_ref=source,
        dst_ref=target,
        send_sem=sems[0].at[slot],
        recv_sem=sems[1].at[slot],
        device_id=to,
        device_id_type=MESH,
    )


def spectrum_kernel(
    nx, nz, scale, force, field, table_z, table_x, velocity, source,
    z_got, x_out, x_got, edge_u, edge_w, edge_w_out, cut, planes, modes, rows,
    z_send, z_recv, x_send, x_recv, e_send, e_recv, c_send, c_recv, m_send, m_recv,
):
    gx, gz = lax.axis_index("gx"), lax.axis_index("gz")
    below = (gx, lax.rem(gz + nz - 1, nz))
    above = (gx, lax.rem(gz + 1, nz))
    left = (lax.rem(gx + nx - 1, nx), gz)
    right = (lax.rem(gx + 1, nx), gz)
    barrier = pltpu.get_barrier_semaphore()

    def greet_z(d, carry):
        pl.semaphore_signal(
            barrier, inc=1, device_id=(gx, lax.rem(gz + d, nz)), device_id_type=MESH
        )
        return carry

    def greet_x(d, carry):
        pl.semaphore_signal(
            barrier, inc=1, device_id=(lax.rem(gx + d, nx), gz), device_id_type=MESH
        )
        return carry

    lax.fori_loop(1, nz, greet_z, 0)
    lax.fori_loop(1, nx, greet_x, 0)
    pl.semaphore_wait(barrier, nx + nz - 2)

    wide, tall = velocity.shape[1], velocity.shape[2]
    order = (0, 2, 1)
    z_copies, x_copies = {}, {}
    for c in order:
        down = remote(
            force.at[c, :, pl.ds(0, SIDE), :], z_got.at[1, c], (z_send, z_recv), (1, c), below
        )
        up = remote(
            force.at[c, :, pl.ds(SIDE + tall, SIDE), :],
            z_got.at[0, c],
            (z_send, z_recv),
            (0, c),
            above,
        )
        down.start()
        up.start()
        z_copies[c] = (down, up)
    for c in order:
        for copy in z_copies[c]:
            copy.wait_recv()
        for part in range(2):
            inner = pl.ds(part * SIDE, SIDE)
            outer = pl.ds(SIDE + part * SIDE, SIDE)
            x_out[0, c, :, inner, :] = (
                force[c, pl.ds(0, HALF), outer, :] + z_got[part, c, pl.ds(0, HALF)]
            )
            x_out[1, c, :, inner, :] = (
                force[c, pl.ds(HALF + wide, HALF), outer, :]
                + z_got[part, c, pl.ds(HALF + wide, HALF)]
            )
        back = remote(x_out.at[0, c], x_got.at[1, c], (x_send, x_recv), (1, c), left)
        ahead = remote(x_out.at[1, c], x_got.at[0, c], (x_send, x_recv), (0, c), right)
        back.start()
        ahead.start()
        x_copies[c] = (back, ahead)
        for part in range(2):
            inner = pl.ds(part * SIDE, SIDE)
            outer = pl.ds(SIDE + part * SIDE, SIDE)
            velocity[c, :, inner, :] = (
                field[c, pl.ds(HALF, wide), outer, :]
                + force[c, pl.ds(HALF, wide), outer, :]
                + z_got[part, c, pl.ds(HALF, wide)]
            )
    edges = []
    for c in order:
        for copy in x_copies[c]:
            copy.wait_recv()
        velocity[c, pl.ds(0, HALF)] += x_got[0, c]
        velocity[c, pl.ds(wide - HALF, HALF)] += x_got[1, c]
        if c == 0:
            edges += [
                remote(velocity.at[0, 0], edge_u.at[1], (e_send, e_recv), 0, left),
                remote(velocity.at[0, wide - 1], edge_u.at[0], (e_send, e_recv), 1, right),
            ]
        if c == 2:
            edge_w_out[0] = velocity[2, :, 0, :]
            edge_w_out[1] = velocity[2, :, tall - 1, :]
            edges += [
                remote(edge_w_out.at[0], edge_w.at[1], (e_send, e_recv), 2, below),
                remote(edge_w_out.at[1], edge_w.at[0], (e_send, e_recv), 3, above),
            ]
        if c != 1:
            edges[-2].start()
            edges[-1].start()
    wall = velocity.shape[3]
    lane = lax.broadcasted_iota(jnp.int32, (1, 1, wall), 2)
    normal = velocity[1]
    upper = jnp.where(lane == wall - 1, 0.0, pltpu.roll(normal, wall - 1, 2))
    lower = jnp.where(lane == 0, 0.0, pltpu.roll(normal, 1, 2))
    divergence = upper - lower
    for copy in edges:
        copy.wait_recv()
    stream = velocity[0]
    divergence += jnp.concatenate([stream[1:], edge_u[1:2]], axis=0) - jnp.concatenate(
        [edge_u[0:1], stream[:-1]], axis=0
    )
    span = velocity[2]
    row = lax.broadcasted_iota(jnp.int32, (1, tall, 1), 1)
    after = jnp.where(row == tall - 1, edge_w[1][:, None, :], pltpu.roll(span, tall - 1, 1))
    before = jnp.where(row == 0, edge_w[0][:, None, :], pltpu.roll(span, 1, 1))
    divergence = (divergence + (after - before)) * 0.5
    for half in range(wide // 8):
        blocks = exchanged([divergence[half * 8 + i] for i in range(8)], (16, 32, 64))
        for j in range(nz):
            cut[j, :, pl.ds(half * 128, 128)] = blocks[j]

    def cut_copy(d):
        to = lax.rem(gz + d, nz)
        return pltpu.make_async_remote_copy(
            src_ref=cut.at[to],
            dst_ref=planes.at[gz],
            send_sem=c_send.at[to],
            recv_sem=c_recv.at[gz],
            device_id=(gx, to),
            device_id_type=MESH,
        )

    def cut_from(d):
        origin = lax.rem(gz + d, nz)
        return pltpu.make_async_remote_copy(
            src_ref=cut.at[origin],
            dst_ref=planes.at[origin],
            send_sem=c_send.at[origin],
            recv_sem=c_recv.at[origin],
            device_id=(gx, origin),
            device_id_type=MESH,
        )

    def start(make):
        def go(d, carry):
            make(d).start()
            return carry

        return go

    def wait_recv(make):
        def go(d, carry):
            make(d).wait_recv()
            return carry

        return go

    def wait_send(make):
        def go(d, carry):
            make(d).wait_send()
            return carry

        return go

    lax.fori_loop(1, nz, start(cut_copy), 0)
    planes[gz] = cut[gz]
    lax.fori_loop(1, nz, wait_recv(cut_from), 0)
    high, low = parts(planes[...].reshape(nz * tall, 2 * 128))
    modes[...] = dot3(table_z[0], table_z[1], high, low).reshape(modes.shape)

    def mode_copy(d):
        to = lax.rem(gx + d, nx)
        return pltpu.make_async_remote_copy(
            src_ref=modes.at[:, to],
            dst_ref=rows.at[gx],
            send_sem=m_send.at[to],
            recv_sem=m_recv.at[gx],
            device_id=(to, gz),
            device_id_type=MESH,
        )

    def mode_from(d):
        origin = lax.rem(gx + d, nx)
        return pltpu.make_async_remote_copy(
            src_ref=modes.at[:, origin],
            dst_ref=rows.at[origin],
            send_sem=m_send.at[origin],
            recv_sem=m_recv.at[origin],
            device_id=(origin, gz),
            device_id_type=MESH,
        )

    lax.fori_loop(1, nx, start(mode_copy), 0)
    rows[gx] = modes[:, gx]
    lax.fori_loop(1, nx, wait_recv(mode_from), 0)
    columns = []
    for h in range(nx // 16):
        for half in range(2):
            blocks = exchanged(
                [rows[h * 16 + b, :, :, half * 128 : half * 128 + 128] for b in range(16)],
                (1, 2, 4, 8),
            )
            columns.append(
                jnp.concatenate([block[0] for block in blocks] + [block[1] for block in blocks])
            )
    high, low = parts(jnp.concatenate(columns, axis=1))
    lines = high.shape[0] // 2
    for q in range(table_x.shape[1]):
        value = dot3(high, low, table_x[0, q], table_x[1, q])
        real = value[:lines, :128] + value[lines:, 128:]
        imag = value[lines:, :128] - value[:lines, 128:]
        out = pl.ds(q * 128, 128)
        source[0, :, :, out] = (real * scale).reshape(source.shape[1], source.shape[2], 128)
        source[1, :, :, out] = (imag * scale).reshape(source.shape[1], source.shape[2], 128)
    for c in order:
        for copy in z_copies[c] + x_copies[c]:
            copy.wait_send()
    for copy in edges:
        copy.wait_send()
    lax.fori_loop(1, nz, wait_send(cut_copy), 0)
    lax.fori_loop(1, nx, wait_send(mode_copy), 0)


def split_table(table):
    high = table.astype(jnp.bfloat16)
    return np.stack([high, (table - high.astype(np.float64)).astype(jnp.bfloat16)])


def transform_tables(length_x, length_z):
    counter = np.arange(length_z)
    angle = counter[:, None] * counter[None, :] % length_z * (2 * math.pi / length_z)
    table_z = np.concatenate([np.cos(angle), -np.sin(angle)])
    h, half, i, b = np.meshgrid(
        np.arange(length_x // 256), np.arange(2), np.arange(8), np.arange(16), indexing="ij"
    )
    place = (16 * (16 * h + b) + 8 * half + i).reshape(-1)
    mode = np.arange(length_x)
    angle = place[:, None] * mode[None, :] % length_x * (2 * math.pi / length_x)
    both = np.stack([np.cos(angle), np.sin(angle)], axis=1)
    both = both.reshape(length_x, 2, length_x // 128, 128).transpose(2, 0, 1, 3)
    return split_table(table_z), split_table(both.reshape(length_x // 128, length_x, 256))


def spectrum(force, field, tile, nx, nz):
    _, wide, tall, wall = tile
    length_x, length_z = wide * nx, tall * nz
    table_z, table_x = transform_tables(length_x, length_z)
    vector = pl.BlockSpec(memory_space=pltpu.VMEM)
    dma = pltpu.SemaphoreType.DMA
    each = wall // nz
    deep = field.shape[1]
    return pl.pallas_call(
        functools.partial(spectrum_kernel, nx, nz, 1.0 / math.sqrt(length_x * length_z)),
        out_shape=(
            jax.ShapeDtypeStruct(tile, jnp.float32),
            jax.ShapeDtypeStruct((2, each, length_z // nx, length_x), jnp.float32),
        ),
        in_specs=[vector] * 4,
        out_specs=(vector, vector),
        scratch_shapes=[
            pltpu.VMEM((2, 3, deep, SIDE, wall), jnp.float32),
            pltpu.VMEM((2, 3, HALF, tall, wall), jnp.float32),
            pltpu.VMEM((2, 3, HALF, tall, wall), jnp.float32),
            pltpu.VMEM((2, tall, wall), jnp.float32),
            pltpu.VMEM((2, wide, wall), jnp.float32),
            pltpu.VMEM((2, wide, wall), jnp.float32),
            pltpu.VMEM((nz, tall, wide * each), jnp.float32),
            pltpu.VMEM((nz, tall, wide * each), jnp.float32),
            pltpu.VMEM((2, nx, length_z // nx, wide * each), jnp.float32),
            pltpu.VMEM((nx, 2, length_z // nx, wide * each), jnp.float32),
            dma((2, 3)), dma((2, 3)), dma((2, 3)), dma((2, 3)), dma((4,)), dma((4,)),
            dma((nz,)), dma((nz,)), dma((nx,)), dma((nx,)),
        ],
        compiler_params=pltpu.CompilerParams(collective_id=1, has_side_effects=True),
        name="spectrum",
    )(force, field, jnp.asarray(table_z), jnp.asarray(table_x))


def on_device(
    nx, nz, flow_state, slot_ids, corners, marker_cells, marker_frac, particle_velocity,
    particle_spin,
):
    tile_x = flow_state.shape[1]
    tile_z = flow_state.shape[2]
    ghosted = with_halo(flow_state, (("gx", 1), ("gz", 2)), 1)
    extended = padded_2(predict(ghosted), (("gx", 1, HALF), ("gz", 2, SIDE)))
    starts = jnp.stack(
        [
            (corners[0] - lax.axis_index("gx") * tile_x + HALF) % (tile_x * nx),
            corners[1],
            (corners[2] - lax.axis_index("gz") * tile_z + SIDE) % (tile_z * nz),
        ]
    )
    force = spread_forces(
        extended,
        slot_ids,
        starts,
        jnp.transpose(marker_cells, (1, 0, 2)),
        jnp.transpose(marker_frac, (1, 0, 2)),
        particle_velocity,
        particle_spin,
    )
    return spectrum(force, extended, (3,) + flow_state.shape[1:], nx, nz)


def solution(mesh):
    both = ("gx", "gz")
    placed = (
        P(None, "gx", "gz", None),
        P(both),
        P(None, both),
        P(None, both, None),
        P(None, both, None),
        P(),
        P(),
    )
    return jax.shard_map(
        functools.partial(on_device, mesh.shape["gx"], mesh.shape["gz"]),
        mesh=mesh,
        in_specs=placed,
        out_specs=(P(None, "gx", "gz", None), P(None, "gz", "gx", None)),
        check_vma=False,
    )
```

```python
import functools
import math

import jax
import jax.numpy as jnp
import numpy as np
from jax import lax
from jax.experimental import pallas as pl
from jax.experimental.pallas import tpu as pltpu
from jax.sharding import PartitionSpec as P

BOX = 24
HALF = 12
BAND = 32
STEP = 8
SIDE = 16
MESH = pl.DeviceIdType.MESH


time_step = 0.1
viscosity = 0.2
drive_force = 1.0


def remote(source, target, sems, slot, to):
    return pltpu.make_async_remote_copy(
        src_ref=source,
        dst_ref=target,
        send_sem=sems[0].at[slot],
        recv_sem=sems[1].at[slot],
        device_id=to,
        device_id_type=MESH,
    )


def around(nx, nz):
    gx, gz = lax.axis_index("gx"), lax.axis_index("gz")
    return (
        (lax.rem(gx + nx - 1, nx), gz),
        (lax.rem(gx + 1, nx), gz),
        (gx, lax.rem(gz + nz - 1, nz)),
        (gx, lax.rem(gz + 1, nz)),
    )


def front_kernel(
    nx, nz, flow, field, edge_x, edge_z_out, edge_z,
    e_send, e_recv, x_send, x_recv, z_send, z_recv,
):
    _, wide, tall, wall = flow.shape
    left, right, below, above = around(nx, nz)
    barrier = pltpu.get_barrier_semaphore()
    for near in (left, right, below, above):
        pl.semaphore_signal(barrier, inc=1, device_id=near, device_id_type=MESH)
    pl.semaphore_wait(barrier, 4)
    edge_z_out[0] = flow[:, :, 0, :]
    edge_z_out[1] = flow[:, :, tall - 1, :]
    edges = [
        remote(flow.at[:, 0], edge_x.at[1], (e_send, e_recv), 0, left),
        remote(flow.at[:, wide - 1], edge_x.at[0], (e_send, e_recv), 1, right),
        remote(edge_z_out.at[0], edge_z.at[1], (e_send, e_recv), 2, below),
        remote(edge_z_out.at[1], edge_z.at[0], (e_send, e_recv), 3, above),
    ]
    for copy in edges:
        copy.start()
    spread = time_step * viscosity
    carry_by = 0.5 * time_step
    lane = lax.broadcasted_iota(jnp.int32, (tall, wall), 1)
    row = lax.broadcasted_iota(jnp.int32, (tall, wall), 0)
    first_y, last_y = lane == 0, lane == wall - 1
    first_z, last_z = row == 0, row == tall - 1

    def layer(x, back, ahead):
        here = [flow[c, x] for c in range(4)]
        moves = [carry_by * here[d] for d in range(3)]
        for c in range(3):
            f = here[c]
            total = f * (1.0 - 6.0 * spread)
            y_plus = jnp.where(last_y, 0.0, pltpu.roll(f, wall - 1, 1))
            y_minus = jnp.where(first_y, 0.0, pltpu.roll(f, 1, 1))
            z_plus = jnp.where(last_z, 0.0, pltpu.roll(f, tall - 1, 0))
            z_minus = jnp.where(first_z, 0.0, pltpu.roll(f, 1, 0))
            for plus, minus, move in (
                (ahead[c], back[c], moves[0]),
                (y_plus, y_minus, moves[1]),
                (z_plus, z_minus, moves[2]),
            ):
                total += plus * (spread - move) + minus * (spread + move)
            p = here[3]
            if c == 0:
                total += time_step * drive_force - carry_by * (ahead[3] - back[3])
            if c == 1:
                p_plus = jnp.where(last_y, p, pltpu.roll(p, wall - 1, 1))
                p_minus = jnp.where(first_y, p, pltpu.roll(p, 1, 1))
                total -= carry_by * (p_plus - p_minus)
            if c == 2:
                p_plus = jnp.where(last_z, 0.0, pltpu.roll(p, tall - 1, 0))
                p_minus = jnp.where(first_z, 0.0, pltpu.roll(p, 1, 0))
                total -= carry_by * (p_plus - p_minus)
            field[c, HALF + x, pl.ds(SIDE, tall), :] = total

    def inside(x, carry):
        layer(x, [flow[c, x - 1] for c in range(4)], [flow[c, x + 1] for c in range(4)])
        return carry

    lax.fori_loop(1, wide - 1, inside, 0)
    for copy in edges:
        copy.wait_recv()
    layer(0, [edge_x[0, c] for c in range(4)], [flow[c, 1] for c in range(4)])
    layer(
        wide - 1, [flow[c, wide - 2] for c in range(4)], [edge_x[1, c] for c in range(4)]
    )
    own = pl.ds(HALF, wide)
    x_copies, z_copies = [], []
    for c in range(3):
        for side, z, sign in ((0, 0, 1.0), (1, tall - 1, -1.0)):
            move = carry_by * edge_z_out[side, 2]
            add = edge_z[side, c] * (spread + sign * move)
            if c == 2:
                add += sign * carry_by * edge_z[side, 3]
            field[c, own, SIDE + z, :] += add
        inner = pl.ds(SIDE, tall)
        back = remote(
            field.at[c, pl.ds(HALF, HALF), inner],
            field.at[c, pl.ds(HALF + wide, HALF), inner],
            (x_send, x_recv), (0, c), left,
        )
        ahead = remote(
            field.at[c, pl.ds(wide, HALF), inner],
            field.at[c, pl.ds(0, HALF), inner],
            (x_send, x_recv), (1, c), right,
        )
        back.start()
        ahead.start()
        x_copies.append((back, ahead))

    def slabs(c, piece, columns):
        down = remote(
            field.at[c, columns, pl.ds(SIDE, SIDE)],
            field.at[c, columns, pl.ds(SIDE + tall, SIDE)],
            (z_send, z_recv), (0, c, piece), below,
        )
        up = remote(
            field.at[c, columns, pl.ds(tall, SIDE)],
            field.at[c, columns, pl.ds(0, SIDE)],
            (z_send, z_recv), (1, c, piece), above,
        )
        down.start()
        up.start()
        z_copies.extend((down, up))

    for c in range(3):
        slabs(c, 0, own)
    for c in range(3):
        x_copies[c][0].wait_recv()
        slabs(c, 1, pl.ds(HALF + wide, HALF))
        x_copies[c][1].wait_recv()
        slabs(c, 2, pl.ds(0, HALF))
    for copy in z_copies:
        copy.wait_recv()
    for copy in edges + z_copies + [copy for pair in x_copies for copy in pair]:
        copy.wait_send()


def predict(flow, nx, nz):
    _, wide, tall, wall = flow.shape
    dma = pltpu.SemaphoreType.DMA
    return pl.pallas_call(
        functools.partial(front_kernel, nx, nz),
        out_shape=jax.ShapeDtypeStruct(
            (3, wide + 2 * HALF, tall + 2 * SIDE, wall), jnp.float32
        ),
        in_specs=[pl.BlockSpec(memory_space=pltpu.VMEM)],
        out_specs=pl.BlockSpec(memory_space=pltpu.VMEM),
        scratch_shapes=[
            pltpu.VMEM((2, 4, tall, wall), jnp.float32),
            pltpu.VMEM((2, 4, wide, wall), jnp.float32),
            pltpu.VMEM((2, 4, wide, wall), jnp.float32),
            dma((4,)), dma((4,)), dma((2, 3)), dma((2, 3)), dma((2, 3, 3)), dma((2, 3, 3)),
        ],
        compiler_params=pltpu.CompilerParams(collective_id=0, has_side_effects=True),
        name="front",
    )(flow)


def parts(value):
    high = value.astype(jnp.bfloat16)
    return high, (value - high.astype(jnp.float32)).astype(jnp.bfloat16)


def tap_weights(length, first, taps):
    offset = lax.broadcasted_iota(jnp.int32, (length, first.shape[-1]), 0) - first
    weight = jnp.where(offset == 3, taps[3], 0.0)
    for t in (2, 1, 0):
        weight = jnp.where(offset == t, taps[t], weight)
    return weight


def dot(a, b, across):
    return lax.dot_general(
        a, b, (((1,), (across,)), ((), ())), preferred_element_type=jnp.float32
    )


def marker_kernel(
    ids, starts, moving, turning, cells, fracs, field, force, tap, cross, spread, way_y, load
):
    force[...] = jnp.zeros_like(force)
    half_pi = 0.5 * math.pi
    angle = fracs[...] * half_pi
    cosine, sine = jnp.cos(angle), jnp.sin(angle)
    tap[0] = 0.25 * (1.0 - sine)
    tap[1] = 0.25 * (1.0 + cosine)
    tap[2] = 0.25 * (1.0 + sine)
    tap[3] = 0.25 * (1.0 - cosine)
    markers = fracs.shape[2]
    wall = field.shape[3]

    def one_slot(s, carry):
        @pl.when(ids[s] >= 0)
        def _():
            n = ids[s]
            x0, y0, z0 = starts[0, s], starts[1, s], starts[2, s]
            zb = pl.multiple_of((z0 // 8) * 8, 8)
            cell = cells[:, pl.ds(s, 1), :].reshape(3, markers)
            frac = fracs[:, pl.ds(s, 1), :].reshape(3, markers)
            taps = [tap[t, :, pl.ds(s, 1), :].reshape(3, markers) for t in range(4)]

            def along(d):
                return [w[d : d + 1] for w in taps]

            weight_x = tap_weights(BOX, cell[0:1] - 1, along(0))
            weight_y = tap_weights(wall, cell[1:2] - 1 + y0, along(1))
            weight_z = tap_weights(BAND, cell[2:3] - 1 + (z0 - zb), along(2))
            for i in range(BOX):
                cross[i // STEP, i % STEP] = weight_x[i : i + 1] * weight_z
            spread[...] = weight_y
            y_high, y_low = parts(weight_y)
            way_y[0] = y_high
            way_y[1] = y_low

            def sample(t, total):
                window = field[:, pl.ds(x0 + t * STEP, STEP), pl.ds(zb, BAND), :]
                high, low = parts(window.reshape(3 * STEP * BAND, wall))
                value = dot(high, way_y[0], 0) + dot(low, way_y[0], 0) + dot(high, way_y[1], 0)
                value = value.reshape(3, STEP * BAND // 8, 8, markers)
                factor = cross[t].reshape(1, STEP * BAND // 8, 8, markers)
                return total + jnp.sum(value * factor, axis=1)

            total = lax.fori_loop(
                0, BOX // STEP, sample, jnp.zeros((3, 8, markers), jnp.float32)
            )
            sampled = jnp.sum(total, axis=1)
            lever = cell.astype(jnp.float32) + frac - float(HALF)
            spin = [turning[c, n] for c in range(3)]
            for c in range(3):
                a, b = (c + 1) % 3, (c + 2) % 3
                target = moving[c, n] + (spin[a] * lever[b : b + 1] - spin[b] * lever[a : a + 1])
                push = target - sampled[c : c + 1]
                high, low = parts(spread[...] * push)
                load[0, pl.ds(c * wall, wall), :] = high
                load[1, pl.ds(c * wall, wall), :] = low

            def scatter(t, carry):
                high, low = parts(cross[t].reshape(STEP * BAND, markers))
                value = dot(high, load[0], 1) + dot(low, load[0], 1) + dot(high, load[1], 1)
                for c in range(3):
                    force[c, pl.ds(x0 + t * STEP, STEP), pl.ds(zb, BAND), :] += value[
                        :, c * wall : (c + 1) * wall
                    ].reshape(STEP, BAND, wall)
                return carry

            lax.fori_loop(0, BOX // STEP, scatter, 0)

        return carry

    lax.fori_loop(0, ids.shape[0], one_slot, 0)


def spread_forces(extended, slot_ids, starts, cells, fracs, moving, turning):
    _, slots, markers = cells.shape
    wall = extended.shape[3]
    scalar = pl.BlockSpec(memory_space=pltpu.SMEM)
    vector = pl.BlockSpec(memory_space=pltpu.VMEM)
    return pl.pallas_call(
        marker_kernel,
        out_shape=jax.ShapeDtypeStruct(extended.shape, jnp.float32),
        in_specs=[scalar] * 4 + [vector] * 3,
        out_specs=vector,
        scratch_shapes=[
            pltpu.VMEM((4, 3, slots, markers), jnp.float32),
            pltpu.VMEM((BOX // STEP, STEP, BAND, markers), jnp.float32),
            pltpu.VMEM((wall, markers), jnp.float32),
            pltpu.VMEM((2, wall, markers), jnp.bfloat16),
            pltpu.VMEM((2, 3 * wall, markers), jnp.bfloat16),
        ],
        name="markers",
    )(slot_ids, starts, moving, turning, cells, fracs, extended)


def dot3(high, low, other_high, other_low):
    return dot(high, other_high, 0) + dot(low, other_high, 0) + dot(high, other_low, 0)


def exchanged(rows, lane_bits):
    lane = lax.broadcasted_iota(jnp.int32, rows[0].shape, rows[0].ndim - 1)
    axis = rows[0].ndim - 1
    for bit, shift in enumerate(lane_bits):
        low = (lane & shift) == 0
        step = 1 << bit
        out = list(rows)
        for m in range(len(rows)):
            if m & step == 0:
                a, b = rows[m], rows[m + step]
                out[m] = jnp.where(low, a, pltpu.roll(b, shift, axis))
                out[m + step] = jnp.where(low, pltpu.roll(a, 128 - shift, axis), b)
        rows = out
    return rows


def spectrum_kernel(
    nx, nz, scale, force, field, table_z, table_x, velocity, source,
    z_got, x_out, x_got, edge_u, edge_w, edge_w_out, cut, planes, modes, rows,
    z_send, z_recv, x_send, x_recv, e_send, e_recv, c_send, c_recv, m_send, m_recv,
):
    gx, gz = lax.axis_index("gx"), lax.axis_index("gz")
    below = (gx, lax.rem(gz + nz - 1, nz))
    above = (gx, lax.rem(gz + 1, nz))
    left = (lax.rem(gx + nx - 1, nx), gz)
    right = (lax.rem(gx + 1, nx), gz)
    barrier = pltpu.get_barrier_semaphore()

    def greet_z(d, carry):
        pl.semaphore_signal(
            barrier, inc=1, device_id=(gx, lax.rem(gz + d, nz)), device_id_type=MESH
        )
        return carry

    def greet_x(d, carry):
        pl.semaphore_signal(
            barrier, inc=1, device_id=(lax.rem(gx + d, nx), gz), device_id_type=MESH
        )
        return carry

    lax.fori_loop(1, nz, greet_z, 0)
    lax.fori_loop(1, nx, greet_x, 0)
    pl.semaphore_wait(barrier, nx + nz - 2)

    wide, tall = velocity.shape[1], velocity.shape[2]
    order = (0, 2, 1)
    z_copies, x_copies = {}, {}
    for c in order:
        down = remote(
            force.at[c, :, pl.ds(0, SIDE), :], z_got.at[1, c], (z_send, z_recv), (1, c), below
        )
        up = remote(
            force.at[c, :, pl.ds(SIDE + tall, SIDE), :],
            z_got.at[0, c],
            (z_send, z_recv),
            (0, c),
            above,
        )
        down.start()
        up.start()
        z_copies[c] = (down, up)
    for c in order:
        for copy in z_copies[c]:
            copy.wait_recv()
        for part in range(2):
            inner = pl.ds(part * SIDE, SIDE)
            outer = pl.ds(SIDE + part * SIDE, SIDE)
            x_out[0, c, :, inner, :] = (
                force[c, pl.ds(0, HALF), outer, :] + z_got[part, c, pl.ds(0, HALF)]
            )
            x_out[1, c, :, inner, :] = (
                force[c, pl.ds(HALF + wide, HALF), outer, :]
                + z_got[part, c, pl.ds(HALF + wide, HALF)]
            )
        back = remote(x_out.at[0, c], x_got.at[1, c], (x_send, x_recv), (1, c), left)
        ahead = remote(x_out.at[1, c], x_got.at[0, c], (x_send, x_recv), (0, c), right)
        back.start()
        ahead.start()
        x_copies[c] = (back, ahead)
        for part in range(2):
            inner = pl.ds(part * SIDE, SIDE)
            outer = pl.ds(SIDE + part * SIDE, SIDE)
            velocity[c, :, inner, :] = (
                field[c, pl.ds(HALF, wide), outer, :]
                + force[c, pl.ds(HALF, wide), outer, :]
                + z_got[part, c, pl.ds(HALF, wide)]
            )
    edges = []
    for c in order:
        for copy in x_copies[c]:
            copy.wait_recv()
        velocity[c, pl.ds(0, HALF)] += x_got[0, c]
        velocity[c, pl.ds(wide - HALF, HALF)] += x_got[1, c]
        if c == 0:
            edges += [
                remote(velocity.at[0, 0], edge_u.at[1], (e_send, e_recv), 0, left),
                remote(velocity.at[0, wide - 1], edge_u.at[0], (e_send, e_recv), 1, right),
            ]
        if c == 2:
            edge_w_out[0] = velocity[2, :, 0, :]
            edge_w_out[1] = velocity[2, :, tall - 1, :]
            edges += [
                remote(edge_w_out.at[0], edge_w.at[1], (e_send, e_recv), 2, below),
                remote(edge_w_out.at[1], edge_w.at[0], (e_send, e_recv), 3, above),
            ]
        if c != 1:
            edges[-2].start()
            edges[-1].start()
    wall = velocity.shape[3]
    lane = lax.broadcasted_iota(jnp.int32, (1, 1, wall), 2)
    normal = velocity[1]
    upper = jnp.where(lane == wall - 1, 0.0, pltpu.roll(normal, wall - 1, 2))
    lower = jnp.where(lane == 0, 0.0, pltpu.roll(normal, 1, 2))
    divergence = upper - lower
    for copy in edges:
        copy.wait_recv()
    stream = velocity[0]
    divergence += jnp.concatenate([stream[1:], edge_u[1:2]], axis=0) - jnp.concatenate(
        [edge_u[0:1], stream[:-1]], axis=0
    )
    span = velocity[2]
    row = lax.broadcasted_iota(jnp.int32, (1, tall, 1), 1)
    after = jnp.where(row == tall - 1, edge_w[1][:, None, :], pltpu.roll(span, tall - 1, 1))
    before = jnp.where(row == 0, edge_w[0][:, None, :], pltpu.roll(span, 1, 1))
    divergence = (divergence + (after - before)) * 0.5
    for half in range(wide // 8):
        blocks = exchanged([divergence[half * 8 + i] for i in range(8)], (16, 32, 64))
        for j in range(nz):
            cut[j, :, pl.ds(half * 128, 128)] = blocks[j]

    def cut_copy(d):
        to = lax.rem(gz + d, nz)
        return pltpu.make_async_remote_copy(
            src_ref=cut.at[to],
            dst_ref=planes.at[gz],
            send_sem=c_send.at[to],
            recv_sem=c_recv.at[gz],
            device_id=(gx, to),
            device_id_type=MESH,
        )

    def cut_from(d):
        origin = lax.rem(gz + d, nz)
        return pltpu.make_async_remote_copy(
            src_ref=cut.at[origin],
            dst_ref=planes.at[origin],
            send_sem=c_send.at[origin],
            recv_sem=c_recv.at[origin],
            device_id=(gx, origin),
            device_id_type=MESH,
        )

    def start(make):
        def go(d, carry):
            make(d).start()
            return carry

        return go

    def wait_recv(make):
        def go(d, carry):
            make(d).wait_recv()
            return carry

        return go

    def wait_send(make):
        def go(d, carry):
            make(d).wait_send()
            return carry

        return go

    lax.fori_loop(1, nz, start(cut_copy), 0)
    planes[gz] = cut[gz]
    lax.fori_loop(1, nz, wait_recv(cut_from), 0)
    high, low = parts(planes[...].reshape(nz * tall, 2 * 128))
    modes[...] = dot3(table_z[0], table_z[1], high, low).reshape(modes.shape)

    def mode_copy(d):
        to = lax.rem(gx + d, nx)
        return pltpu.make_async_remote_copy(
            src_ref=modes.at[:, to],
            dst_ref=rows.at[gx],
            send_sem=m_send.at[to],
            recv_sem=m_recv.at[gx],
            device_id=(to, gz),
            device_id_type=MESH,
        )

    def mode_from(d):
        origin = lax.rem(gx + d, nx)
        return pltpu.make_async_remote_copy(
            src_ref=modes.at[:, origin],
            dst_ref=rows.at[origin],
            send_sem=m_send.at[origin],
            recv_sem=m_recv.at[origin],
            device_id=(origin, gz),
            device_id_type=MESH,
        )

    lax.fori_loop(1, nx, start(mode_copy), 0)
    rows[gx] = modes[:, gx]
    lax.fori_loop(1, nx, wait_recv(mode_from), 0)
    columns = []
    for h in range(nx // 16):
        for half in range(2):
            blocks = exchanged(
                [rows[h * 16 + b, :, :, half * 128 : half * 128 + 128] for b in range(16)],
                (1, 2, 4, 8),
            )
            columns.append(
                jnp.concatenate([block[0] for block in blocks] + [block[1] for block in blocks])
            )
    high, low = parts(jnp.concatenate(columns, axis=1))
    lines = high.shape[0] // 2
    for q in range(table_x.shape[1]):
        value = dot3(high, low, table_x[0, q], table_x[1, q])
        real = value[:lines, :128] + value[lines:, 128:]
        imag = value[lines:, :128] - value[:lines, 128:]
        out = pl.ds(q * 128, 128)
        source[0, :, :, out] = (real * scale).reshape(source.shape[1], source.shape[2], 128)
        source[1, :, :, out] = (imag * scale).reshape(source.shape[1], source.shape[2], 128)
    for c in order:
        for copy in z_copies[c] + x_copies[c]:
            copy.wait_send()
    for copy in edges:
        copy.wait_send()
    lax.fori_loop(1, nz, wait_send(cut_copy), 0)
    lax.fori_loop(1, nx, wait_send(mode_copy), 0)


def split_table(table):
    high = table.astype(jnp.bfloat16)
    return np.stack([high, (table - high.astype(np.float64)).astype(jnp.bfloat16)])


def transform_tables(length_x, length_z):
    counter = np.arange(length_z)
    angle = counter[:, None] * counter[None, :] % length_z * (2 * math.pi / length_z)
    table_z = np.concatenate([np.cos(angle), -np.sin(angle)])
    h, half, i, b = np.meshgrid(
        np.arange(length_x // 256), np.arange(2), np.arange(8), np.arange(16), indexing="ij"
    )
    place = (16 * (16 * h + b) + 8 * half + i).reshape(-1)
    mode = np.arange(length_x)
    angle = place[:, None] * mode[None, :] % length_x * (2 * math.pi / length_x)
    both = np.stack([np.cos(angle), np.sin(angle)], axis=1)
    both = both.reshape(length_x, 2, length_x // 128, 128).transpose(2, 0, 1, 3)
    return split_table(table_z), split_table(both.reshape(length_x // 128, length_x, 256))


def spectrum(force, field, tile, nx, nz):
    _, wide, tall, wall = tile
    length_x, length_z = wide * nx, tall * nz
    table_z, table_x = transform_tables(length_x, length_z)
    vector = pl.BlockSpec(memory_space=pltpu.VMEM)
    dma = pltpu.SemaphoreType.DMA
    each = wall // nz
    deep = field.shape[1]
    return pl.pallas_call(
        functools.partial(spectrum_kernel, nx, nz, 1.0 / math.sqrt(length_x * length_z)),
        out_shape=(
            jax.ShapeDtypeStruct(tile, jnp.float32),
            jax.ShapeDtypeStruct((2, each, length_z // nx, length_x), jnp.float32),
        ),
        in_specs=[vector] * 4,
        out_specs=(vector, vector),
        scratch_shapes=[
            pltpu.VMEM((2, 3, deep, SIDE, wall), jnp.float32),
            pltpu.VMEM((2, 3, HALF, tall, wall), jnp.float32),
            pltpu.VMEM((2, 3, HALF, tall, wall), jnp.float32),
            pltpu.VMEM((2, tall, wall), jnp.float32),
            pltpu.VMEM((2, wide, wall), jnp.float32),
            pltpu.VMEM((2, wide, wall), jnp.float32),
            pltpu.VMEM((nz, tall, wide * each), jnp.float32),
            pltpu.VMEM((nz, tall, wide * each), jnp.float32),
            pltpu.VMEM((2, nx, length_z // nx, wide * each), jnp.float32),
            pltpu.VMEM((nx, 2, length_z // nx, wide * each), jnp.float32),
            dma((2, 3)), dma((2, 3)), dma((2, 3)), dma((2, 3)), dma((4,)), dma((4,)),
            dma((nz,)), dma((nz,)), dma((nx,)), dma((nx,)),
        ],
        compiler_params=pltpu.CompilerParams(collective_id=1, has_side_effects=True),
        name="spectrum",
    )(force, field, jnp.asarray(table_z), jnp.asarray(table_x))


def on_device(
    nx, nz, flow_state, slot_ids, corners, marker_cells, marker_frac, particle_velocity,
    particle_spin,
):
    tile_x = flow_state.shape[1]
    tile_z = flow_state.shape[2]
    extended = predict(flow_state, nx, nz)
    starts = jnp.stack(
        [
            (corners[0] - lax.axis_index("gx") * tile_x + HALF) % (tile_x * nx),
            corners[1],
            (corners[2] - lax.axis_index("gz") * tile_z + SIDE) % (tile_z * nz),
        ]
    )
    force = spread_forces(
        extended,
        slot_ids,
        starts,
        marker_cells,
        marker_frac,
        particle_velocity,
        particle_spin,
    )
    return spectrum(force, extended, (3,) + flow_state.shape[1:], nx, nz)


def solution(mesh):
    both = ("gx", "gz")
    placed = (
        P(None, "gx", "gz", None),
        P(both),
        P(None, both),
        P(None, both, None),
        P(None, both, None),
        P(),
        P(),
    )
    return jax.shard_map(
        functools.partial(on_device, mesh.shape["gx"], mesh.shape["gz"]),
        mesh=mesh,
        in_specs=placed,
        out_specs=(P(None, "gx", "gz", None), P(None, "gz", "gx", None)),
        check_vma=False,
    )
```

```python
import functools
import math

import jax
import jax.numpy as jnp
import numpy as np
from jax import lax
from jax.experimental import pallas as pl
from jax.experimental.pallas import tpu as pltpu
from jax.sharding import PartitionSpec as P

BOX = 24
HALF = 12
BAND = 32
SIDE = 16
MESH = pl.DeviceIdType.MESH


time_step = 0.1
viscosity = 0.2
drive_force = 1.0


def remote(source, target, sems, slot, to):
    return pltpu.make_async_remote_copy(
        src_ref=source,
        dst_ref=target,
        send_sem=sems[0].at[slot],
        recv_sem=sems[1].at[slot],
        device_id=to,
        device_id_type=MESH,
    )


def around(nx, nz):
    gx, gz = lax.axis_index("gx"), lax.axis_index("gz")
    return (
        (lax.rem(gx + nx - 1, nx), gz),
        (lax.rem(gx + 1, nx), gz),
        (gx, lax.rem(gz + nz - 1, nz)),
        (gx, lax.rem(gz + 1, nz)),
    )


def front_kernel(
    nx, nz, flow, field, edge_x, edge_z_out, edge_z,
    e_send, e_recv, x_send, x_recv, z_send, z_recv,
):
    _, wide, tall, wall = flow.shape
    left, right, below, above = around(nx, nz)
    barrier = pltpu.get_barrier_semaphore()
    for near in (left, right, below, above):
        pl.semaphore_signal(barrier, inc=1, device_id=near, device_id_type=MESH)
    pl.semaphore_wait(barrier, 4)
    edge_z_out[0] = flow[:, :, 0, :]
    edge_z_out[1] = flow[:, :, tall - 1, :]
    edges = [
        remote(flow.at[:, 0], edge_x.at[1], (e_send, e_recv), 0, left),
        remote(flow.at[:, wide - 1], edge_x.at[0], (e_send, e_recv), 1, right),
        remote(edge_z_out.at[0], edge_z.at[1], (e_send, e_recv), 2, below),
        remote(edge_z_out.at[1], edge_z.at[0], (e_send, e_recv), 3, above),
    ]
    for copy in edges:
        copy.start()
    spread = time_step * viscosity
    carry_by = 0.5 * time_step
    lane = lax.broadcasted_iota(jnp.int32, (tall, wall), 1)
    row = lax.broadcasted_iota(jnp.int32, (tall, wall), 0)
    first_y, last_y = lane == 0, lane == wall - 1
    first_z, last_z = row == 0, row == tall - 1

    def layer(x, back, ahead):
        here = [flow[c, x] for c in range(4)]
        moves = [carry_by * here[d] for d in range(3)]
        for c in range(3):
            f = here[c]
            total = f * (1.0 - 6.0 * spread)
            y_plus = jnp.where(last_y, 0.0, pltpu.roll(f, wall - 1, 1))
            y_minus = jnp.where(first_y, 0.0, pltpu.roll(f, 1, 1))
            z_plus = jnp.where(last_z, 0.0, pltpu.roll(f, tall - 1, 0))
            z_minus = jnp.where(first_z, 0.0, pltpu.roll(f, 1, 0))
            for plus, minus, move in (
                (ahead[c], back[c], moves[0]),
                (y_plus, y_minus, moves[1]),
                (z_plus, z_minus, moves[2]),
            ):
                total += plus * (spread - move) + minus * (spread + move)
            p = here[3]
            if c == 0:
                total += time_step * drive_force - carry_by * (ahead[3] - back[3])
            if c == 1:
                p_plus = jnp.where(last_y, p, pltpu.roll(p, wall - 1, 1))
                p_minus = jnp.where(first_y, p, pltpu.roll(p, 1, 1))
                total -= carry_by * (p_plus - p_minus)
            if c == 2:
                p_plus = jnp.where(last_z, 0.0, pltpu.roll(p, tall - 1, 0))
                p_minus = jnp.where(first_z, 0.0, pltpu.roll(p, 1, 0))
                total -= carry_by * (p_plus - p_minus)
            field[c, HALF + x, pl.ds(SIDE, tall), :] = total

    def inside(x, carry):
        layer(x, [flow[c, x - 1] for c in range(4)], [flow[c, x + 1] for c in range(4)])
        return carry

    lax.fori_loop(1, wide - 1, inside, 0)
    for copy in edges:
        copy.wait_recv()
    layer(0, [edge_x[0, c] for c in range(4)], [flow[c, 1] for c in range(4)])
    layer(
        wide - 1, [flow[c, wide - 2] for c in range(4)], [edge_x[1, c] for c in range(4)]
    )
    own = pl.ds(HALF, wide)
    x_copies, z_copies = [], []
    for c in range(3):
        for side, z, sign in ((0, 0, 1.0), (1, tall - 1, -1.0)):
            move = carry_by * edge_z_out[side, 2]
            add = edge_z[side, c] * (spread + sign * move)
            if c == 2:
                add += sign * carry_by * edge_z[side, 3]
            field[c, own, SIDE + z, :] += add
        inner = pl.ds(SIDE, tall)
        back = remote(
            field.at[c, pl.ds(HALF, HALF), inner],
            field.at[c, pl.ds(HALF + wide, HALF), inner],
            (x_send, x_recv), (0, c), left,
        )
        ahead = remote(
            field.at[c, pl.ds(wide, HALF), inner],
            field.at[c, pl.ds(0, HALF), inner],
            (x_send, x_recv), (1, c), right,
        )
        back.start()
        ahead.start()
        x_copies.append((back, ahead))

    def slabs(c, piece, columns):
        down = remote(
            field.at[c, columns, pl.ds(SIDE, SIDE)],
            field.at[c, columns, pl.ds(SIDE + tall, SIDE)],
            (z_send, z_recv), (0, c, piece), below,
        )
        up = remote(
            field.at[c, columns, pl.ds(tall, SIDE)],
            field.at[c, columns, pl.ds(0, SIDE)],
            (z_send, z_recv), (1, c, piece), above,
        )
        down.start()
        up.start()
        z_copies.extend((down, up))

    for c in range(3):
        slabs(c, 0, own)
    for c in range(3):
        x_copies[c][0].wait_recv()
        slabs(c, 1, pl.ds(HALF + wide, HALF))
        x_copies[c][1].wait_recv()
        slabs(c, 2, pl.ds(0, HALF))
    for copy in z_copies:
        copy.wait_recv()
    for copy in edges + z_copies + [copy for pair in x_copies for copy in pair]:
        copy.wait_send()


def predict(flow, nx, nz):
    _, wide, tall, wall = flow.shape
    dma = pltpu.SemaphoreType.DMA
    return pl.pallas_call(
        functools.partial(front_kernel, nx, nz),
        out_shape=jax.ShapeDtypeStruct(
            (3, wide + 2 * HALF, tall + 2 * SIDE, wall), jnp.float32
        ),
        in_specs=[pl.BlockSpec(memory_space=pltpu.VMEM)],
        out_specs=pl.BlockSpec(memory_space=pltpu.VMEM),
        scratch_shapes=[
            pltpu.VMEM((2, 4, tall, wall), jnp.float32),
            pltpu.VMEM((2, 4, wide, wall), jnp.float32),
            pltpu.VMEM((2, 4, wide, wall), jnp.float32),
            dma((4,)), dma((4,)), dma((2, 3)), dma((2, 3)), dma((2, 3, 3)), dma((2, 3, 3)),
        ],
        compiler_params=pltpu.CompilerParams(
            collective_id=0, has_side_effects=True, vmem_limit_bytes=12 << 20
        ),
        name="front",
    )(flow)


def parts(value):
    high = value.astype(jnp.bfloat16)
    return high, (value - high.astype(jnp.float32)).astype(jnp.bfloat16)


def tap_weights(length, first, taps):
    offset = lax.broadcasted_iota(jnp.int32, (length, first.shape[-1]), 0) - first
    weight = jnp.where(offset == 3, taps[3], 0.0)
    for t in (2, 1, 0):
        weight = jnp.where(offset == t, taps[t], weight)
    return weight


def dot(a, b, across):
    return lax.dot_general(
        a, b, (((1,), (across,)), ((), ())), preferred_element_type=jnp.float32
    )


def pair(a, b, across):
    rows = a[0].shape[0]
    both = dot(jnp.concatenate(a), b[0], across)
    return both[:rows] + both[rows:] + dot(a[0], b[1], across)


def marker_kernel(
    nx, nz, ids, corners, moving, turning, cells, fracs, field, force, tap, cross
):
    force[...] = jnp.zeros_like(force)
    half_pi = 0.5 * math.pi
    angle = fracs[...] * half_pi
    cosine, sine = jnp.cos(angle), jnp.sin(angle)
    tap[0] = 0.25 * (1.0 - sine)
    tap[1] = 0.25 * (1.0 + cosine)
    tap[2] = 0.25 * (1.0 + sine)
    tap[3] = 0.25 * (1.0 - cosine)
    markers = fracs.shape[2]
    wall = field.shape[3]
    wide, tall = field.shape[1] - 2 * HALF, field.shape[2] - 2 * SIDE
    first_x = lax.axis_index("gx") * wide - HALF
    first_z = lax.axis_index("gz") * tall - SIDE
    many = wall // BAND
    lane = lax.broadcasted_iota(jnp.int32, (1, 1, wall), 2)

    def one_slot(s, carry):
        @pl.when(ids[s] >= 0)
        def _():
            n = ids[s]
            x0 = lax.rem(corners[0, s] - first_x + wide * nx, wide * nx)
            y0 = corners[1, s]
            z0 = lax.rem(corners[2, s] - first_z + tall * nz, tall * nz)
            zb = pl.multiple_of((z0 // 8) * 8, 8)
            cell = cells[:, pl.ds(s, 1), :].reshape(3, markers)
            frac = fracs[:, pl.ds(s, 1), :].reshape(3, markers)
            taps = [tap[t, :, pl.ds(s, 1), :].reshape(3, markers) for t in range(4)]

            def along(d):
                return [w[d : d + 1] for w in taps]

            weight_x = tap_weights(BOX, cell[0:1] - 1, along(0))
            weight_y = tap_weights(BAND, cell[1:2] - 1, along(1))
            weight_z = tap_weights(BAND, cell[2:3] - 1 + (z0 - zb), along(2))
            for i in range(BOX):
                high, low = parts(weight_x[i : i + 1] * weight_y)
                cross[0, pl.ds(i * BAND, BAND), :] = high
                cross[1, pl.ds(i * BAND, BAND), :] = low
            columns = []
            for q in range(BOX // many):
                packed = None
                for r in range(many):
                    piece = field[:, x0 + (q * many + r), pl.ds(zb, BAND), :]
                    piece = pltpu.roll(piece, lax.rem(wall + r * BAND - y0, wall), 2)
                    packed = piece if r == 0 else jnp.where(lane < r * BAND, packed, piece)
                columns.append(packed.reshape(3 * BAND, wall))
            window = parts(jnp.concatenate(columns, axis=1))
            value = pair(window, (cross[0], cross[1]), 0).reshape(3, BAND, markers)
            sampled = jnp.sum(value * weight_z[None], axis=1)
            lever = cell.astype(jnp.float32) + frac - float(HALF)
            spin = [turning[c, n] for c in range(3)]
            loads = []
            for c in range(3):
                a, b = (c + 1) % 3, (c + 2) % 3
                target = moving[c, n] + (spin[a] * lever[b : b + 1] - spin[b] * lever[a : a + 1])
                loads.append((target - sampled[c : c + 1]) * weight_z)
            load = parts(jnp.concatenate(loads))
            value = pair(load, (cross[0], cross[1]), 1).reshape(3, BAND, BOX * BAND)
            inside = (lane >= y0) & (lane < y0 + BOX)
            for i in range(BOX):
                q, r = i // many, i % many
                piece = value[:, :, q * wall : (q + 1) * wall]
                piece = pltpu.roll(piece, lax.rem(wall + y0 - r * BAND, wall), 2)
                force[:, x0 + i, pl.ds(zb, BAND), :] += jnp.where(inside, piece, 0.0)

        return carry

    lax.fori_loop(0, ids.shape[0], one_slot, 0)


def spread_forces(nx, nz, extended, slot_ids, corners, cells, fracs, moving, turning):
    _, slots, markers = cells.shape
    scalar = pl.BlockSpec(memory_space=pltpu.SMEM)
    vector = pl.BlockSpec(memory_space=pltpu.VMEM)
    return pl.pallas_call(
        functools.partial(marker_kernel, nx, nz),
        out_shape=jax.ShapeDtypeStruct(extended.shape, jnp.float32),
        in_specs=[scalar] * 4 + [vector] * 3,
        out_specs=vector,
        scratch_shapes=[
            pltpu.VMEM((4, 3, slots, markers), jnp.float32),
            pltpu.VMEM((2, BOX * BAND, markers), jnp.bfloat16),
        ],
        compiler_params=pltpu.CompilerParams(vmem_limit_bytes=24 << 20),
        name="markers",
    )(slot_ids, corners, moving, turning, cells, fracs, extended)


def dot3(high, low, other_high, other_low):
    return dot(high, other_high, 0) + dot(low, other_high, 0) + dot(high, other_low, 0)


def exchanged(rows, lane_bits):
    lane = lax.broadcasted_iota(jnp.int32, rows[0].shape, rows[0].ndim - 1)
    axis = rows[0].ndim - 1
    for bit, shift in enumerate(lane_bits):
        low = (lane & shift) == 0
        step = 1 << bit
        out = list(rows)
        for m in range(len(rows)):
            if m & step == 0:
                a, b = rows[m], rows[m + step]
                out[m] = jnp.where(low, a, pltpu.roll(b, shift, axis))
                out[m + step] = jnp.where(low, pltpu.roll(a, 128 - shift, axis), b)
        rows = out
    return rows


def spectrum_kernel(
    nx, nz, scale, force, field, table_z, table_x, velocity, source,
    z_got, x_out, x_got, edge_u, edge_w, edge_w_out, cut, planes, modes, rows,
    z_send, z_recv, x_send, x_recv, e_send, e_recv, c_send, c_recv, m_send, m_recv,
):
    gx, gz = lax.axis_index("gx"), lax.axis_index("gz")
    below = (gx, lax.rem(gz + nz - 1, nz))
    above = (gx, lax.rem(gz + 1, nz))
    left = (lax.rem(gx + nx - 1, nx), gz)
    right = (lax.rem(gx + 1, nx), gz)
    barrier = pltpu.get_barrier_semaphore()

    def greet_z(d, carry):
        pl.semaphore_signal(
            barrier, inc=1, device_id=(gx, lax.rem(gz + d, nz)), device_id_type=MESH
        )
        return carry

    def greet_x(d, carry):
        pl.semaphore_signal(
            barrier, inc=1, device_id=(lax.rem(gx + d, nx), gz), device_id_type=MESH
        )
        return carry

    lax.fori_loop(1, nz, greet_z, 0)
    lax.fori_loop(1, nx, greet_x, 0)
    pl.semaphore_wait(barrier, nx + nz - 2)

    wide, tall = velocity.shape[1], velocity.shape[2]
    order = (0, 2, 1)
    z_copies, x_copies = {}, {}
    for c in order:
        down = remote(
            force.at[c, :, pl.ds(0, SIDE), :], z_got.at[1, c], (z_send, z_recv), (1, c), below
        )
        up = remote(
            force.at[c, :, pl.ds(SIDE + tall, SIDE), :],
            z_got.at[0, c],
            (z_send, z_recv),
            (0, c),
            above,
        )
        down.start()
        up.start()
        z_copies[c] = (down, up)
    for c in order:
        for copy in z_copies[c]:
            copy.wait_recv()
        for part in range(2):
            inner = pl.ds(part * SIDE, SIDE)
            outer = pl.ds(SIDE + part * SIDE, SIDE)
            x_out[0, c, :, inner, :] = (
                force[c, pl.ds(0, HALF), outer, :] + z_got[part, c, pl.ds(0, HALF)]
            )
            x_out[1, c, :, inner, :] = (
                force[c, pl.ds(HALF + wide, HALF), outer, :]
                + z_got[part, c, pl.ds(HALF + wide, HALF)]
            )
        back = remote(x_out.at[0, c], x_got.at[1, c], (x_send, x_recv), (1, c), left)
        ahead = remote(x_out.at[1, c], x_got.at[0, c], (x_send, x_recv), (0, c), right)
        back.start()
        ahead.start()
        x_copies[c] = (back, ahead)
        for part in range(2):
            inner = pl.ds(part * SIDE, SIDE)
            outer = pl.ds(SIDE + part * SIDE, SIDE)
            velocity[c, :, inner, :] = (
                field[c, pl.ds(HALF, wide), outer, :]
                + force[c, pl.ds(HALF, wide), outer, :]
                + z_got[part, c, pl.ds(HALF, wide)]
            )
    edges = []
    for c in order:
        for copy in x_copies[c]:
            copy.wait_recv()
        velocity[c, pl.ds(0, HALF)] += x_got[0, c]
        velocity[c, pl.ds(wide - HALF, HALF)] += x_got[1, c]
        if c == 0:
            edges += [
                remote(velocity.at[0, 0], edge_u.at[1], (e_send, e_recv), 0, left),
                remote(velocity.at[0, wide - 1], edge_u.at[0], (e_send, e_recv), 1, right),
            ]
        if c == 2:
            edge_w_out[0] = velocity[2, :, 0, :]
            edge_w_out[1] = velocity[2, :, tall - 1, :]
            edges += [
                remote(edge_w_out.at[0], edge_w.at[1], (e_send, e_recv), 2, below),
                remote(edge_w_out.at[1], edge_w.at[0], (e_send, e_recv), 3, above),
            ]
        if c != 1:
            edges[-2].start()
            edges[-1].start()
    wall = velocity.shape[3]
    lane = lax.broadcasted_iota(jnp.int32, (1, 1, wall), 2)
    normal = velocity[1]
    upper = jnp.where(lane == wall - 1, 0.0, pltpu.roll(normal, wall - 1, 2))
    lower = jnp.where(lane == 0, 0.0, pltpu.roll(normal, 1, 2))
    divergence = upper - lower
    for copy in edges:
        copy.wait_recv()
    stream = velocity[0]
    divergence += jnp.concatenate([stream[1:], edge_u[1:2]], axis=0) - jnp.concatenate(
        [edge_u[0:1], stream[:-1]], axis=0
    )
    span = velocity[2]
    row = lax.broadcasted_iota(jnp.int32, (1, tall, 1), 1)
    after = jnp.where(row == tall - 1, edge_w[1][:, None, :], pltpu.roll(span, tall - 1, 1))
    before = jnp.where(row == 0, edge_w[0][:, None, :], pltpu.roll(span, 1, 1))
    divergence = (divergence + (after - before)) * 0.5
    for half in range(wide // 8):
        blocks = exchanged([divergence[half * 8 + i] for i in range(8)], (16, 32, 64))
        for j in range(nz):
            cut[j, :, pl.ds(half * 128, 128)] = blocks[j]

    def cut_copy(d):
        to = lax.rem(gz + d, nz)
        return pltpu.make_async_remote_copy(
            src_ref=cut.at[to],
            dst_ref=planes.at[gz],
            send_sem=c_send.at[to],
            recv_sem=c_recv.at[gz],
            device_id=(gx, to),
            device_id_type=MESH,
        )

    def cut_from(d):
        origin = lax.rem(gz + d, nz)
        return pltpu.make_async_remote_copy(
            src_ref=cut.at[origin],
            dst_ref=planes.at[origin],
            send_sem=c_send.at[origin],
            recv_sem=c_recv.at[origin],
            device_id=(gx, origin),
            device_id_type=MESH,
        )

    def start(make):
        def go(d, carry):
            make(d).start()
            return carry

        return go

    def wait_recv(make):
        def go(d, carry):
            make(d).wait_recv()
            return carry

        return go

    def wait_send(make):
        def go(d, carry):
            make(d).wait_send()
            return carry

        return go

    lax.fori_loop(1, nz, start(cut_copy), 0)
    planes[gz] = cut[gz]
    lax.fori_loop(1, nz, wait_recv(cut_from), 0)
    high, low = parts(planes[...].reshape(nz * tall, 2 * 128))
    modes[...] = dot3(table_z[0], table_z[1], high, low).reshape(modes.shape)

    def mode_copy(d):
        to = lax.rem(gx + d, nx)
        return pltpu.make_async_remote_copy(
            src_ref=modes.at[:, to],
            dst_ref=rows.at[gx],
            send_sem=m_send.at[to],
            recv_sem=m_recv.at[gx],
            device_id=(to, gz),
            device_id_type=MESH,
        )

    def mode_from(d):
        origin = lax.rem(gx + d, nx)
        return pltpu.make_async_remote_copy(
            src_ref=modes.at[:, origin],
            dst_ref=rows.at[origin],
            send_sem=m_send.at[origin],
            recv_sem=m_recv.at[origin],
            device_id=(origin, gz),
            device_id_type=MESH,
        )

    lax.fori_loop(1, nx, start(mode_copy), 0)
    rows[gx] = modes[:, gx]
    lax.fori_loop(1, nx, wait_recv(mode_from), 0)
    columns = []
    for h in range(nx // 16):
        for half in range(2):
            blocks = exchanged(
                [rows[h * 16 + b, :, :, half * 128 : half * 128 + 128] for b in range(16)],
                (1, 2, 4, 8),
            )
            columns.append(
                jnp.concatenate([block[0] for block in blocks] + [block[1] for block in blocks])
            )
    high, low = parts(jnp.concatenate(columns, axis=1))
    lines = high.shape[0] // 2
    for q in range(table_x.shape[1]):
        value = dot3(high, low, table_x[0, q], table_x[1, q])
        real = value[:lines, :128] + value[lines:, 128:]
        imag = value[lines:, :128] - value[:lines, 128:]
        out = pl.ds(q * 128, 128)
        source[0, :, :, out] = (real * scale).reshape(source.shape[1], source.shape[2], 128)
        source[1, :, :, out] = (imag * scale).reshape(source.shape[1], source.shape[2], 128)
    for c in order:
        for copy in z_copies[c] + x_copies[c]:
            copy.wait_send()
    for copy in edges:
        copy.wait_send()
    lax.fori_loop(1, nz, wait_send(cut_copy), 0)
    lax.fori_loop(1, nx, wait_send(mode_copy), 0)


def split_table(table):
    high = table.astype(jnp.bfloat16)
    return np.stack([high, (table - high.astype(np.float64)).astype(jnp.bfloat16)])


def transform_tables(length_x, length_z):
    counter = np.arange(length_z)
    angle = counter[:, None] * counter[None, :] % length_z * (2 * math.pi / length_z)
    table_z = np.concatenate([np.cos(angle), -np.sin(angle)])
    h, half, i, b = np.meshgrid(
        np.arange(length_x // 256), np.arange(2), np.arange(8), np.arange(16), indexing="ij"
    )
    place = (16 * (16 * h + b) + 8 * half + i).reshape(-1)
    mode = np.arange(length_x)
    angle = place[:, None] * mode[None, :] % length_x * (2 * math.pi / length_x)
    both = np.stack([np.cos(angle), np.sin(angle)], axis=1)
    both = both.reshape(length_x, 2, length_x // 128, 128).transpose(2, 0, 1, 3)
    return split_table(table_z), split_table(both.reshape(length_x // 128, length_x, 256))


def spectrum(force, field, tile, nx, nz):
    _, wide, tall, wall = tile
    length_x, length_z = wide * nx, tall * nz
    table_z, table_x = transform_tables(length_x, length_z)
    vector = pl.BlockSpec(memory_space=pltpu.VMEM)
    dma = pltpu.SemaphoreType.DMA
    each = wall // nz
    deep = field.shape[1]
    return pl.pallas_call(
        functools.partial(spectrum_kernel, nx, nz, 1.0 / math.sqrt(length_x * length_z)),
        out_shape=(
            jax.ShapeDtypeStruct(tile, jnp.float32),
            jax.ShapeDtypeStruct((2, each, length_z // nx, length_x), jnp.float32),
        ),
        in_specs=[vector] * 4,
        out_specs=(vector, vector),
        scratch_shapes=[
            pltpu.VMEM((2, 3, deep, SIDE, wall), jnp.float32),
            pltpu.VMEM((2, 3, HALF, tall, wall), jnp.float32),
            pltpu.VMEM((2, 3, HALF, tall, wall), jnp.float32),
            pltpu.VMEM((2, tall, wall), jnp.float32),
            pltpu.VMEM((2, wide, wall), jnp.float32),
            pltpu.VMEM((2, wide, wall), jnp.float32),
            pltpu.VMEM((nz, tall, wide * each), jnp.float32),
            pltpu.VMEM((nz, tall, wide * each), jnp.float32),
            pltpu.VMEM((2, nx, length_z // nx, wide * each), jnp.float32),
            pltpu.VMEM((nx, 2, length_z // nx, wide * each), jnp.float32),
            dma((2, 3)), dma((2, 3)), dma((2, 3)), dma((2, 3)), dma((4,)), dma((4,)),
            dma((nz,)), dma((nz,)), dma((nx,)), dma((nx,)),
        ],
        compiler_params=pltpu.CompilerParams(
            collective_id=1, has_side_effects=True, vmem_limit_bytes=28 << 20
        ),
        name="spectrum",
    )(force, field, jnp.asarray(table_z), jnp.asarray(table_x))


def on_device(
    nx, nz, flow_state, slot_ids, corners, marker_cells, marker_frac, particle_velocity,
    particle_spin,
):
    extended = predict(flow_state, nx, nz)
    force = spread_forces(
        nx,
        nz,
        extended,
        slot_ids,
        corners,
        marker_cells,
        marker_frac,
        particle_velocity,
        particle_spin,
    )
    return spectrum(force, extended, (3,) + flow_state.shape[1:], nx, nz)


def solution(mesh):
    both = ("gx", "gz")
    placed = (
        P(None, "gx", "gz", None),
        P(both),
        P(None, both),
        P(None, both, None),
        P(None, both, None),
        P(),
        P(),
    )
    return jax.shard_map(
        functools.partial(on_device, mesh.shape["gx"], mesh.shape["gz"]),
        mesh=mesh,
        in_specs=placed,
        out_specs=(P(None, "gx", "gz", None), P(None, "gz", "gx", None)),
        check_vma=False,
    )
```

```python
import functools
import math

import jax
import jax.numpy as jnp
import numpy as np
from jax import lax
from jax.experimental import pallas as pl
from jax.experimental.pallas import tpu as pltpu
from jax.sharding import PartitionSpec as P

BOX = 24
HALF = 12
BAND = 32
SIDE = 16
MESH = pl.DeviceIdType.MESH


time_step = 0.1
viscosity = 0.2
drive_force = 1.0


def remote(source, target, sems, slot, to):
    return pltpu.make_async_remote_copy(
        src_ref=source,
        dst_ref=target,
        send_sem=sems[0].at[slot],
        recv_sem=sems[1].at[slot],
        device_id=to,
        device_id_type=MESH,
    )


def around(nx, nz):
    gx, gz = lax.axis_index("gx"), lax.axis_index("gz")
    return (
        (lax.rem(gx + nx - 1, nx), gz),
        (lax.rem(gx + 1, nx), gz),
        (gx, lax.rem(gz + nz - 1, nz)),
        (gx, lax.rem(gz + 1, nz)),
    )


def front_kernel(
    nx, nz, flow_in, field, flow, edge_x, edge_z_out, edge_z,
    f_sem, e_send, e_recv, x_send, x_recv, z_send, z_recv,
):
    _, wide, tall, wall = flow.shape
    left, right, below, above = around(nx, nz)
    barrier = pltpu.get_barrier_semaphore()
    for near in (left, right, below, above):
        pl.semaphore_signal(barrier, inc=1, device_id=near, device_id_type=MESH)
    loads = [pltpu.make_async_copy(flow_in.at[c], flow.at[c], f_sem.at[c]) for c in range(4)]
    for load in loads:
        load.start()
    pl.semaphore_wait(barrier, 4)
    for load in loads:
        load.wait()
    edge_z_out[0] = flow[:, :, 0, :]
    edge_z_out[1] = flow[:, :, tall - 1, :]
    edges = [
        remote(flow.at[:, 0], edge_x.at[1], (e_send, e_recv), 0, left),
        remote(flow.at[:, wide - 1], edge_x.at[0], (e_send, e_recv), 1, right),
        remote(edge_z_out.at[0], edge_z.at[1], (e_send, e_recv), 2, below),
        remote(edge_z_out.at[1], edge_z.at[0], (e_send, e_recv), 3, above),
    ]
    for copy in edges:
        copy.start()
    spread = time_step * viscosity
    carry_by = 0.5 * time_step
    lane = lax.broadcasted_iota(jnp.int32, (tall, wall), 1)
    row = lax.broadcasted_iota(jnp.int32, (tall, wall), 0)
    first_y, last_y = lane == 0, lane == wall - 1
    first_z, last_z = row == 0, row == tall - 1

    def layer(x, back, ahead):
        here = [flow[c, x] for c in range(4)]
        moves = [carry_by * here[d] for d in range(3)]
        for c in range(3):
            f = here[c]
            total = f * (1.0 - 6.0 * spread)
            y_plus = jnp.where(last_y, 0.0, pltpu.roll(f, wall - 1, 1))
            y_minus = jnp.where(first_y, 0.0, pltpu.roll(f, 1, 1))
            z_plus = jnp.where(last_z, 0.0, pltpu.roll(f, tall - 1, 0))
            z_minus = jnp.where(first_z, 0.0, pltpu.roll(f, 1, 0))
            for plus, minus, move in (
                (ahead[c], back[c], moves[0]),
                (y_plus, y_minus, moves[1]),
                (z_plus, z_minus, moves[2]),
            ):
                total += plus * (spread - move) + minus * (spread + move)
            p = here[3]
            if c == 0:
                total += time_step * drive_force - carry_by * (ahead[3] - back[3])
            if c == 1:
                p_plus = jnp.where(last_y, p, pltpu.roll(p, wall - 1, 1))
                p_minus = jnp.where(first_y, p, pltpu.roll(p, 1, 1))
                total -= carry_by * (p_plus - p_minus)
            if c == 2:
                p_plus = jnp.where(last_z, 0.0, pltpu.roll(p, tall - 1, 0))
                p_minus = jnp.where(first_z, 0.0, pltpu.roll(p, 1, 0))
                total -= carry_by * (p_plus - p_minus)
            field[c, HALF + x, pl.ds(SIDE, tall), :] = total

    def inside(x, carry):
        layer(x, [flow[c, x - 1] for c in range(4)], [flow[c, x + 1] for c in range(4)])
        return carry

    lax.fori_loop(1, wide - 1, inside, 0)
    for copy in edges:
        copy.wait_recv()
    layer(0, [edge_x[0, c] for c in range(4)], [flow[c, 1] for c in range(4)])
    layer(
        wide - 1, [flow[c, wide - 2] for c in range(4)], [edge_x[1, c] for c in range(4)]
    )
    own = pl.ds(HALF, wide)
    x_copies, z_copies = [], []
    for c in range(3):
        for side, z, sign in ((0, 0, 1.0), (1, tall - 1, -1.0)):
            move = carry_by * edge_z_out[side, 2]
            add = edge_z[side, c] * (spread + sign * move)
            if c == 2:
                add += sign * carry_by * edge_z[side, 3]
            field[c, own, SIDE + z, :] += add
        inner = pl.ds(SIDE, tall)
        back = remote(
            field.at[c, pl.ds(HALF, HALF), inner],
            field.at[c, pl.ds(HALF + wide, HALF), inner],
            (x_send, x_recv), (0, c), left,
        )
        ahead = remote(
            field.at[c, pl.ds(wide, HALF), inner],
            field.at[c, pl.ds(0, HALF), inner],
            (x_send, x_recv), (1, c), right,
        )
        back.start()
        ahead.start()
        x_copies.append((back, ahead))

    def slabs(c, piece, columns):
        down = remote(
            field.at[c, columns, pl.ds(SIDE, SIDE)],
            field.at[c, columns, pl.ds(SIDE + tall, SIDE)],
            (z_send, z_recv), (0, c, piece), below,
        )
        up = remote(
            field.at[c, columns, pl.ds(tall, SIDE)],
            field.at[c, columns, pl.ds(0, SIDE)],
            (z_send, z_recv), (1, c, piece), above,
        )
        down.start()
        up.start()
        z_copies.extend((down, up))

    for c in range(3):
        slabs(c, 0, own)
    for c in range(3):
        x_copies[c][0].wait_recv()
        slabs(c, 1, pl.ds(HALF + wide, HALF))
        x_copies[c][1].wait_recv()
        slabs(c, 2, pl.ds(0, HALF))
    for copy in z_copies:
        copy.wait_recv()
    for copy in edges + z_copies + [copy for pair in x_copies for copy in pair]:
        copy.wait_send()


def predict(flow, nx, nz):
    _, wide, tall, wall = flow.shape
    dma = pltpu.SemaphoreType.DMA
    return pl.pallas_call(
        functools.partial(front_kernel, nx, nz),
        out_shape=jax.ShapeDtypeStruct(
            (3, wide + 2 * HALF, tall + 2 * SIDE, wall), jnp.float32
        ),
        in_specs=[pl.BlockSpec(memory_space=pltpu.HBM)],
        out_specs=pl.BlockSpec(memory_space=pltpu.VMEM),
        scratch_shapes=[
            pltpu.VMEM(flow.shape, jnp.float32),
            pltpu.VMEM((2, 4, tall, wall), jnp.float32),
            pltpu.VMEM((2, 4, wide, wall), jnp.float32),
            pltpu.VMEM((2, 4, wide, wall), jnp.float32),
            dma((4,)), dma((4,)), dma((4,)), dma((2, 3)), dma((2, 3)), dma((2, 3, 3)),
            dma((2, 3, 3)),
        ],
        compiler_params=pltpu.CompilerParams(
            collective_id=0, has_side_effects=True, vmem_limit_bytes=12 << 20
        ),
        name="front",
    )(pltpu.with_memory_space_constraint(flow, pltpu.HBM))


def parts(value):
    high = value.astype(jnp.bfloat16)
    return high, (value - high.astype(jnp.float32)).astype(jnp.bfloat16)


def tap_weights(length, first, taps):
    offset = lax.broadcasted_iota(jnp.int32, (length, first.shape[-1]), 0) - first
    weight = jnp.where(offset == 3, taps[3], 0.0)
    for t in (2, 1, 0):
        weight = jnp.where(offset == t, taps[t], weight)
    return weight


def dot(a, b, across):
    return lax.dot_general(
        a, b, (((1,), (across,)), ((), ())), preferred_element_type=jnp.float32
    )


def pair(a, b, across):
    rows = a[0].shape[0]
    both = dot(jnp.concatenate(a), b[0], across)
    return both[:rows] + both[rows:] + dot(a[0], b[1], across)


def marker_kernel(
    nx, nz, ids, corners, moving, turning, cells, fracs, field, force, tap, cross
):
    force[...] = jnp.zeros_like(force)
    half_pi = 0.5 * math.pi
    angle = fracs[...] * half_pi
    cosine, sine = jnp.cos(angle), jnp.sin(angle)
    tap[0] = 0.25 * (1.0 - sine)
    tap[1] = 0.25 * (1.0 + cosine)
    tap[2] = 0.25 * (1.0 + sine)
    tap[3] = 0.25 * (1.0 - cosine)
    markers = fracs.shape[2]
    wall = field.shape[3]
    wide, tall = field.shape[1] - 2 * HALF, field.shape[2] - 2 * SIDE
    first_x = lax.axis_index("gx") * wide - HALF
    first_z = lax.axis_index("gz") * tall - SIDE
    many = wall // BAND
    lane = lax.broadcasted_iota(jnp.int32, (1, 1, wall), 2)

    def one_slot(s, carry):
        @pl.when(ids[s] >= 0)
        def _():
            n = ids[s]
            x0 = lax.rem(corners[0, s] - first_x + wide * nx, wide * nx)
            y0 = corners[1, s]
            z0 = lax.rem(corners[2, s] - first_z + tall * nz, tall * nz)
            zb = pl.multiple_of((z0 // 8) * 8, 8)
            cell = cells[:, pl.ds(s, 1), :].reshape(3, markers)
            frac = fracs[:, pl.ds(s, 1), :].reshape(3, markers)
            taps = [tap[t, :, pl.ds(s, 1), :].reshape(3, markers) for t in range(4)]

            def along(d):
                return [w[d : d + 1] for w in taps]

            weight_x = tap_weights(BOX, cell[0:1] - 1, along(0))
            weight_y = tap_weights(BAND, cell[1:2] - 1, along(1))
            weight_z = tap_weights(BAND, cell[2:3] - 1 + (z0 - zb), along(2))
            for i in range(BOX):
                high, low = parts(weight_x[i : i + 1] * weight_y)
                cross[0, pl.ds(i * BAND, BAND), :] = high
                cross[1, pl.ds(i * BAND, BAND), :] = low
            columns = []
            for q in range(BOX // many):
                packed = None
                for r in range(many):
                    piece = field[:, x0 + (q * many + r), pl.ds(zb, BAND), :]
                    piece = pltpu.roll(piece, lax.rem(wall + r * BAND - y0, wall), 2)
                    packed = piece if r == 0 else jnp.where(lane < r * BAND, packed, piece)
                columns.append(packed.reshape(3 * BAND, wall))
            window = parts(jnp.concatenate(columns, axis=1))
            value = pair(window, (cross[0], cross[1]), 0).reshape(3, BAND, markers)
            sampled = jnp.sum(value * weight_z[None], axis=1)
            lever = cell.astype(jnp.float32) + frac - float(HALF)
            spin = [turning[c, n] for c in range(3)]
            loads = []
            for c in range(3):
                a, b = (c + 1) % 3, (c + 2) % 3
                target = moving[c, n] + (spin[a] * lever[b : b + 1] - spin[b] * lever[a : a + 1])
                loads.append((target - sampled[c : c + 1]) * weight_z)
            load = parts(jnp.concatenate(loads))
            value = pair(load, (cross[0], cross[1]), 1).reshape(3, BAND, BOX * BAND)
            inside = (lane >= y0) & (lane < y0 + BOX)
            for i in range(BOX):
                q, r = i // many, i % many
                piece = value[:, :, q * wall : (q + 1) * wall]
                piece = pltpu.roll(piece, lax.rem(wall + y0 - r * BAND, wall), 2)
                force[:, x0 + i, pl.ds(zb, BAND), :] += jnp.where(inside, piece, 0.0)

        return carry

    lax.fori_loop(0, ids.shape[0], one_slot, 0)


def spread_forces(nx, nz, extended, slot_ids, corners, cells, fracs, moving, turning):
    _, slots, markers = cells.shape
    scalar = pl.BlockSpec(memory_space=pltpu.SMEM)
    vector = pl.BlockSpec(memory_space=pltpu.VMEM)
    return pl.pallas_call(
        functools.partial(marker_kernel, nx, nz),
        out_shape=jax.ShapeDtypeStruct(extended.shape, jnp.float32),
        in_specs=[scalar] * 4 + [vector] * 3,
        out_specs=vector,
        scratch_shapes=[
            pltpu.VMEM((4, 3, slots, markers), jnp.float32),
            pltpu.VMEM((2, BOX * BAND, markers), jnp.bfloat16),
        ],
        compiler_params=pltpu.CompilerParams(vmem_limit_bytes=24 << 20),
        name="markers",
    )(slot_ids, corners, moving, turning, cells, fracs, extended)


def exchanged(rows, lane_bits):
    lane = lax.broadcasted_iota(jnp.int32, rows[0].shape, rows[0].ndim - 1)
    axis = rows[0].ndim - 1
    for bit, shift in enumerate(lane_bits):
        low = (lane & shift) == 0
        step = 1 << bit
        out = list(rows)
        for m in range(len(rows)):
            if m & step == 0:
                a, b = rows[m], rows[m + step]
                out[m] = jnp.where(low, a, pltpu.roll(b, shift, axis))
                out[m + step] = jnp.where(low, pltpu.roll(a, 128 - shift, axis), b)
        rows = out
    return rows


def spectrum_kernel(
    nx, nz, force, field, table_z, velocity, rows,
    z_got, x_out, x_got, u_out, u_got, row_out, row_got, row_sum, rim_out, rim_got, edge_u,
    edge_w, cut, planes, modes,
    z_send, z_recv, x_send, x_recv, e_send, e_recv, c_send, c_recv, m_send, m_recv,
):
    gx, gz = lax.axis_index("gx"), lax.axis_index("gz")
    left, right, below, above = around(nx, nz)
    barrier = pltpu.get_barrier_semaphore()

    def greet_z(d, carry):
        pl.semaphore_signal(
            barrier, inc=1, device_id=(gx, lax.rem(gz + d, nz)), device_id_type=MESH
        )
        return carry

    def greet_x(d, carry):
        pl.semaphore_signal(
            barrier, inc=1, device_id=(lax.rem(gx + d, nx), gz), device_id_type=MESH
        )
        return carry

    lax.fori_loop(1, nx, greet_x, 0)
    lax.fori_loop(1, nz, greet_z, 0)
    wide, tall = velocity.shape[1], velocity.shape[2]
    row_out[0] = force[2, :, SIDE, :]
    row_out[1] = force[2, :, SIDE + tall - 1, :]
    pl.semaphore_wait(barrier, nx + nz - 2)

    order = (0, 2, 1)
    own = pl.ds(HALF, wide)
    pieces = (pl.ds(0, HALF), pl.ds(HALF + wide, HALF), own)

    def fold_z(c, piece):
        columns = pieces[piece]
        down = remote(
            force.at[c, columns, pl.ds(0, SIDE), :],
            z_got.at[1, c, columns],
            (z_send, z_recv), (1, c, piece), below,
        )
        up = remote(
            force.at[c, columns, pl.ds(SIDE + tall, SIDE), :],
            z_got.at[0, c, columns],
            (z_send, z_recv), (0, c, piece), above,
        )
        down.start()
        up.start()
        return [down, up]

    rims, inner = {}, {}
    for c in order:
        rims[c] = fold_z(c, 0) + fold_z(c, 1)
        if c == 2:
            lines = [
                remote(row_out.at[0], row_got.at[1], (e_send, e_recv), 0, below),
                remote(row_out.at[1], row_got.at[0], (e_send, e_recv), 1, above),
            ]
            for copy in lines:
                copy.start()
    for c in order:
        inner[c] = fold_z(c, 2)
    x_copies = {}
    for c in order:
        for copy in rims[c]:
            copy.wait_recv()
        for part in range(2):
            inside = pl.ds(part * SIDE, SIDE)
            outside = pl.ds(SIDE + part * SIDE, SIDE)
            for side in range(2):
                x_out[side, c, :, inside, :] = (
                    force[c, pieces[side], outside, :] + z_got[part, c, pieces[side]]
                )
        back = remote(x_out.at[0, c], x_got.at[1, c], (x_send, x_recv), (1, c), left)
        ahead = remote(x_out.at[1, c], x_got.at[0, c], (x_send, x_recv), (0, c), right)
        back.start()
        ahead.start()
        x_copies[c] = [back, ahead]
        if c == 2:
            for copy in lines:
                copy.wait_recv()
            row_sum[0] = force[2, :, SIDE - 1, :] + row_got[0]
            row_sum[1] = force[2, :, SIDE + tall, :] + row_got[1]
            rim_out[0] = row_sum[:, pl.ds(0, HALF), :]
            rim_out[1] = row_sum[:, pl.ds(HALF + wide, HALF), :]
            ends = [
                remote(rim_out.at[0], rim_got.at[1], (e_send, e_recv), 2, left),
                remote(rim_out.at[1], rim_got.at[0], (e_send, e_recv), 3, right),
            ]
            for copy in ends:
                copy.start()
        if c == 0:
            for copy in inner[0]:
                copy.wait_recv()
            for part in range(2):
                inside = pl.ds(part * SIDE, SIDE)
                outside = pl.ds(SIDE + part * SIDE, SIDE)
                u_out[0, inside, :] = force[0, HALF, outside, :] + z_got[part, 0, HALF]
                u_out[1, inside, :] = (
                    force[0, HALF + wide - 1, outside, :] + z_got[part, 0, HALF + wide - 1]
                )
            layers = [
                remote(u_out.at[0], u_got.at[1], (e_send, e_recv), 4, left),
                remote(u_out.at[1], u_got.at[0], (e_send, e_recv), 5, right),
            ]
            for copy in layers:
                copy.start()
    for c in order:
        if c != 0:
            for copy in inner[c]:
                copy.wait_recv()
        for part in range(2):
            inside = pl.ds(part * SIDE, SIDE)
            outside = pl.ds(SIDE + part * SIDE, SIDE)
            velocity[c, :, inside, :] = (
                field[c, own, outside, :] + force[c, own, outside, :] + z_got[part, c, own]
            )
    for c in order:
        for copy in x_copies[c]:
            copy.wait_recv()
        velocity[c, pl.ds(0, HALF)] += x_got[0, c]
        velocity[c, pl.ds(wide - HALF, HALF)] += x_got[1, c]
        if c == 0:
            for copy in layers:
                copy.wait_recv()
            body = pl.ds(SIDE, tall)
            edge_u[0] = field[0, HALF - 1, body, :] + x_out[0, 0, HALF - 1] + u_got[0]
            edge_u[1] = field[0, HALF + wide, body, :] + x_out[1, 0, 0] + u_got[1]
        if c == 2:
            for copy in ends:
                copy.wait_recv()
            edge_w[0] = field[2, own, SIDE - 1, :] + row_sum[0, own, :]
            edge_w[1] = field[2, own, SIDE + tall, :] + row_sum[1, own, :]
            edge_w[:, pl.ds(0, HALF), :] += rim_got[0]
            edge_w[:, pl.ds(wide - HALF, HALF), :] += rim_got[1]
    edges = lines + ends + layers
    wall = velocity.shape[3]
    lane = lax.broadcasted_iota(jnp.int32, (1, 1, wall), 2)
    normal = velocity[1]
    upper = jnp.where(lane == wall - 1, 0.0, pltpu.roll(normal, wall - 1, 2))
    lower = jnp.where(lane == 0, 0.0, pltpu.roll(normal, 1, 2))
    divergence = upper - lower
    stream = velocity[0]
    divergence += jnp.concatenate([stream[1:], edge_u[1:2]], axis=0) - jnp.concatenate(
        [edge_u[0:1], stream[:-1]], axis=0
    )
    span = velocity[2]
    row = lax.broadcasted_iota(jnp.int32, (1, tall, 1), 1)
    after = jnp.where(row == tall - 1, edge_w[1][:, None, :], pltpu.roll(span, tall - 1, 1))
    before = jnp.where(row == 0, edge_w[0][:, None, :], pltpu.roll(span, 1, 1))
    divergence = (divergence + (after - before)) * 0.5
    for half in range(wide // 8):
        blocks = exchanged([divergence[half * 8 + i] for i in range(8)], (16, 32, 64))
        for j in range(nz):
            cut[j, :, pl.ds(half * 128, 128)] = blocks[j]

    def cut_copy(d):
        to = lax.rem(gz + d, nz)
        return pltpu.make_async_remote_copy(
            src_ref=cut.at[to],
            dst_ref=planes.at[gz],
            send_sem=c_send.at[to],
            recv_sem=c_recv.at[gz],
            device_id=(gx, to),
            device_id_type=MESH,
        )

    def cut_from(d):
        origin = lax.rem(gz + d, nz)
        return pltpu.make_async_remote_copy(
            src_ref=cut.at[origin],
            dst_ref=planes.at[origin],
            send_sem=c_send.at[origin],
            recv_sem=c_recv.at[origin],
            device_id=(gx, origin),
            device_id_type=MESH,
        )

    def start(make):
        def go(d, carry):
            make(d).start()
            return carry

        return go

    def wait_recv(make):
        def go(d, carry):
            make(d).wait_recv()
            return carry

        return go

    def wait_send(make):
        def go(d, carry):
            make(d).wait_send()
            return carry

        return go

    lax.fori_loop(1, nz, start(cut_copy), 0)
    planes[gz] = cut[gz]
    lax.fori_loop(1, nz, wait_recv(cut_from), 0)
    high, low = parts(planes[...].reshape(nz * tall, 2 * 128))
    modes[...] = pair((table_z[0], table_z[1]), (high, low), 0).reshape(modes.shape)

    deep = nx // 8
    deep_at, along_at = lax.div(gx, 8), lax.rem(gx, 8)

    def partner(t):
        k, j = lax.div(t, deep), lax.rem(t, deep)
        odd = lax.rem(k, 2)
        step = 4 - odd + lax.div(k, 2) * (1 - 2 * odd)
        return lax.rem(deep_at + j + 1, deep) * 8 + lax.rem(along_at + step, 8)

    def mode_copy(t):
        to = partner(t)
        return pltpu.make_async_remote_copy(
            src_ref=modes.at[:, to],
            dst_ref=rows.at[gx],
            send_sem=m_send.at[to],
            recv_sem=m_recv.at[gx],
            device_id=(to, gz),
            device_id_type=MESH,
        )

    def mode_from(t):
        origin = partner(t)
        return pltpu.make_async_remote_copy(
            src_ref=modes.at[:, origin],
            dst_ref=rows.at[origin],
            send_sem=m_send.at[origin],
            recv_sem=m_recv.at[origin],
            device_id=(origin, gz),
            device_id_type=MESH,
        )

    lax.fori_loop(0, nx - 1, start(mode_copy), 0)
    rows[gx] = modes[:, gx]
    lax.fori_loop(0, nx - 1, wait_recv(mode_from), 0)
    for c in order:
        for copy in rims[c] + inner[c] + x_copies[c]:
            copy.wait_send()
    for copy in edges:
        copy.wait_send()
    lax.fori_loop(1, nz, wait_send(cut_copy), 0)
    lax.fori_loop(0, nx - 1, wait_send(mode_copy), 0)


def finish_kernel(scale, velocity_in, rows, table_x, velocity, source, held, sems):
    through = pltpu.make_async_copy(velocity_in, velocity, sems.at[0])
    through.start()
    columns = []
    for h in range(rows.shape[0] // 16):
        for half in range(2):
            blocks = exchanged(
                [rows[h * 16 + b, :, :, half * 128 : half * 128 + 128] for b in range(16)],
                (1, 2, 4, 8),
            )
            columns.append(
                jnp.concatenate([block[0] for block in blocks] + [block[1] for block in blocks])
            )
    high, low = parts(jnp.concatenate(columns, axis=1))
    lines = high.shape[0] // 2
    copies = [through]
    for q in range(table_x.shape[1]):
        value = pair((high, low), (table_x[0, q], table_x[1, q]), 0)
        real = value[:lines, :128] + value[lines:, 128:]
        imag = value[lines:, :128] - value[:lines, 128:]
        out = pl.ds(q * 128, 128)
        held[0, :, :, out] = (real * scale).reshape(held.shape[1], held.shape[2], 128)
        held[1, :, :, out] = (imag * scale).reshape(held.shape[1], held.shape[2], 128)
        copy = pltpu.make_async_copy(
            held.at[:, :, :, out], source.at[:, :, :, out], sems.at[1 + q]
        )
        copy.start()
        copies.append(copy)
    for copy in copies:
        copy.wait()


def split_table(table):
    high = table.astype(jnp.bfloat16)
    return np.stack([high, (table - high.astype(np.float64)).astype(jnp.bfloat16)])


def transform_tables(length_x, length_z):
    counter = np.arange(length_z)
    angle = counter[:, None] * counter[None, :] % length_z * (2 * math.pi / length_z)
    table_z = np.concatenate([np.cos(angle), -np.sin(angle)])
    h, half, i, b = np.meshgrid(
        np.arange(length_x // 256), np.arange(2), np.arange(8), np.arange(16), indexing="ij"
    )
    place = (16 * (16 * h + b) + 8 * half + i).reshape(-1)
    mode = np.arange(length_x)
    angle = place[:, None] * mode[None, :] % length_x * (2 * math.pi / length_x)
    both = np.stack([np.cos(angle), np.sin(angle)], axis=1)
    both = both.reshape(length_x, 2, length_x // 128, 128).transpose(2, 0, 1, 3)
    return split_table(table_z), split_table(both.reshape(length_x // 128, length_x, 256))


def spectrum(force, field, tile, nx, nz):
    _, wide, tall, wall = tile
    length_x, length_z = wide * nx, tall * nz
    table_z, table_x = transform_tables(length_x, length_z)
    vector = pl.BlockSpec(memory_space=pltpu.VMEM)
    dma = pltpu.SemaphoreType.DMA
    each = wall // nz
    deep = field.shape[1]
    modes = length_z // nx
    velocity, rows = pl.pallas_call(
        functools.partial(spectrum_kernel, nx, nz),
        out_shape=(
            jax.ShapeDtypeStruct(tile, jnp.float32),
            jax.ShapeDtypeStruct((nx, 2, modes, wide * each), jnp.float32),
        ),
        in_specs=[vector] * 3,
        out_specs=(vector, vector),
        scratch_shapes=[
            pltpu.VMEM((2, 3, deep, SIDE, wall), jnp.float32),
            pltpu.VMEM((2, 3, HALF, tall, wall), jnp.float32),
            pltpu.VMEM((2, 3, HALF, tall, wall), jnp.float32),
            pltpu.VMEM((2, tall, wall), jnp.float32),
            pltpu.VMEM((2, tall, wall), jnp.float32),
            pltpu.VMEM((2, deep, wall), jnp.float32),
            pltpu.VMEM((2, deep, wall), jnp.float32),
            pltpu.VMEM((2, deep, wall), jnp.float32),
            pltpu.VMEM((2, 2, HALF, wall), jnp.float32),
            pltpu.VMEM((2, 2, HALF, wall), jnp.float32),
            pltpu.VMEM((2, tall, wall), jnp.float32),
            pltpu.VMEM((2, wide, wall), jnp.float32),
            pltpu.VMEM((nz, tall, wide * each), jnp.float32),
            pltpu.VMEM((nz, tall, wide * each), jnp.float32),
            pltpu.VMEM((2, nx, modes, wide * each), jnp.float32),
            dma((2, 3, 3)), dma((2, 3, 3)), dma((2, 3)), dma((2, 3)), dma((6,)), dma((6,)),
            dma((nz,)), dma((nz,)), dma((nx,)), dma((nx,)),
        ],
        compiler_params=pltpu.CompilerParams(
            collective_id=1, has_side_effects=True, vmem_limit_bytes=28 << 20
        ),
        name="spectrum",
    )(force, field, jnp.asarray(table_z))
    shape = (2, each, modes, length_x)
    return pl.pallas_call(
        functools.partial(finish_kernel, 1.0 / math.sqrt(length_x * length_z)),
        out_shape=(
            jax.ShapeDtypeStruct(tile, jnp.float32),
            jax.ShapeDtypeStruct(shape, jnp.float32),
        ),
        in_specs=[vector] * 3,
        out_specs=(pl.BlockSpec(memory_space=pltpu.HBM), pl.BlockSpec(memory_space=pltpu.HBM)),
        scratch_shapes=[
            pltpu.VMEM(shape, jnp.float32),
            dma((1 + length_x // 128,)),
        ],
        compiler_params=pltpu.CompilerParams(vmem_limit_bytes=16 << 20),
        name="finish",
    )(velocity, rows, jnp.asarray(table_x))


def on_device(
    nx, nz, flow_state, slot_ids, corners, marker_cells, marker_frac, particle_velocity,
    particle_spin,
):
    extended = predict(flow_state, nx, nz)
    force = spread_forces(
        nx,
        nz,
        extended,
        slot_ids,
        corners,
        marker_cells,
        marker_frac,
        particle_velocity,
        particle_spin,
    )
    return spectrum(force, extended, (3,) + flow_state.shape[1:], nx, nz)


def solution(mesh):
    both = ("gx", "gz")
    placed = (
        P(None, "gx", "gz", None),
        P(both),
        P(None, both),
        P(None, both, None),
        P(None, both, None),
        P(),
        P(),
    )
    return jax.shard_map(
        functools.partial(on_device, mesh.shape["gx"], mesh.shape["gz"]),
        mesh=mesh,
        in_specs=placed,
        out_specs=(P(None, "gx", "gz", None), P(None, "gz", "gx", None)),
        check_vma=False,
    )
```

```python
import functools
import math

import jax
import jax.numpy as jnp
import numpy as np
from jax import lax
from jax.experimental import pallas as pl
from jax.experimental.pallas import tpu as pltpu
from jax.sharding import PartitionSpec as P

BOX = 24
HALF = 12
BAND = 32
SIDE = 16
MESH = pl.DeviceIdType.MESH


time_step = 0.1
viscosity = 0.2
drive_force = 1.0


def remote(source, target, sems, slot, to):
    return pltpu.make_async_remote_copy(
        src_ref=source,
        dst_ref=target,
        send_sem=sems[0].at[slot],
        recv_sem=sems[1].at[slot],
        device_id=to,
        device_id_type=MESH,
    )


def around(nx, nz):
    gx, gz = lax.axis_index("gx"), lax.axis_index("gz")
    return (
        (lax.rem(gx + nx - 1, nx), gz),
        (lax.rem(gx + 1, nx), gz),
        (gx, lax.rem(gz + nz - 1, nz)),
        (gx, lax.rem(gz + 1, nz)),
    )


def parts(value):
    high = value.astype(jnp.bfloat16)
    return high, (value - high.astype(jnp.float32)).astype(jnp.bfloat16)


def tap_weights(length, first, taps):
    offset = lax.broadcasted_iota(jnp.int32, (length, first.shape[-1]), 0) - first
    weight = jnp.where(offset == 3, taps[3], 0.0)
    for t in (2, 1, 0):
        weight = jnp.where(offset == t, taps[t], weight)
    return weight


def fill_taps(fracs, tap):
    angle = fracs[...] * (0.5 * math.pi)
    cosine, sine = jnp.cos(angle), jnp.sin(angle)
    tap[0] = 0.25 * (1.0 - sine)
    tap[1] = 0.25 * (1.0 + cosine)
    tap[2] = 0.25 * (1.0 + sine)
    tap[3] = 0.25 * (1.0 - cosine)


def cross_weights(cells, fracs, tap, cross):
    fill_taps(fracs, tap)
    markers = fracs.shape[2]

    def one_slot(s, carry):
        cell = cells[:, pl.ds(s, 1), :].reshape(3, markers)
        taps = [tap[t, :, pl.ds(s, 1), :].reshape(3, markers) for t in range(4)]
        weight_x = tap_weights(BOX, cell[0:1] - 1, [w[0:1] for w in taps])
        weight_y = tap_weights(BAND, cell[1:2] - 1, [w[1:2] for w in taps])
        for i in range(BOX):
            high, low = parts(weight_x[i : i + 1] * weight_y)
            cross[s, 0, pl.ds(i * BAND, BAND), :] = high
            cross[s, 1, pl.ds(i * BAND, BAND), :] = low
        return carry

    lax.fori_loop(0, cells.shape[1], one_slot, 0)


def front_kernel(
    nx, nz, flow_in, cells, fracs, field, cross, tap, flow, edge_x, edge_z_out, edge_z,
    f_sem, e_send, e_recv, x_send, x_recv, z_send, z_recv, r_send, r_recv,
):
    _, wide, tall, wall = flow.shape
    left, right, below, above = around(nx, nz)
    barrier = pltpu.get_barrier_semaphore()
    for near in (left, right, below, above):
        pl.semaphore_signal(barrier, inc=1, device_id=near, device_id_type=MESH)
    loads = [pltpu.make_async_copy(flow_in.at[c], flow.at[c], f_sem.at[c]) for c in range(4)]
    for load in loads:
        load.start()
    pl.semaphore_wait(barrier, 4)
    for load in loads:
        load.wait()
    edge_z_out[0] = flow[:, :, 0, :]
    edge_z_out[1] = flow[:, :, tall - 1, :]
    edges = [
        remote(flow.at[:, 0], edge_x.at[1], (e_send, e_recv), 0, left),
        remote(flow.at[:, wide - 1], edge_x.at[0], (e_send, e_recv), 1, right),
        remote(edge_z_out.at[0], edge_z.at[1], (e_send, e_recv), 2, below),
        remote(edge_z_out.at[1], edge_z.at[0], (e_send, e_recv), 3, above),
    ]
    for copy in edges:
        copy.start()
    spread = time_step * viscosity
    carry_by = 0.5 * time_step
    lane = lax.broadcasted_iota(jnp.int32, (tall, wall), 1)
    row = lax.broadcasted_iota(jnp.int32, (tall, wall), 0)
    first_y, last_y = lane == 0, lane == wall - 1
    first_z, last_z = row == 0, row == tall - 1

    def layer(x, back, ahead):
        here = [flow[c, x] for c in range(4)]
        moves = [carry_by * here[d] for d in range(3)]
        for c in range(3):
            f = here[c]
            total = f * (1.0 - 6.0 * spread)
            y_plus = jnp.where(last_y, 0.0, pltpu.roll(f, wall - 1, 1))
            y_minus = jnp.where(first_y, 0.0, pltpu.roll(f, 1, 1))
            z_plus = jnp.where(last_z, 0.0, pltpu.roll(f, tall - 1, 0))
            z_minus = jnp.where(first_z, 0.0, pltpu.roll(f, 1, 0))
            for plus, minus, move in (
                (ahead[c], back[c], moves[0]),
                (y_plus, y_minus, moves[1]),
                (z_plus, z_minus, moves[2]),
            ):
                total += plus * (spread - move) + minus * (spread + move)
            p = here[3]
            if c == 0:
                total += time_step * drive_force - carry_by * (ahead[3] - back[3])
            if c == 1:
                p_plus = jnp.where(last_y, p, pltpu.roll(p, wall - 1, 1))
                p_minus = jnp.where(first_y, p, pltpu.roll(p, 1, 1))
                total -= carry_by * (p_plus - p_minus)
            if c == 2:
                p_plus = jnp.where(last_z, 0.0, pltpu.roll(p, tall - 1, 0))
                p_minus = jnp.where(first_z, 0.0, pltpu.roll(p, 1, 0))
                total -= carry_by * (p_plus - p_minus)
            field[c, HALF + x, pl.ds(SIDE, tall), :] = total

    def inside(x, carry):
        layer(x, [flow[c, x - 1] for c in range(4)], [flow[c, x + 1] for c in range(4)])
        return carry

    lax.fori_loop(1, wide - 1, inside, 0)
    rim = HALF - 1
    half = SIDE // 2
    spans = (
        {0: (1, rim), 1: (0, 1), 2: (0, HALF), 3: (0, HALF)},
        {0: (0, rim), 1: (rim, 1), 2: (0, HALF), 3: (0, HALF)},
    )
    lines = {0: (half, SIDE), 1: (half, SIDE), 2: (0, half), 3: (tall - half, half)}
    x_copies, z_copies = {}, []

    def send(c, piece):
        for side in range(2):
            first, count = spans[side][piece]
            at, height = lines[piece]
            source, target = ((HALF, HALF + wide), (wide, 0))[side]
            rows = pl.ds(SIDE + at, height)
            copy = remote(
                field.at[c, pl.ds(source + first, count), rows],
                field.at[c, pl.ds(target + first, count), rows],
                (x_send, x_recv), (side, c, piece), (left, right)[side],
            )
            copy.start()
            x_copies[c, piece, side] = copy

    def forward(c, piece, side):
        first, count = spans[side][piece]
        columns = pl.ds((HALF + wide, 0)[side] + first, count)
        at, height = lines[piece]
        slot = min(piece, 2)
        if piece != 3:
            copy = remote(
                field.at[c, columns, pl.ds(SIDE + at, half)],
                field.at[c, columns, pl.ds(SIDE + tall + at, half)],
                (r_send, r_recv), (0, c, side, slot), below,
            )
            copy.start()
            z_copies.append(copy)
        if piece != 2:
            start = at + height - half
            copy = remote(
                field.at[c, columns, pl.ds(SIDE + start, half)],
                field.at[c, columns, pl.ds(SIDE + start - tall, half)],
                (r_send, r_recv), (1, c, side, slot), above,
            )
            copy.start()
            z_copies.append(copy)

    for c in range(3):
        send(c, 0)
    for copy in edges:
        copy.wait_recv()
    layer(0, [edge_x[0, c] for c in range(4)], [flow[c, 1] for c in range(4)])
    layer(
        wide - 1, [flow[c, wide - 2] for c in range(4)], [edge_x[1, c] for c in range(4)]
    )
    own = pl.ds(HALF, wide)
    for c in range(3):
        for side, z, sign in ((0, 0, 1.0), (1, tall - 1, -1.0)):
            move = carry_by * edge_z_out[side, 2]
            add = edge_z[side, c] * (spread + sign * move)
            if c == 2:
                add += sign * carry_by * edge_z[side, 3]
            field[c, own, SIDE + z, :] += add
        for piece in (2, 3, 1):
            send(c, piece)
    for c in range(3):
        down = remote(
            field.at[c, own, pl.ds(SIDE, SIDE)],
            field.at[c, own, pl.ds(SIDE + tall, SIDE)],
            (z_send, z_recv), (0, c), below,
        )
        up = remote(
            field.at[c, own, pl.ds(tall, SIDE)],
            field.at[c, own, pl.ds(0, SIDE)],
            (z_send, z_recv), (1, c), above,
        )
        down.start()
        up.start()
        z_copies.extend((down, up))
    cross_weights(cells, fracs, tap, cross)
    for c, piece in [(c, 0) for c in range(3)] + [(c, p) for c in range(3) for p in (2, 3, 1)]:
        for side in range(2):
            x_copies[c, piece, side].wait_recv()
            forward(c, piece, side)
    for copy in z_copies:
        copy.wait_recv()
    for copy in edges + z_copies + list(x_copies.values()):
        copy.wait_send()


def predict(flow, cells, fracs, nx, nz):
    _, wide, tall, wall = flow.shape
    _, slots, markers = cells.shape
    vector = pl.BlockSpec(memory_space=pltpu.VMEM)
    dma = pltpu.SemaphoreType.DMA
    return pl.pallas_call(
        functools.partial(front_kernel, nx, nz),
        out_shape=(
            jax.ShapeDtypeStruct(
                (3, wide + 2 * HALF, tall + 2 * SIDE, wall), jnp.float32
            ),
            jax.ShapeDtypeStruct((slots, 2, BOX * BAND, markers), jnp.bfloat16),
        ),
        in_specs=[pl.BlockSpec(memory_space=pltpu.HBM), vector, vector],
        out_specs=(vector, vector),
        scratch_shapes=[
            pltpu.VMEM((4,) + cells.shape, jnp.float32),
            pltpu.VMEM(flow.shape, jnp.float32),
            pltpu.VMEM((2, 4, tall, wall), jnp.float32),
            pltpu.VMEM((2, 4, wide, wall), jnp.float32),
            pltpu.VMEM((2, 4, wide, wall), jnp.float32),
            dma((4,)), dma((4,)), dma((4,)), dma((2, 3, 4)), dma((2, 3, 4)), dma((2, 3)),
            dma((2, 3)), dma((2, 3, 2, 3)), dma((2, 3, 2, 3)),
        ],
        compiler_params=pltpu.CompilerParams(
            collective_id=0, has_side_effects=True, vmem_limit_bytes=12 << 20
        ),
        name="front",
    )(pltpu.with_memory_space_constraint(flow, pltpu.HBM), cells, fracs)


def dot(a, b, across):
    return lax.dot_general(
        a, b, (((1,), (across,)), ((), ())), preferred_element_type=jnp.float32
    )


def pair(a, b, across):
    rows = a[0].shape[0]
    both = dot(jnp.concatenate(a), b[0], across)
    return both[:rows] + both[rows:] + dot(a[0], b[1], across)


def marker_kernel(
    nx, nz, ids, corners, moving, turning, cells, fracs, field, cross, force, tap
):
    force[...] = jnp.zeros_like(force)
    fill_taps(fracs, tap)
    markers = fracs.shape[2]
    wall = field.shape[3]
    wide, tall = field.shape[1] - 2 * HALF, field.shape[2] - 2 * SIDE
    first_x = lax.axis_index("gx") * wide - HALF
    first_z = lax.axis_index("gz") * tall - SIDE
    many = wall // BAND
    lane = lax.broadcasted_iota(jnp.int32, (1, 1, wall), 2)

    def one_slot(s, carry):
        @pl.when(ids[s] >= 0)
        def _():
            n = ids[s]
            x0 = lax.rem(corners[0, s] - first_x + wide * nx, wide * nx)
            y0 = corners[1, s]
            z0 = lax.rem(corners[2, s] - first_z + tall * nz, tall * nz)
            zb = pl.multiple_of((z0 // 8) * 8, 8)
            cell = cells[:, pl.ds(s, 1), :].reshape(3, markers)
            frac = fracs[:, pl.ds(s, 1), :].reshape(3, markers)
            taps = [tap[t, :, pl.ds(s, 1), :].reshape(3, markers) for t in range(4)]

            weight_z = tap_weights(BAND, cell[2:3] - 1 + (z0 - zb), [w[2:3] for w in taps])
            columns = []
            for q in range(BOX // many):
                packed = None
                for r in range(many):
                    piece = field[:, x0 + (q * many + r), pl.ds(zb, BAND), :]
                    piece = pltpu.roll(piece, lax.rem(wall + r * BAND - y0, wall), 2)
                    packed = piece if r == 0 else jnp.where(lane < r * BAND, packed, piece)
                columns.append(packed.reshape(3 * BAND, wall))
            window = parts(jnp.concatenate(columns, axis=1))
            value = pair(window, (cross[s, 0], cross[s, 1]), 0).reshape(3, BAND, markers)
            sampled = jnp.sum(value * weight_z[None], axis=1)
            lever = cell.astype(jnp.float32) + frac - float(HALF)
            spin = [turning[c, n] for c in range(3)]
            loads = []
            for c in range(3):
                a, b = (c + 1) % 3, (c + 2) % 3
                target = moving[c, n] + (spin[a] * lever[b : b + 1] - spin[b] * lever[a : a + 1])
                loads.append((target - sampled[c : c + 1]) * weight_z)
            load = parts(jnp.concatenate(loads))
            value = pair(load, (cross[s, 0], cross[s, 1]), 1).reshape(3, BAND, BOX * BAND)
            inside = (lane >= y0) & (lane < y0 + BOX)
            for i in range(BOX):
                q, r = i // many, i % many
                piece = value[:, :, q * wall : (q + 1) * wall]
                piece = pltpu.roll(piece, lax.rem(wall + y0 - r * BAND, wall), 2)
                force[:, x0 + i, pl.ds(zb, BAND), :] += jnp.where(inside, piece, 0.0)

        return carry

    lax.fori_loop(0, ids.shape[0], one_slot, 0)


def spread_forces(nx, nz, extended, cross, slot_ids, corners, cells, fracs, moving, turning):
    _, slots, markers = cells.shape
    scalar = pl.BlockSpec(memory_space=pltpu.SMEM)
    vector = pl.BlockSpec(memory_space=pltpu.VMEM)
    return pl.pallas_call(
        functools.partial(marker_kernel, nx, nz),
        out_shape=jax.ShapeDtypeStruct(extended.shape, jnp.float32),
        in_specs=[scalar] * 4 + [vector] * 4,
        out_specs=vector,
        scratch_shapes=[
            pltpu.VMEM((4, 3, slots, markers), jnp.float32),
        ],
        compiler_params=pltpu.CompilerParams(vmem_limit_bytes=16 << 20),
        name="markers",
    )(slot_ids, corners, moving, turning, cells, fracs, extended, cross)


def exchanged(rows, lane_bits):
    lane = lax.broadcasted_iota(jnp.int32, rows[0].shape, rows[0].ndim - 1)
    axis = rows[0].ndim - 1
    for bit, shift in enumerate(lane_bits):
        low = (lane & shift) == 0
        step = 1 << bit
        out = list(rows)
        for m in range(len(rows)):
            if m & step == 0:
                a, b = rows[m], rows[m + step]
                out[m] = jnp.where(low, a, pltpu.roll(b, shift, axis))
                out[m + step] = jnp.where(low, pltpu.roll(a, 128 - shift, axis), b)
        rows = out
    return rows


def spectrum_kernel(
    nx, nz, force, field, table_z, velocity, rows,
    z_got, x_out, x_got, u_out, u_got, row_out, row_got, row_sum, rim_out, rim_got, edge_u,
    edge_w, cut, planes, modes,
    z_send, z_recv, x_send, x_recv, e_send, e_recv, c_send, c_recv, m_send, m_recv,
):
    gx, gz = lax.axis_index("gx"), lax.axis_index("gz")
    left, right, below, above = around(nx, nz)
    barrier = pltpu.get_barrier_semaphore()

    def greet_z(d, carry):
        pl.semaphore_signal(
            barrier, inc=1, device_id=(gx, lax.rem(gz + d, nz)), device_id_type=MESH
        )
        return carry

    def greet_x(d, carry):
        pl.semaphore_signal(
            barrier, inc=1, device_id=(lax.rem(gx + d, nx), gz), device_id_type=MESH
        )
        return carry

    lax.fori_loop(1, nx, greet_x, 0)
    lax.fori_loop(1, nz, greet_z, 0)
    wide, tall = velocity.shape[1], velocity.shape[2]
    row_out[0] = force[2, :, SIDE, :]
    row_out[1] = force[2, :, SIDE + tall - 1, :]
    pl.semaphore_wait(barrier, nx + nz - 2)

    order = (0, 2, 1)
    own = pl.ds(HALF, wide)
    pieces = (pl.ds(0, HALF), pl.ds(HALF + wide, HALF), own)

    def fold_z(c, piece):
        columns = pieces[piece]
        down = remote(
            force.at[c, columns, pl.ds(0, SIDE), :],
            z_got.at[1, c, columns],
            (z_send, z_recv), (1, c, piece), below,
        )
        up = remote(
            force.at[c, columns, pl.ds(SIDE + tall, SIDE), :],
            z_got.at[0, c, columns],
            (z_send, z_recv), (0, c, piece), above,
        )
        down.start()
        up.start()
        return [down, up]

    rims, inner = {}, {}
    for c in order:
        rims[c] = fold_z(c, 0) + fold_z(c, 1)
        if c == 2:
            lines = [
                remote(row_out.at[0], row_got.at[1], (e_send, e_recv), 0, below),
                remote(row_out.at[1], row_got.at[0], (e_send, e_recv), 1, above),
            ]
            for copy in lines:
                copy.start()
    for c in order:
        inner[c] = fold_z(c, 2)
    x_copies = {}
    for c in order:
        for copy in rims[c]:
            copy.wait_recv()
        for part in range(2):
            inside = pl.ds(part * SIDE, SIDE)
            outside = pl.ds(SIDE + part * SIDE, SIDE)
            for side in range(2):
                x_out[side, c, :, inside, :] = (
                    force[c, pieces[side], outside, :] + z_got[part, c, pieces[side]]
                )
        back = remote(x_out.at[0, c], x_got.at[1, c], (x_send, x_recv), (1, c), left)
        ahead = remote(x_out.at[1, c], x_got.at[0, c], (x_send, x_recv), (0, c), right)
        back.start()
        ahead.start()
        x_copies[c] = [back, ahead]
        if c == 2:
            for copy in lines:
                copy.wait_recv()
            row_sum[0] = force[2, :, SIDE - 1, :] + row_got[0]
            row_sum[1] = force[2, :, SIDE + tall, :] + row_got[1]
            rim_out[0] = row_sum[:, pl.ds(0, HALF), :]
            rim_out[1] = row_sum[:, pl.ds(HALF + wide, HALF), :]
            ends = [
                remote(rim_out.at[0], rim_got.at[1], (e_send, e_recv), 2, left),
                remote(rim_out.at[1], rim_got.at[0], (e_send, e_recv), 3, right),
            ]
            for copy in ends:
                copy.start()
        if c == 0:
            for copy in inner[0]:
                copy.wait_recv()
            for part in range(2):
                inside = pl.ds(part * SIDE, SIDE)
                outside = pl.ds(SIDE + part * SIDE, SIDE)
                u_out[0, inside, :] = force[0, HALF, outside, :] + z_got[part, 0, HALF]
                u_out[1, inside, :] = (
                    force[0, HALF + wide - 1, outside, :] + z_got[part, 0, HALF + wide - 1]
                )
            layers = [
                remote(u_out.at[0], u_got.at[1], (e_send, e_recv), 4, left),
                remote(u_out.at[1], u_got.at[0], (e_send, e_recv), 5, right),
            ]
            for copy in layers:
                copy.start()
    for c in order:
        if c != 0:
            for copy in inner[c]:
                copy.wait_recv()
        for part in range(2):
            inside = pl.ds(part * SIDE, SIDE)
            outside = pl.ds(SIDE + part * SIDE, SIDE)
            velocity[c, :, inside, :] = (
                field[c, own, outside, :] + force[c, own, outside, :] + z_got[part, c, own]
            )
    for c in order:
        for copy in x_copies[c]:
            copy.wait_recv()
        velocity[c, pl.ds(0, HALF)] += x_got[0, c]
        velocity[c, pl.ds(wide - HALF, HALF)] += x_got[1, c]
        if c == 0:
            for copy in layers:
                copy.wait_recv()
            body = pl.ds(SIDE, tall)
            edge_u[0] = field[0, HALF - 1, body, :] + x_out[0, 0, HALF - 1] + u_got[0]
            edge_u[1] = field[0, HALF + wide, body, :] + x_out[1, 0, 0] + u_got[1]
        if c == 2:
            for copy in ends:
                copy.wait_recv()
            edge_w[0] = field[2, own, SIDE - 1, :] + row_sum[0, own, :]
            edge_w[1] = field[2, own, SIDE + tall, :] + row_sum[1, own, :]
            edge_w[:, pl.ds(0, HALF), :] += rim_got[0]
            edge_w[:, pl.ds(wide - HALF, HALF), :] += rim_got[1]
    edges = lines + ends + layers
    wall = velocity.shape[3]
    lane = lax.broadcasted_iota(jnp.int32, (1, 1, wall), 2)
    normal = velocity[1]
    upper = jnp.where(lane == wall - 1, 0.0, pltpu.roll(normal, wall - 1, 2))
    lower = jnp.where(lane == 0, 0.0, pltpu.roll(normal, 1, 2))
    divergence = upper - lower
    stream = velocity[0]
    divergence += jnp.concatenate([stream[1:], edge_u[1:2]], axis=0) - jnp.concatenate(
        [edge_u[0:1], stream[:-1]], axis=0
    )
    span = velocity[2]
    row = lax.broadcasted_iota(jnp.int32, (1, tall, 1), 1)
    after = jnp.where(row == tall - 1, edge_w[1][:, None, :], pltpu.roll(span, tall - 1, 1))
    before = jnp.where(row == 0, edge_w[0][:, None, :], pltpu.roll(span, 1, 1))
    divergence = (divergence + (after - before)) * 0.5
    for half in range(wide // 8):
        blocks = exchanged([divergence[half * 8 + i] for i in range(8)], (16, 32, 64))
        for j in range(nz):
            cut[j, :, pl.ds(half * 128, 128)] = blocks[j]

    def cut_copy(d):
        to = lax.rem(gz + d, nz)
        return pltpu.make_async_remote_copy(
            src_ref=cut.at[to],
            dst_ref=planes.at[gz],
            send_sem=c_send.at[to],
            recv_sem=c_recv.at[gz],
            device_id=(gx, to),
            device_id_type=MESH,
        )

    def cut_from(d):
        origin = lax.rem(gz + d, nz)
        return pltpu.make_async_remote_copy(
            src_ref=cut.at[origin],
            dst_ref=planes.at[origin],
            send_sem=c_send.at[origin],
            recv_sem=c_recv.at[origin],
            device_id=(gx, origin),
            device_id_type=MESH,
        )

    def start(make):
        def go(d, carry):
            make(d).start()
            return carry

        return go

    def wait_recv(make):
        def go(d, carry):
            make(d).wait_recv()
            return carry

        return go

    def wait_send(make):
        def go(d, carry):
            make(d).wait_send()
            return carry

        return go

    lax.fori_loop(1, nz, start(cut_copy), 0)
    planes[gz] = cut[gz]
    lax.fori_loop(1, nz, wait_recv(cut_from), 0)
    high, low = parts(planes[...].reshape(nz * tall, 2 * 128))
    modes[...] = pair((table_z[0], table_z[1]), (high, low), 0).reshape(modes.shape)

    deep = nx // 8
    deep_at, along_at = lax.div(gx, 8), lax.rem(gx, 8)

    def partner(t):
        k, j = lax.div(t, deep), lax.rem(t, deep)
        odd = lax.rem(k, 2)
        step = 4 - odd + lax.div(k, 2) * (1 - 2 * odd)
        return lax.rem(deep_at + j + 1, deep) * 8 + lax.rem(along_at + step, 8)

    def mode_copy(t):
        to = partner(t)
        return pltpu.make_async_remote_copy(
            src_ref=modes.at[:, to],
            dst_ref=rows.at[gx],
            send_sem=m_send.at[to],
            recv_sem=m_recv.at[gx],
            device_id=(to, gz),
            device_id_type=MESH,
        )

    def mode_from(t):
        origin = partner(t)
        return pltpu.make_async_remote_copy(
            src_ref=modes.at[:, origin],
            dst_ref=rows.at[origin],
            send_sem=m_send.at[origin],
            recv_sem=m_recv.at[origin],
            device_id=(origin, gz),
            device_id_type=MESH,
        )

    lax.fori_loop(0, nx - 1, start(mode_copy), 0)
    rows[gx] = modes[:, gx]
    lax.fori_loop(0, nx - 1, wait_recv(mode_from), 0)
    for c in order:
        for copy in rims[c] + inner[c] + x_copies[c]:
            copy.wait_send()
    for copy in edges:
        copy.wait_send()
    lax.fori_loop(1, nz, wait_send(cut_copy), 0)
    lax.fori_loop(0, nx - 1, wait_send(mode_copy), 0)


def finish_kernel(scale, velocity_in, rows, table_x, velocity, source, held, sems):
    through = pltpu.make_async_copy(velocity_in, velocity, sems.at[0])
    through.start()
    columns = []
    for h in range(rows.shape[0] // 16):
        for half in range(2):
            blocks = exchanged(
                [rows[h * 16 + b, :, :, half * 128 : half * 128 + 128] for b in range(16)],
                (1, 2, 4, 8),
            )
            columns.append(
                jnp.concatenate([block[0] for block in blocks] + [block[1] for block in blocks])
            )
    high, low = parts(jnp.concatenate(columns, axis=1))
    lines = high.shape[0] // 2
    copies = [through]
    for q in range(table_x.shape[1]):
        value = pair((high, low), (table_x[0, q], table_x[1, q]), 0)
        real = value[:lines, :128] + value[lines:, 128:]
        imag = value[lines:, :128] - value[:lines, 128:]
        out = pl.ds(q * 128, 128)
        held[0, :, :, out] = (real * scale).reshape(held.shape[1], held.shape[2], 128)
        held[1, :, :, out] = (imag * scale).reshape(held.shape[1], held.shape[2], 128)
        copy = pltpu.make_async_copy(
            held.at[:, :, :, out], source.at[:, :, :, out], sems.at[1 + q]
        )
        copy.start()
        copies.append(copy)
    for copy in copies:
        copy.wait()


def split_table(table):
    high = table.astype(jnp.bfloat16)
    return np.stack([high, (table - high.astype(np.float64)).astype(jnp.bfloat16)])


def transform_tables(length_x, length_z):
    counter = np.arange(length_z)
    angle = counter[:, None] * counter[None, :] % length_z * (2 * math.pi / length_z)
    table_z = np.concatenate([np.cos(angle), -np.sin(angle)])
    h, half, i, b = np.meshgrid(
        np.arange(length_x // 256), np.arange(2), np.arange(8), np.arange(16), indexing="ij"
    )
    place = (16 * (16 * h + b) + 8 * half + i).reshape(-1)
    mode = np.arange(length_x)
    angle = place[:, None] * mode[None, :] % length_x * (2 * math.pi / length_x)
    both = np.stack([np.cos(angle), np.sin(angle)], axis=1)
    both = both.reshape(length_x, 2, length_x // 128, 128).transpose(2, 0, 1, 3)
    return split_table(table_z), split_table(both.reshape(length_x // 128, length_x, 256))


def spectrum(force, field, tile, nx, nz):
    _, wide, tall, wall = tile
    length_x, length_z = wide * nx, tall * nz
    table_z, table_x = transform_tables(length_x, length_z)
    vector = pl.BlockSpec(memory_space=pltpu.VMEM)
    dma = pltpu.SemaphoreType.DMA
    each = wall // nz
    deep = field.shape[1]
    modes = length_z // nx
    velocity, rows = pl.pallas_call(
        functools.partial(spectrum_kernel, nx, nz),
        out_shape=(
            jax.ShapeDtypeStruct(tile, jnp.float32),
            jax.ShapeDtypeStruct((nx, 2, modes, wide * each), jnp.float32),
        ),
        in_specs=[vector] * 3,
        out_specs=(vector, vector),
        scratch_shapes=[
            pltpu.VMEM((2, 3, deep, SIDE, wall), jnp.float32),
            pltpu.VMEM((2, 3, HALF, tall, wall), jnp.float32),
            pltpu.VMEM((2, 3, HALF, tall, wall), jnp.float32),
            pltpu.VMEM((2, tall, wall), jnp.float32),
            pltpu.VMEM((2, tall, wall), jnp.float32),
            pltpu.VMEM((2, deep, wall), jnp.float32),
            pltpu.VMEM((2, deep, wall), jnp.float32),
            pltpu.VMEM((2, deep, wall), jnp.float32),
            pltpu.VMEM((2, 2, HALF, wall), jnp.float32),
            pltpu.VMEM((2, 2, HALF, wall), jnp.float32),
            pltpu.VMEM((2, tall, wall), jnp.float32),
            pltpu.VMEM((2, wide, wall), jnp.float32),
            pltpu.VMEM((nz, tall, wide * each), jnp.float32),
            pltpu.VMEM((nz, tall, wide * each), jnp.float32),
            pltpu.VMEM((2, nx, modes, wide * each), jnp.float32),
            dma((2, 3, 3)), dma((2, 3, 3)), dma((2, 3)), dma((2, 3)), dma((6,)), dma((6,)),
            dma((nz,)), dma((nz,)), dma((nx,)), dma((nx,)),
        ],
        compiler_params=pltpu.CompilerParams(
            collective_id=1, has_side_effects=True, vmem_limit_bytes=28 << 20
        ),
        name="spectrum",
    )(force, field, jnp.asarray(table_z))
    shape = (2, each, modes, length_x)
    return pl.pallas_call(
        functools.partial(finish_kernel, 1.0 / math.sqrt(length_x * length_z)),
        out_shape=(
            jax.ShapeDtypeStruct(tile, jnp.float32),
            jax.ShapeDtypeStruct(shape, jnp.float32),
        ),
        in_specs=[vector] * 3,
        out_specs=(pl.BlockSpec(memory_space=pltpu.HBM), pl.BlockSpec(memory_space=pltpu.HBM)),
        scratch_shapes=[
            pltpu.VMEM(shape, jnp.float32),
            dma((1 + length_x // 128,)),
        ],
        compiler_params=pltpu.CompilerParams(vmem_limit_bytes=16 << 20),
        name="finish",
    )(velocity, rows, jnp.asarray(table_x))


def on_device(
    nx, nz, flow_state, slot_ids, corners, marker_cells, marker_frac, particle_velocity,
    particle_spin,
):
    extended, cross = predict(flow_state, marker_cells, marker_frac, nx, nz)
    force = spread_forces(
        nx,
        nz,
        extended,
        cross,
        slot_ids,
        corners,
        marker_cells,
        marker_frac,
        particle_velocity,
        particle_spin,
    )
    return spectrum(force, extended, (3,) + flow_state.shape[1:], nx, nz)


def solution(mesh):
    both = ("gx", "gz")
    placed = (
        P(None, "gx", "gz", None),
        P(both),
        P(None, both),
        P(None, both, None),
        P(None, both, None),
        P(),
        P(),
    )
    return jax.shard_map(
        functools.partial(on_device, mesh.shape["gx"], mesh.shape["gz"]),
        mesh=mesh,
        in_specs=placed,
        out_specs=(P(None, "gx", "gz", None), P(None, "gz", "gx", None)),
        check_vma=False,
    )
```

```python
import functools
import math

import jax
import jax.numpy as jnp
import numpy as np
from jax import lax
from jax.experimental import pallas as pl
from jax.experimental.pallas import tpu as pltpu
from jax.sharding import PartitionSpec as P

BOX = 24
HALF = 12
BAND = 32
SIDE = 16
MESH = pl.DeviceIdType.MESH


time_step = 0.1
viscosity = 0.2
drive_force = 1.0


def remote(source, target, sems, slot, to):
    return pltpu.make_async_remote_copy(
        src_ref=source,
        dst_ref=target,
        send_sem=sems[0].at[slot],
        recv_sem=sems[1].at[slot],
        device_id=to,
        device_id_type=MESH,
    )


def around(nx, nz):
    gx, gz = lax.axis_index("gx"), lax.axis_index("gz")
    return (
        (lax.rem(gx + nx - 1, nx), gz),
        (lax.rem(gx + 1, nx), gz),
        (gx, lax.rem(gz + nz - 1, nz)),
        (gx, lax.rem(gz + 1, nz)),
    )


def parts(value):
    high = value.astype(jnp.bfloat16)
    return high, (value - high.astype(jnp.float32)).astype(jnp.bfloat16)


def tap_weights(length, first, taps):
    offset = lax.broadcasted_iota(jnp.int32, (length, first.shape[-1]), 0) - first
    weight = jnp.where(offset == 3, taps[3], 0.0)
    for t in (2, 1, 0):
        weight = jnp.where(offset == t, taps[t], weight)
    return weight


def fill_taps(fracs, tap):
    angle = fracs[...] * (0.5 * math.pi)
    cosine, sine = jnp.cos(angle), jnp.sin(angle)
    tap[0] = 0.25 * (1.0 - sine)
    tap[1] = 0.25 * (1.0 + cosine)
    tap[2] = 0.25 * (1.0 + sine)
    tap[3] = 0.25 * (1.0 - cosine)


def cross_weights(cells, fracs, tap, cross):
    fill_taps(fracs, tap)
    markers = fracs.shape[2]

    def one_slot(s, carry):
        cell = cells[:, pl.ds(s, 1), :].reshape(3, markers)
        taps = [tap[t, :, pl.ds(s, 1), :].reshape(3, markers) for t in range(4)]
        weight_x = tap_weights(BOX, cell[0:1] - 1, [w[0:1] for w in taps])
        weight_y = tap_weights(BAND, cell[1:2] - 1, [w[1:2] for w in taps])
        for i in range(BOX):
            high, low = parts(weight_x[i : i + 1] * weight_y)
            cross[s, 0, pl.ds(i * BAND, BAND), :] = high
            cross[s, 1, pl.ds(i * BAND, BAND), :] = low
        return carry

    lax.fori_loop(0, cells.shape[1], one_slot, 0)


def front_kernel(
    nx, nz, flow_in, cells_in, fracs_in, field, cross, tap, cells, fracs, flow, edge_x, edge_z_out, edge_z,
    f_sem, e_send, e_recv, x_send, x_recv, z_send, z_recv, r_send, r_recv,
):
    _, wide, tall, wall = flow.shape
    left, right, below, above = around(nx, nz)
    barrier = pltpu.get_barrier_semaphore()
    for near in (left, right, below, above):
        pl.semaphore_signal(barrier, inc=1, device_id=near, device_id_type=MESH)
    loads = [pltpu.make_async_copy(flow_in.at[c], flow.at[c], f_sem.at[c]) for c in range(4)]
    lists = [
        pltpu.make_async_copy(cells_in, cells, f_sem.at[4]),
        pltpu.make_async_copy(fracs_in, fracs, f_sem.at[5]),
    ]
    for load in loads + lists:
        load.start()
    pl.semaphore_wait(barrier, 4)
    for load in loads:
        load.wait()
    edge_z_out[0] = flow[:, :, 0, :]
    edge_z_out[1] = flow[:, :, tall - 1, :]
    edges = [
        remote(flow.at[:, 0], edge_x.at[1], (e_send, e_recv), 0, left),
        remote(flow.at[:, wide - 1], edge_x.at[0], (e_send, e_recv), 1, right),
        remote(edge_z_out.at[0], edge_z.at[1], (e_send, e_recv), 2, below),
        remote(edge_z_out.at[1], edge_z.at[0], (e_send, e_recv), 3, above),
    ]
    for copy in edges:
        copy.start()
    spread = time_step * viscosity
    carry_by = 0.5 * time_step
    lane = lax.broadcasted_iota(jnp.int32, (tall, wall), 1)
    row = lax.broadcasted_iota(jnp.int32, (tall, wall), 0)
    first_y, last_y = lane == 0, lane == wall - 1
    first_z, last_z = row == 0, row == tall - 1

    def layer(x, back, ahead):
        here = [flow[c, x] for c in range(4)]
        moves = [carry_by * here[d] for d in range(3)]
        for c in range(3):
            f = here[c]
            total = f * (1.0 - 6.0 * spread)
            y_plus = jnp.where(last_y, 0.0, pltpu.roll(f, wall - 1, 1))
            y_minus = jnp.where(first_y, 0.0, pltpu.roll(f, 1, 1))
            z_plus = jnp.where(last_z, 0.0, pltpu.roll(f, tall - 1, 0))
            z_minus = jnp.where(first_z, 0.0, pltpu.roll(f, 1, 0))
            for plus, minus, move in (
                (ahead[c], back[c], moves[0]),
                (y_plus, y_minus, moves[1]),
                (z_plus, z_minus, moves[2]),
            ):
                total += plus * (spread - move) + minus * (spread + move)
            p = here[3]
            if c == 0:
                total += time_step * drive_force - carry_by * (ahead[3] - back[3])
            if c == 1:
                p_plus = jnp.where(last_y, p, pltpu.roll(p, wall - 1, 1))
                p_minus = jnp.where(first_y, p, pltpu.roll(p, 1, 1))
                total -= carry_by * (p_plus - p_minus)
            if c == 2:
                p_plus = jnp.where(last_z, 0.0, pltpu.roll(p, tall - 1, 0))
                p_minus = jnp.where(first_z, 0.0, pltpu.roll(p, 1, 0))
                total -= carry_by * (p_plus - p_minus)
            field[c, HALF + x, pl.ds(SIDE, tall), :] = total

    def inside(x, carry):
        layer(x, [flow[c, x - 1] for c in range(4)], [flow[c, x + 1] for c in range(4)])
        return carry

    lax.fori_loop(1, wide - 1, inside, 0)
    rim = HALF - 1
    half = SIDE // 2
    spans = (
        {0: (1, rim), 1: (0, 1), 2: (0, HALF), 3: (0, HALF)},
        {0: (0, rim), 1: (rim, 1), 2: (0, HALF), 3: (0, HALF)},
    )
    lines = {0: (half, SIDE), 1: (half, SIDE), 2: (0, half), 3: (tall - half, half)}
    x_copies, z_copies = {}, []

    def send(c, piece):
        for side in range(2):
            first, count = spans[side][piece]
            at, height = lines[piece]
            source, target = ((HALF, HALF + wide), (wide, 0))[side]
            rows = pl.ds(SIDE + at, height)
            copy = remote(
                field.at[c, pl.ds(source + first, count), rows],
                field.at[c, pl.ds(target + first, count), rows],
                (x_send, x_recv), (side, c, piece), (left, right)[side],
            )
            copy.start()
            x_copies[c, piece, side] = copy

    def forward(c, piece, side):
        first, count = spans[side][piece]
        columns = pl.ds((HALF + wide, 0)[side] + first, count)
        at, height = lines[piece]
        slot = min(piece, 2)
        if piece != 3:
            copy = remote(
                field.at[c, columns, pl.ds(SIDE + at, half)],
                field.at[c, columns, pl.ds(SIDE + tall + at, half)],
                (r_send, r_recv), (0, c, side, slot), below,
            )
            copy.start()
            z_copies.append(copy)
        if piece != 2:
            start = at + height - half
            copy = remote(
                field.at[c, columns, pl.ds(SIDE + start, half)],
                field.at[c, columns, pl.ds(SIDE + start - tall, half)],
                (r_send, r_recv), (1, c, side, slot), above,
            )
            copy.start()
            z_copies.append(copy)

    for c in range(3):
        send(c, 0)
    for copy in edges:
        copy.wait_recv()
    layer(0, [edge_x[0, c] for c in range(4)], [flow[c, 1] for c in range(4)])
    layer(
        wide - 1, [flow[c, wide - 2] for c in range(4)], [edge_x[1, c] for c in range(4)]
    )
    own = pl.ds(HALF, wide)
    for c in range(3):
        for side, z, sign in ((0, 0, 1.0), (1, tall - 1, -1.0)):
            move = carry_by * edge_z_out[side, 2]
            add = edge_z[side, c] * (spread + sign * move)
            if c == 2:
                add += sign * carry_by * edge_z[side, 3]
            field[c, own, SIDE + z, :] += add
        for piece in (2, 3, 1):
            send(c, piece)
    for c in range(3):
        down = remote(
            field.at[c, own, pl.ds(SIDE, SIDE)],
            field.at[c, own, pl.ds(SIDE + tall, SIDE)],
            (z_send, z_recv), (0, c), below,
        )
        up = remote(
            field.at[c, own, pl.ds(tall, SIDE)],
            field.at[c, own, pl.ds(0, SIDE)],
            (z_send, z_recv), (1, c), above,
        )
        down.start()
        up.start()
        z_copies.extend((down, up))
    for load in lists:
        load.wait()
    cross_weights(cells, fracs, tap, cross)
    for c, piece in [(c, 0) for c in range(3)] + [(c, p) for c in range(3) for p in (2, 3, 1)]:
        for side in range(2):
            x_copies[c, piece, side].wait_recv()
            forward(c, piece, side)
    for copy in z_copies:
        copy.wait_recv()
    for copy in edges + z_copies + list(x_copies.values()):
        copy.wait_send()


def predict(flow, cells, fracs, nx, nz):
    _, wide, tall, wall = flow.shape
    _, slots, markers = cells.shape
    vector = pl.BlockSpec(memory_space=pltpu.VMEM)
    dma = pltpu.SemaphoreType.DMA
    return pl.pallas_call(
        functools.partial(front_kernel, nx, nz),
        out_shape=(
            jax.ShapeDtypeStruct(
                (3, wide + 2 * HALF, tall + 2 * SIDE, wall), jnp.float32
            ),
            jax.ShapeDtypeStruct((slots, 2, BOX * BAND, markers), jnp.bfloat16),
            jax.ShapeDtypeStruct((4,) + cells.shape, jnp.float32),
            jax.ShapeDtypeStruct(cells.shape, jnp.int32),
            jax.ShapeDtypeStruct(cells.shape, jnp.float32),
        ),
        in_specs=[pl.BlockSpec(memory_space=pltpu.HBM)] * 3,
        out_specs=(vector,) * 5,
        scratch_shapes=[
            pltpu.VMEM(flow.shape, jnp.float32),
            pltpu.VMEM((2, 4, tall, wall), jnp.float32),
            pltpu.VMEM((2, 4, wide, wall), jnp.float32),
            pltpu.VMEM((2, 4, wide, wall), jnp.float32),
            dma((6,)), dma((4,)), dma((4,)), dma((2, 3, 4)), dma((2, 3, 4)), dma((2, 3)),
            dma((2, 3)), dma((2, 3, 2, 3)), dma((2, 3, 2, 3)),
        ],
        compiler_params=pltpu.CompilerParams(
            collective_id=0, has_side_effects=True, vmem_limit_bytes=12 << 20
        ),
        name="front",
    )(*(pltpu.with_memory_space_constraint(each, pltpu.HBM) for each in (flow, cells, fracs)))


def dot(a, b, across):
    return lax.dot_general(
        a, b, (((1,), (across,)), ((), ())), preferred_element_type=jnp.float32
    )


def pair(a, b, across):
    rows = a[0].shape[0]
    both = dot(jnp.concatenate(a), b[0], across)
    return both[:rows] + both[rows:] + dot(a[0], b[1], across)


def marker_kernel(
    nx, nz, ids, corners, moving, turning, cells, fracs, tap, field, cross, force
):
    force[...] = jnp.zeros_like(force)
    markers = fracs.shape[2]
    wall = field.shape[3]
    wide, tall = field.shape[1] - 2 * HALF, field.shape[2] - 2 * SIDE
    first_x = lax.axis_index("gx") * wide - HALF
    first_z = lax.axis_index("gz") * tall - SIDE
    many = wall // BAND
    lane = lax.broadcasted_iota(jnp.int32, (1, 1, wall), 2)

    def one_slot(s, carry):
        if True:
            n = lax.max(ids[s], 0)
            living = jnp.where(ids[s] >= 0, 1.0, 0.0)
            x0 = lax.rem(corners[0, s] - first_x + wide * nx, wide * nx)
            y0 = corners[1, s]
            z0 = lax.rem(corners[2, s] - first_z + tall * nz, tall * nz)
            zb = pl.multiple_of((z0 // 8) * 8, 8)
            cell = cells[:, pl.ds(s, 1), :].reshape(3, markers)
            frac = fracs[:, pl.ds(s, 1), :].reshape(3, markers)
            taps = [tap[t, :, pl.ds(s, 1), :].reshape(3, markers) for t in range(4)]

            weight_z = tap_weights(BAND, cell[2:3] - 1 + (z0 - zb), [w[2:3] for w in taps])
            columns = []
            for q in range(BOX // many):
                packed = None
                for r in range(many):
                    piece = field[:, x0 + (q * many + r), pl.ds(zb, BAND), :]
                    piece = pltpu.roll(piece, lax.rem(wall + r * BAND - y0, wall), 2)
                    packed = piece if r == 0 else jnp.where(lane < r * BAND, packed, piece)
                columns.append(packed.reshape(3 * BAND, wall))
            window = parts(jnp.concatenate(columns, axis=1))
            value = pair(window, (cross[s, 0], cross[s, 1]), 0).reshape(3, BAND, markers)
            sampled = jnp.sum(value * weight_z[None], axis=1)
            lever = cell.astype(jnp.float32) + frac - float(HALF)
            spin = [turning[c, n] for c in range(3)]
            loads = []
            for c in range(3):
                a, b = (c + 1) % 3, (c + 2) % 3
                target = moving[c, n] + (spin[a] * lever[b : b + 1] - spin[b] * lever[a : a + 1])
                loads.append((living * (target - sampled[c : c + 1])) * weight_z)
            load = parts(jnp.concatenate(loads))
            value = pair(load, (cross[s, 0], cross[s, 1]), 1).reshape(3, BAND, BOX * BAND)
            inside = (lane >= y0) & (lane < y0 + BOX)
            for i in range(BOX):
                q, r = i // many, i % many
                piece = value[:, :, q * wall : (q + 1) * wall]
                piece = pltpu.roll(piece, lax.rem(wall + y0 - r * BAND, wall), 2)
                force[:, x0 + i, pl.ds(zb, BAND), :] += jnp.where(inside, piece, 0.0)

        return carry

    def four_slots(h, carry):
        for k in range(4):
            one_slot(4 * h + k, carry)
        return carry

    lax.fori_loop(0, ids.shape[0] // 4, four_slots, 0)


def spread_forces(nx, nz, extended, cross, tap, slot_ids, corners, cells, fracs, moving, turning):
    scalar = pl.BlockSpec(memory_space=pltpu.SMEM)
    vector = pl.BlockSpec(memory_space=pltpu.VMEM)
    scalars = [
        pltpu.with_memory_space_constraint(each, pltpu.HBM)
        for each in (slot_ids, corners, moving, turning)
    ]
    return pl.pallas_call(
        functools.partial(marker_kernel, nx, nz),
        out_shape=jax.ShapeDtypeStruct(extended.shape, jnp.float32),
        in_specs=[scalar] * 4 + [vector] * 5,
        out_specs=vector,
        compiler_params=pltpu.CompilerParams(vmem_limit_bytes=16 << 20),
        name="markers",
    )(*scalars, cells, fracs, tap, extended, cross)


def exchanged(rows, lane_bits):
    lane = lax.broadcasted_iota(jnp.int32, rows[0].shape, rows[0].ndim - 1)
    axis = rows[0].ndim - 1
    for bit, shift in enumerate(lane_bits):
        low = (lane & shift) == 0
        step = 1 << bit
        out = list(rows)
        for m in range(len(rows)):
            if m & step == 0:
                a, b = rows[m], rows[m + step]
                out[m] = jnp.where(low, a, pltpu.roll(b, shift, axis))
                out[m + step] = jnp.where(low, pltpu.roll(a, 128 - shift, axis), b)
        rows = out
    return rows


def spectrum_kernel(
    nx, nz, force, field, table_z, velocity, rows,
    z_got, x_out, x_got, u_out, u_got, row_out, row_got, row_sum, rim_out, rim_got, edge_u,
    edge_w, cut, planes, modes,
    z_send, z_recv, x_send, x_recv, e_send, e_recv, c_send, c_recv, m_send, m_recv,
):
    gx, gz = lax.axis_index("gx"), lax.axis_index("gz")
    left, right, below, above = around(nx, nz)
    barrier = pltpu.get_barrier_semaphore()

    def greet_z(d, carry):
        pl.semaphore_signal(
            barrier, inc=1, device_id=(gx, lax.rem(gz + d, nz)), device_id_type=MESH
        )
        return carry

    def greet_x(d, carry):
        pl.semaphore_signal(
            barrier, inc=1, device_id=(lax.rem(gx + d, nx), gz), device_id_type=MESH
        )
        return carry

    lax.fori_loop(1, nx, greet_x, 0)
    lax.fori_loop(1, nz, greet_z, 0)
    wide, tall = velocity.shape[1], velocity.shape[2]
    row_out[0] = force[2, :, SIDE, :]
    row_out[1] = force[2, :, SIDE + tall - 1, :]
    pl.semaphore_wait(barrier, nx + nz - 2)

    order = (0, 2, 1)
    own = pl.ds(HALF, wide)
    pieces = (pl.ds(0, HALF), pl.ds(HALF + wide, HALF), own)

    def fold_z(c, piece):
        columns = pieces[piece]
        down = remote(
            force.at[c, columns, pl.ds(0, SIDE), :],
            z_got.at[1, c, columns],
            (z_send, z_recv), (1, c, piece), below,
        )
        up = remote(
            force.at[c, columns, pl.ds(SIDE + tall, SIDE), :],
            z_got.at[0, c, columns],
            (z_send, z_recv), (0, c, piece), above,
        )
        down.start()
        up.start()
        return [down, up]

    rims, inner = {}, {}
    for c in order:
        rims[c] = fold_z(c, 0) + fold_z(c, 1)
        if c == 2:
            lines = [
                remote(row_out.at[0], row_got.at[1], (e_send, e_recv), 0, below),
                remote(row_out.at[1], row_got.at[0], (e_send, e_recv), 1, above),
            ]
            for copy in lines:
                copy.start()
    for c in order:
        inner[c] = fold_z(c, 2)
    x_copies = {}
    for c in order:
        for copy in rims[c]:
            copy.wait_recv()
        for part in range(2):
            inside = pl.ds(part * SIDE, SIDE)
            outside = pl.ds(SIDE + part * SIDE, SIDE)
            for side in range(2):
                x_out[side, c, :, inside, :] = (
                    force[c, pieces[side], outside, :] + z_got[part, c, pieces[side]]
                )
        back = remote(x_out.at[0, c], x_got.at[1, c], (x_send, x_recv), (1, c), left)
        ahead = remote(x_out.at[1, c], x_got.at[0, c], (x_send, x_recv), (0, c), right)
        back.start()
        ahead.start()
        x_copies[c] = [back, ahead]
        if c == 2:
            for copy in lines:
                copy.wait_recv()
            row_sum[0] = force[2, :, SIDE - 1, :] + row_got[0]
            row_sum[1] = force[2, :, SIDE + tall, :] + row_got[1]
            rim_out[0] = row_sum[:, pl.ds(0, HALF), :]
            rim_out[1] = row_sum[:, pl.ds(HALF + wide, HALF), :]
            ends = [
                remote(rim_out.at[0], rim_got.at[1], (e_send, e_recv), 2, left),
                remote(rim_out.at[1], rim_got.at[0], (e_send, e_recv), 3, right),
            ]
            for copy in ends:
                copy.start()
        if c == 0:
            for copy in inner[0]:
                copy.wait_recv()
            for part in range(2):
                inside = pl.ds(part * SIDE, SIDE)
                outside = pl.ds(SIDE + part * SIDE, SIDE)
                u_out[0, inside, :] = force[0, HALF, outside, :] + z_got[part, 0, HALF]
                u_out[1, inside, :] = (
                    force[0, HALF + wide - 1, outside, :] + z_got[part, 0, HALF + wide - 1]
                )
            layers = [
                remote(u_out.at[0], u_got.at[1], (e_send, e_recv), 4, left),
                remote(u_out.at[1], u_got.at[0], (e_send, e_recv), 5, right),
            ]
            for copy in layers:
                copy.start()
    for c in order:
        if c != 0:
            for copy in inner[c]:
                copy.wait_recv()
        for part in range(2):
            inside = pl.ds(part * SIDE, SIDE)
            outside = pl.ds(SIDE + part * SIDE, SIDE)
            velocity[c, :, inside, :] = (
                field[c, own, outside, :] + force[c, own, outside, :] + z_got[part, c, own]
            )
    for c in order:
        for copy in x_copies[c]:
            copy.wait_recv()
        velocity[c, pl.ds(0, HALF)] += x_got[0, c]
        velocity[c, pl.ds(wide - HALF, HALF)] += x_got[1, c]
        if c == 0:
            for copy in layers:
                copy.wait_recv()
            body = pl.ds(SIDE, tall)
            edge_u[0] = field[0, HALF - 1, body, :] + x_out[0, 0, HALF - 1] + u_got[0]
            edge_u[1] = field[0, HALF + wide, body, :] + x_out[1, 0, 0] + u_got[1]
        if c == 2:
            for copy in ends:
                copy.wait_recv()
            edge_w[0] = field[2, own, SIDE - 1, :] + row_sum[0, own, :]
            edge_w[1] = field[2, own, SIDE + tall, :] + row_sum[1, own, :]
            edge_w[:, pl.ds(0, HALF), :] += rim_got[0]
            edge_w[:, pl.ds(wide - HALF, HALF), :] += rim_got[1]
    edges = lines + ends + layers
    wall = velocity.shape[3]
    lane = lax.broadcasted_iota(jnp.int32, (1, 1, wall), 2)
    normal = velocity[1]
    upper = jnp.where(lane == wall - 1, 0.0, pltpu.roll(normal, wall - 1, 2))
    lower = jnp.where(lane == 0, 0.0, pltpu.roll(normal, 1, 2))
    divergence = upper - lower
    stream = velocity[0]
    divergence += jnp.concatenate([stream[1:], edge_u[1:2]], axis=0) - jnp.concatenate(
        [edge_u[0:1], stream[:-1]], axis=0
    )
    span = velocity[2]
    row = lax.broadcasted_iota(jnp.int32, (1, tall, 1), 1)
    after = jnp.where(row == tall - 1, edge_w[1][:, None, :], pltpu.roll(span, tall - 1, 1))
    before = jnp.where(row == 0, edge_w[0][:, None, :], pltpu.roll(span, 1, 1))
    divergence = (divergence + (after - before)) * 0.5
    for half in range(wide // 8):
        blocks = exchanged([divergence[half * 8 + i] for i in range(8)], (16, 32, 64))
        for j in range(nz):
            cut[j, :, pl.ds(half * 128, 128)] = blocks[j]

    def cut_copy(d):
        to = lax.rem(gz + d, nz)
        return pltpu.make_async_remote_copy(
            src_ref=cut.at[to],
            dst_ref=planes.at[gz],
            send_sem=c_send.at[to],
            recv_sem=c_recv.at[gz],
            device_id=(gx, to),
            device_id_type=MESH,
        )

    def cut_from(d):
        origin = lax.rem(gz + d, nz)
        return pltpu.make_async_remote_copy(
            src_ref=cut.at[origin],
            dst_ref=planes.at[origin],
            send_sem=c_send.at[origin],
            recv_sem=c_recv.at[origin],
            device_id=(gx, origin),
            device_id_type=MESH,
        )

    def start(make):
        def go(d, carry):
            make(d).start()
            return carry

        return go

    def wait_recv(make):
        def go(d, carry):
            make(d).wait_recv()
            return carry

        return go

    def wait_send(make):
        def go(d, carry):
            make(d).wait_send()
            return carry

        return go

    lax.fori_loop(1, nz, start(cut_copy), 0)
    planes[gz] = cut[gz]
    lax.fori_loop(1, nz, wait_recv(cut_from), 0)
    high, low = parts(planes[...].reshape(nz * tall, 2 * 128))
    modes[...] = pair((table_z[0], table_z[1]), (high, low), 0).reshape(modes.shape)

    deep = nx // 8
    deep_at, along_at = lax.div(gx, 8), lax.rem(gx, 8)

    def partner(t):
        k, j = lax.div(t, deep), lax.rem(t, deep)
        odd = lax.rem(k, 2)
        step = 4 - odd + lax.div(k, 2) * (1 - 2 * odd)
        return lax.rem(deep_at + j + 1, deep) * 8 + lax.rem(along_at + step, 8)

    def mode_copy(t):
        to = partner(t)
        return pltpu.make_async_remote_copy(
            src_ref=modes.at[:, to],
            dst_ref=rows.at[gx],
            send_sem=m_send.at[to],
            recv_sem=m_recv.at[gx],
            device_id=(to, gz),
            device_id_type=MESH,
        )

    def mode_from(t):
        origin = partner(t)
        return pltpu.make_async_remote_copy(
            src_ref=modes.at[:, origin],
            dst_ref=rows.at[origin],
            send_sem=m_send.at[origin],
            recv_sem=m_recv.at[origin],
            device_id=(origin, gz),
            device_id_type=MESH,
        )

    lax.fori_loop(0, nx - 1, start(mode_copy), 0)
    rows[gx] = modes[:, gx]
    lax.fori_loop(0, nx - 1, wait_recv(mode_from), 0)
    for c in order:
        for copy in rims[c] + inner[c] + x_copies[c]:
            copy.wait_send()
    for copy in edges:
        copy.wait_send()
    lax.fori_loop(1, nz, wait_send(cut_copy), 0)
    lax.fori_loop(0, nx - 1, wait_send(mode_copy), 0)


def finish_kernel(scale, velocity_in, rows, table_x, velocity, source, held, sems):
    through = pltpu.make_async_copy(velocity_in, velocity, sems.at[0])
    through.start()
    columns = []
    for h in range(rows.shape[0] // 16):
        for half in range(2):
            blocks = exchanged(
                [rows[h * 16 + b, :, :, half * 128 : half * 128 + 128] for b in range(16)],
                (1, 2, 4, 8),
            )
            columns.append(
                jnp.concatenate([block[0] for block in blocks] + [block[1] for block in blocks])
            )
    high, low = parts(jnp.concatenate(columns, axis=1))
    lines = high.shape[0] // 2
    copies = [through]
    for q in range(table_x.shape[1]):
        value = pair((high, low), (table_x[0, q], table_x[1, q]), 0)
        real = value[:lines, :128] + value[lines:, 128:]
        imag = value[lines:, :128] - value[:lines, 128:]
        out = pl.ds(q * 128, 128)
        held[0, :, :, out] = (real * scale).reshape(held.shape[1], held.shape[2], 128)
        held[1, :, :, out] = (imag * scale).reshape(held.shape[1], held.shape[2], 128)
        copy = pltpu.make_async_copy(
            held.at[:, :, :, out], source.at[:, :, :, out], sems.at[1 + q]
        )
        copy.start()
        copies.append(copy)
    for copy in copies:
        copy.wait()


def split_table(table):
    high = table.astype(jnp.bfloat16)
    return np.stack([high, (table - high.astype(np.float64)).astype(jnp.bfloat16)])


def transform_tables(length_x, length_z):
    counter = np.arange(length_z)
    angle = counter[:, None] * counter[None, :] % length_z * (2 * math.pi / length_z)
    table_z = np.concatenate([np.cos(angle), -np.sin(angle)])
    h, half, i, b = np.meshgrid(
        np.arange(length_x // 256), np.arange(2), np.arange(8), np.arange(16), indexing="ij"
    )
    place = (16 * (16 * h + b) + 8 * half + i).reshape(-1)
    mode = np.arange(length_x)
    angle = place[:, None] * mode[None, :] % length_x * (2 * math.pi / length_x)
    both = np.stack([np.cos(angle), np.sin(angle)], axis=1)
    both = both.reshape(length_x, 2, length_x // 128, 128).transpose(2, 0, 1, 3)
    return split_table(table_z), split_table(both.reshape(length_x // 128, length_x, 256))


def spectrum(force, field, tile, nx, nz):
    _, wide, tall, wall = tile
    length_x, length_z = wide * nx, tall * nz
    table_z, table_x = transform_tables(length_x, length_z)
    vector = pl.BlockSpec(memory_space=pltpu.VMEM)
    dma = pltpu.SemaphoreType.DMA
    each = wall // nz
    deep = field.shape[1]
    modes = length_z // nx
    velocity, rows = pl.pallas_call(
        functools.partial(spectrum_kernel, nx, nz),
        out_shape=(
            jax.ShapeDtypeStruct(tile, jnp.float32),
            jax.ShapeDtypeStruct((nx, 2, modes, wide * each), jnp.float32),
        ),
        in_specs=[vector] * 3,
        out_specs=(vector, vector),
        scratch_shapes=[
            pltpu.VMEM((2, 3, deep, SIDE, wall), jnp.float32),
            pltpu.VMEM((2, 3, HALF, tall, wall), jnp.float32),
            pltpu.VMEM((2, 3, HALF, tall, wall), jnp.float32),
            pltpu.VMEM((2, tall, wall), jnp.float32),
            pltpu.VMEM((2, tall, wall), jnp.float32),
            pltpu.VMEM((2, deep, wall), jnp.float32),
            pltpu.VMEM((2, deep, wall), jnp.float32),
            pltpu.VMEM((2, deep, wall), jnp.float32),
            pltpu.VMEM((2, 2, HALF, wall), jnp.float32),
            pltpu.VMEM((2, 2, HALF, wall), jnp.float32),
            pltpu.VMEM((2, tall, wall), jnp.float32),
            pltpu.VMEM((2, wide, wall), jnp.float32),
            pltpu.VMEM((nz, tall, wide * each), jnp.float32),
            pltpu.VMEM((nz, tall, wide * each), jnp.float32),
            pltpu.VMEM((2, nx, modes, wide * each), jnp.float32),
            dma((2, 3, 3)), dma((2, 3, 3)), dma((2, 3)), dma((2, 3)), dma((6,)), dma((6,)),
            dma((nz,)), dma((nz,)), dma((nx,)), dma((nx,)),
        ],
        compiler_params=pltpu.CompilerParams(
            collective_id=1, has_side_effects=True, vmem_limit_bytes=28 << 20
        ),
        name="spectrum",
    )(force, field, jnp.asarray(table_z))
    shape = (2, each, modes, length_x)
    return pl.pallas_call(
        functools.partial(finish_kernel, 1.0 / math.sqrt(length_x * length_z)),
        out_shape=(
            jax.ShapeDtypeStruct(tile, jnp.float32),
            jax.ShapeDtypeStruct(shape, jnp.float32),
        ),
        in_specs=[vector] * 3,
        out_specs=(pl.BlockSpec(memory_space=pltpu.HBM), pl.BlockSpec(memory_space=pltpu.HBM)),
        scratch_shapes=[
            pltpu.VMEM(shape, jnp.float32),
            dma((1 + length_x // 128,)),
        ],
        compiler_params=pltpu.CompilerParams(vmem_limit_bytes=16 << 20),
        name="finish",
    )(velocity, rows, jnp.asarray(table_x))


def on_device(
    nx, nz, flow_state, slot_ids, corners, marker_cells, marker_frac, particle_velocity,
    particle_spin,
):
    extended, cross, tap, cells, fracs = predict(flow_state, marker_cells, marker_frac, nx, nz)
    force = spread_forces(
        nx,
        nz,
        extended,
        cross,
        tap,
        slot_ids,
        corners,
        cells,
        fracs,
        particle_velocity,
        particle_spin,
    )
    return spectrum(force, extended, (3,) + flow_state.shape[1:], nx, nz)


def solution(mesh):
    both = ("gx", "gz")
    placed = (
        P(None, "gx", "gz", None),
        P(both),
        P(None, both),
        P(None, both, None),
        P(None, both, None),
        P(),
        P(),
    )
    return jax.shard_map(
        functools.partial(on_device, mesh.shape["gx"], mesh.shape["gz"]),
        mesh=mesh,
        in_specs=placed,
        out_specs=(P(None, "gx", "gz", None), P(None, "gz", "gx", None)),
        check_vma=False,
    )
```

```python
import functools
import math

import jax
import jax.numpy as jnp
import numpy as np
from jax import lax
from jax.experimental import pallas as pl
from jax.experimental.pallas import tpu as pltpu
from jax.sharding import PartitionSpec as P

BOX = 24
HALF = 12
BAND = 32
SIDE = 16
MESH = pl.DeviceIdType.MESH


time_step = 0.1
viscosity = 0.2
drive_force = 1.0


def remote(source, target, sems, slot, to):
    return pltpu.make_async_remote_copy(
        src_ref=source,
        dst_ref=target,
        send_sem=sems[0].at[slot],
        recv_sem=sems[1].at[slot],
        device_id=to,
        device_id_type=MESH,
    )


def around(nx, nz):
    gx, gz = lax.axis_index("gx"), lax.axis_index("gz")
    return (
        (lax.rem(gx + nx - 1, nx), gz),
        (lax.rem(gx + 1, nx), gz),
        (gx, lax.rem(gz + nz - 1, nz)),
        (gx, lax.rem(gz + 1, nz)),
    )


def parts(value):
    high = value.astype(jnp.bfloat16)
    return high, (value - high.astype(jnp.float32)).astype(jnp.bfloat16)


def tap_weights(length, first, taps):
    offset = lax.broadcasted_iota(jnp.int32, (length, first.shape[-1]), 0) - first
    weight = jnp.where(offset == 3, taps[3], 0.0)
    for t in (2, 1, 0):
        weight = jnp.where(offset == t, taps[t], weight)
    return weight


def fill_taps(fracs, tap):
    angle = fracs[...] * (0.5 * math.pi)
    cosine, sine = jnp.cos(angle), jnp.sin(angle)
    tap[0] = 0.25 * (1.0 - sine)
    tap[1] = 0.25 * (1.0 + cosine)
    tap[2] = 0.25 * (1.0 + sine)
    tap[3] = 0.25 * (1.0 - cosine)


def cross_weights(cells, fracs, tap, cross):
    fill_taps(fracs, tap)
    markers = fracs.shape[2]

    def one_slot(s, carry):
        cell = cells[:, pl.ds(s, 1), :].reshape(3, markers)
        taps = [tap[t, :, pl.ds(s, 1), :].reshape(3, markers) for t in range(4)]
        weight_x = tap_weights(BOX, cell[0:1] - 1, [w[0:1] for w in taps])
        weight_y = tap_weights(BAND, cell[1:2] - 1, [w[1:2] for w in taps])
        for i in range(BOX):
            high, low = parts(weight_x[i : i + 1] * weight_y)
            cross[s, 0, pl.ds(i * BAND, BAND), :] = high
            cross[s, 1, pl.ds(i * BAND, BAND), :] = low
        return carry

    lax.fori_loop(0, cells.shape[1], one_slot, 0)


def front_kernel(
    nx, nz, flow_in, cells_in, fracs_in, field, cross, tap, cells, fracs, flow, edge_x, edge_z_out, edge_z,
    f_sem, e_send, e_recv, x_send, x_recv, z_send, z_recv, r_send, r_recv,
):
    _, wide, tall, wall = flow.shape
    left, right, below, above = around(nx, nz)
    barrier = pltpu.get_barrier_semaphore()
    for near in (left, right, below, above):
        pl.semaphore_signal(barrier, inc=1, device_id=near, device_id_type=MESH)
    loads = [pltpu.make_async_copy(flow_in.at[c], flow.at[c], f_sem.at[c]) for c in range(4)]
    lists = [
        pltpu.make_async_copy(cells_in, cells, f_sem.at[4]),
        pltpu.make_async_copy(fracs_in, fracs, f_sem.at[5]),
    ]
    for load in loads + lists:
        load.start()
    pl.semaphore_wait(barrier, 4)
    for load in loads:
        load.wait()
    edge_z_out[0] = flow[:, :, 0, :]
    edge_z_out[1] = flow[:, :, tall - 1, :]
    edges = [
        remote(flow.at[:, 0], edge_x.at[1], (e_send, e_recv), 0, left),
        remote(flow.at[:, wide - 1], edge_x.at[0], (e_send, e_recv), 1, right),
        remote(edge_z_out.at[0], edge_z.at[1], (e_send, e_recv), 2, below),
        remote(edge_z_out.at[1], edge_z.at[0], (e_send, e_recv), 3, above),
    ]
    for copy in edges:
        copy.start()
    spread = time_step * viscosity
    carry_by = 0.5 * time_step
    lane = lax.broadcasted_iota(jnp.int32, (tall, wall), 1)
    row = lax.broadcasted_iota(jnp.int32, (tall, wall), 0)
    first_y, last_y = lane == 0, lane == wall - 1
    first_z, last_z = row == 0, row == tall - 1

    def layer(x, back, ahead):
        here = [flow[c, x] for c in range(4)]
        moves = [carry_by * here[d] for d in range(3)]
        for c in range(3):
            f = here[c]
            total = f * (1.0 - 6.0 * spread)
            y_plus = jnp.where(last_y, 0.0, pltpu.roll(f, wall - 1, 1))
            y_minus = jnp.where(first_y, 0.0, pltpu.roll(f, 1, 1))
            z_plus = jnp.where(last_z, 0.0, pltpu.roll(f, tall - 1, 0))
            z_minus = jnp.where(first_z, 0.0, pltpu.roll(f, 1, 0))
            for plus, minus, move in (
                (ahead[c], back[c], moves[0]),
                (y_plus, y_minus, moves[1]),
                (z_plus, z_minus, moves[2]),
            ):
                total += plus * (spread - move) + minus * (spread + move)
            p = here[3]
            if c == 0:
                total += time_step * drive_force - carry_by * (ahead[3] - back[3])
            if c == 1:
                p_plus = jnp.where(last_y, p, pltpu.roll(p, wall - 1, 1))
                p_minus = jnp.where(first_y, p, pltpu.roll(p, 1, 1))
                total -= carry_by * (p_plus - p_minus)
            if c == 2:
                p_plus = jnp.where(last_z, 0.0, pltpu.roll(p, tall - 1, 0))
                p_minus = jnp.where(first_z, 0.0, pltpu.roll(p, 1, 0))
                total -= carry_by * (p_plus - p_minus)
            field[c, HALF + x, pl.ds(SIDE, tall), :] = total

    def inside(x, carry):
        layer(x, [flow[c, x - 1] for c in range(4)], [flow[c, x + 1] for c in range(4)])
        return carry

    lax.fori_loop(1, wide - 1, inside, 0)
    rim = HALF - 1
    half = SIDE // 2
    spans = (
        {0: (1, rim), 1: (0, 1), 2: (0, HALF), 3: (0, HALF)},
        {0: (0, rim), 1: (rim, 1), 2: (0, HALF), 3: (0, HALF)},
    )
    lines = {0: (half, SIDE), 1: (half, SIDE), 2: (0, half), 3: (tall - half, half)}
    x_copies, z_copies = {}, []

    def send(c, piece):
        for side in range(2):
            first, count = spans[side][piece]
            at, height = lines[piece]
            source, target = ((HALF, HALF + wide), (wide, 0))[side]
            rows = pl.ds(SIDE + at, height)
            copy = remote(
                field.at[c, pl.ds(source + first, count), rows],
                field.at[c, pl.ds(target + first, count), rows],
                (x_send, x_recv), (side, c, piece), (left, right)[side],
            )
            copy.start()
            x_copies[c, piece, side] = copy

    def forward(c, piece, side):
        first, count = spans[side][piece]
        columns = pl.ds((HALF + wide, 0)[side] + first, count)
        at, height = lines[piece]
        slot = min(piece, 2)
        if piece != 3:
            count = min(at + height, HALF) - at
            copy = remote(
                field.at[c, columns, pl.ds(SIDE + at, count)],
                field.at[c, columns, pl.ds(SIDE + tall + at, count)],
                (r_send, r_recv), (0, c, side, slot), below,
            )
            copy.start()
            z_copies.append(copy)
        if piece != 2:
            start = max(at, tall - HALF)
            count = at + height - start
            copy = remote(
                field.at[c, columns, pl.ds(SIDE + start, count)],
                field.at[c, columns, pl.ds(SIDE + start - tall, count)],
                (r_send, r_recv), (1, c, side, slot), above,
            )
            copy.start()
            z_copies.append(copy)

    for c in range(3):
        send(c, 0)
    for copy in edges:
        copy.wait_recv()
    layer(0, [edge_x[0, c] for c in range(4)], [flow[c, 1] for c in range(4)])
    layer(
        wide - 1, [flow[c, wide - 2] for c in range(4)], [edge_x[1, c] for c in range(4)]
    )
    own = pl.ds(HALF, wide)
    for c in range(3):
        for side, z, sign in ((0, 0, 1.0), (1, tall - 1, -1.0)):
            move = carry_by * edge_z_out[side, 2]
            add = edge_z[side, c] * (spread + sign * move)
            if c == 2:
                add += sign * carry_by * edge_z[side, 3]
            field[c, own, SIDE + z, :] += add
        for piece in (2, 3, 1):
            send(c, piece)
    for c in range(3):
        down = remote(
            field.at[c, own, pl.ds(SIDE, HALF)],
            field.at[c, own, pl.ds(SIDE + tall, HALF)],
            (z_send, z_recv), (0, c), below,
        )
        up = remote(
            field.at[c, own, pl.ds(SIDE + tall - HALF, HALF)],
            field.at[c, own, pl.ds(SIDE - HALF, HALF)],
            (z_send, z_recv), (1, c), above,
        )
        down.start()
        up.start()
        z_copies.extend((down, up))
    blank = jnp.zeros(field.shape[:2] + (SIDE - HALF, wall), jnp.float32)
    field[:, :, pl.ds(0, SIDE - HALF), :] = blank
    field[:, :, pl.ds(SIDE + tall + HALF, SIDE - HALF), :] = blank
    for load in lists:
        load.wait()
    cross_weights(cells, fracs, tap, cross)
    for c, piece in [(c, 0) for c in range(3)] + [(c, p) for c in range(3) for p in (2, 3, 1)]:
        for side in range(2):
            x_copies[c, piece, side].wait_recv()
            forward(c, piece, side)
    for copy in z_copies:
        copy.wait_recv()
    for copy in edges + z_copies + list(x_copies.values()):
        copy.wait_send()


def predict(flow, cells, fracs, nx, nz):
    _, wide, tall, wall = flow.shape
    _, slots, markers = cells.shape
    vector = pl.BlockSpec(memory_space=pltpu.VMEM)
    dma = pltpu.SemaphoreType.DMA
    return pl.pallas_call(
        functools.partial(front_kernel, nx, nz),
        out_shape=(
            jax.ShapeDtypeStruct(
                (3, wide + 2 * HALF, tall + 2 * SIDE, wall), jnp.float32
            ),
            jax.ShapeDtypeStruct((slots, 2, BOX * BAND, markers), jnp.bfloat16),
            jax.ShapeDtypeStruct((4,) + cells.shape, jnp.float32),
            jax.ShapeDtypeStruct(cells.shape, jnp.int32),
            jax.ShapeDtypeStruct(cells.shape, jnp.float32),
        ),
        in_specs=[pl.BlockSpec(memory_space=pltpu.HBM)] * 3,
        out_specs=(vector,) * 5,
        scratch_shapes=[
            pltpu.VMEM(flow.shape, jnp.float32),
            pltpu.VMEM((2, 4, tall, wall), jnp.float32),
            pltpu.VMEM((2, 4, wide, wall), jnp.float32),
            pltpu.VMEM((2, 4, wide, wall), jnp.float32),
            dma((6,)), dma((4,)), dma((4,)), dma((2, 3, 4)), dma((2, 3, 4)), dma((2, 3)),
            dma((2, 3)), dma((2, 3, 2, 3)), dma((2, 3, 2, 3)),
        ],
        compiler_params=pltpu.CompilerParams(
            collective_id=0, has_side_effects=True, vmem_limit_bytes=12 << 20
        ),
        name="front",
    )(*(pltpu.with_memory_space_constraint(each, pltpu.HBM) for each in (flow, cells, fracs)))


def dot(a, b, across):
    return lax.dot_general(
        a, b, (((1,), (across,)), ((), ())), preferred_element_type=jnp.float32
    )


def pair(a, b, across):
    rows = a[0].shape[0]
    both = dot(jnp.concatenate(a), b[0], across)
    return both[:rows] + both[rows:] + dot(a[0], b[1], across)


def marker_kernel(
    nx, nz, ids, corners, moving, turning, cells, fracs, tap, field, cross, force
):
    force[...] = jnp.zeros_like(force)
    markers = fracs.shape[2]
    wall = field.shape[3]
    wide, tall = field.shape[1] - 2 * HALF, field.shape[2] - 2 * SIDE
    first_x = lax.axis_index("gx") * wide - HALF
    first_z = lax.axis_index("gz") * tall - SIDE
    many = wall // BAND
    lane = lax.broadcasted_iota(jnp.int32, (1, 1, wall), 2)

    def one_slot(s, carry):
        if True:
            n = lax.max(ids[s], 0)
            living = jnp.where(ids[s] >= 0, 1.0, 0.0)
            x0 = lax.rem(corners[0, s] - first_x + wide * nx, wide * nx)
            y0 = corners[1, s]
            z0 = lax.rem(corners[2, s] - first_z + tall * nz, tall * nz)
            zb = pl.multiple_of((z0 // 8) * 8, 8)
            cell = cells[:, pl.ds(s, 1), :].reshape(3, markers)
            frac = fracs[:, pl.ds(s, 1), :].reshape(3, markers)
            taps = [tap[t, :, pl.ds(s, 1), :].reshape(3, markers) for t in range(4)]

            weight_z = tap_weights(BAND, cell[2:3] - 1 + (z0 - zb), [w[2:3] for w in taps])
            columns = []
            for q in range(BOX // many):
                packed = None
                for r in range(many):
                    piece = field[:, x0 + (q * many + r), pl.ds(zb, BAND), :]
                    piece = pltpu.roll(piece, lax.rem(wall + r * BAND - y0, wall), 2)
                    packed = piece if r == 0 else jnp.where(lane < r * BAND, packed, piece)
                columns.append(packed.reshape(3 * BAND, wall))
            window = parts(jnp.concatenate(columns, axis=1))
            value = pair(window, (cross[s, 0], cross[s, 1]), 0).reshape(3, BAND, markers)
            sampled = jnp.sum(value * weight_z[None], axis=1)
            lever = cell.astype(jnp.float32) + frac - float(HALF)
            spin = [turning[c, n] for c in range(3)]
            loads = []
            for c in range(3):
                a, b = (c + 1) % 3, (c + 2) % 3
                target = moving[c, n] + (spin[a] * lever[b : b + 1] - spin[b] * lever[a : a + 1])
                loads.append((living * (target - sampled[c : c + 1])) * weight_z)
            load = parts(jnp.concatenate(loads))
            value = pair(load, (cross[s, 0], cross[s, 1]), 1).reshape(3, BAND, BOX * BAND)
            inside = (lane >= y0) & (lane < y0 + BOX)
            for i in range(BOX):
                q, r = i // many, i % many
                piece = value[:, :, q * wall : (q + 1) * wall]
                piece = pltpu.roll(piece, lax.rem(wall + y0 - r * BAND, wall), 2)
                force[:, x0 + i, pl.ds(zb, BAND), :] += jnp.where(inside, piece, 0.0)

        return carry

    def four_slots(h, carry):
        for k in range(4):
            one_slot(4 * h + k, carry)
        return carry

    lax.fori_loop(0, ids.shape[0] // 4, four_slots, 0)


def spread_forces(nx, nz, extended, cross, tap, slot_ids, corners, cells, fracs, moving, turning):
    scalar = pl.BlockSpec(memory_space=pltpu.SMEM)
    vector = pl.BlockSpec(memory_space=pltpu.VMEM)
    scalars = [
        pltpu.with_memory_space_constraint(each, pltpu.HBM)
        for each in (slot_ids, corners, moving, turning)
    ]
    return pl.pallas_call(
        functools.partial(marker_kernel, nx, nz),
        out_shape=jax.ShapeDtypeStruct(extended.shape, jnp.float32),
        in_specs=[scalar] * 4 + [vector] * 5,
        out_specs=vector,
        compiler_params=pltpu.CompilerParams(vmem_limit_bytes=16 << 20),
        name="markers",
    )(*scalars, cells, fracs, tap, extended, cross)


def exchanged(rows, lane_bits):
    lane = lax.broadcasted_iota(jnp.int32, rows[0].shape, rows[0].ndim - 1)
    axis = rows[0].ndim - 1
    for bit, shift in enumerate(lane_bits):
        low = (lane & shift) == 0
        step = 1 << bit
        out = list(rows)
        for m in range(len(rows)):
            if m & step == 0:
                a, b = rows[m], rows[m + step]
                out[m] = jnp.where(low, a, pltpu.roll(b, shift, axis))
                out[m + step] = jnp.where(low, pltpu.roll(a, 128 - shift, axis), b)
        rows = out
    return rows


def spectrum_kernel(
    nx, nz, force, field, table_z, velocity, rows,
    z_got, x_out, x_got, u_out, u_got, row_out, row_got, row_sum, rim_out, rim_got, edge_u,
    edge_w, cut, planes, modes,
    z_send, z_recv, x_send, x_recv, e_send, e_recv, c_send, c_recv, m_send, m_recv,
):
    gx, gz = lax.axis_index("gx"), lax.axis_index("gz")
    left, right, below, above = around(nx, nz)
    barrier = pltpu.get_barrier_semaphore()

    def greet_z(d, carry):
        pl.semaphore_signal(
            barrier, inc=1, device_id=(gx, lax.rem(gz + d, nz)), device_id_type=MESH
        )
        return carry

    def greet_x(d, carry):
        pl.semaphore_signal(
            barrier, inc=1, device_id=(lax.rem(gx + d, nx), gz), device_id_type=MESH
        )
        return carry

    lax.fori_loop(1, nx, greet_x, 0)
    lax.fori_loop(1, nz, greet_z, 0)
    wide, tall = velocity.shape[1], velocity.shape[2]
    blank = jnp.zeros(z_got.shape[1:3] + (SIDE - HALF, z_got.shape[4]), jnp.float32)
    z_got[0, :, :, pl.ds(HALF, SIDE - HALF), :] = blank
    z_got[1, :, :, pl.ds(0, SIDE - HALF), :] = blank
    row_out[0] = force[2, :, SIDE, :]
    row_out[1] = force[2, :, SIDE + tall - 1, :]
    pl.semaphore_wait(barrier, nx + nz - 2)

    order = (0, 2, 1)
    own = pl.ds(HALF, wide)
    pieces = (pl.ds(0, HALF), pl.ds(HALF + wide, HALF), own)

    def fold_z(c, piece):
        columns = pieces[piece]
        down = remote(
            force.at[c, columns, pl.ds(SIDE - HALF, HALF), :],
            z_got.at[1, c, columns, pl.ds(SIDE - HALF, HALF), :],
            (z_send, z_recv), (1, c, piece), below,
        )
        up = remote(
            force.at[c, columns, pl.ds(SIDE + tall, HALF), :],
            z_got.at[0, c, columns, pl.ds(0, HALF), :],
            (z_send, z_recv), (0, c, piece), above,
        )
        down.start()
        up.start()
        return [down, up]

    rims, inner = {}, {}
    rims[0] = fold_z(0, 0) + fold_z(0, 1)
    lines = [
        remote(row_out.at[0], row_got.at[1], (e_send, e_recv), 0, below),
        remote(row_out.at[1], row_got.at[0], (e_send, e_recv), 1, above),
    ]
    x_copies = {}
    for c in order:
        for copy in rims[c]:
            copy.wait_recv()
        if c == 0:
            rims[2] = fold_z(2, 0) + fold_z(2, 1)
            for copy in lines:
                copy.start()
            inner[0] = fold_z(0, 2)
        if c == 2:
            rims[1] = fold_z(1, 0) + fold_z(1, 1)
            inner[2] = fold_z(2, 2)
            inner[1] = fold_z(1, 2)
        for part in range(2):
            inside = pl.ds(part * SIDE, SIDE)
            outside = pl.ds(SIDE + part * SIDE, SIDE)
            for side in range(2):
                x_out[side, c, :, inside, :] = (
                    force[c, pieces[side], outside, :] + z_got[part, c, pieces[side]]
                )
        back = remote(x_out.at[0, c], x_got.at[1, c], (x_send, x_recv), (1, c), left)
        ahead = remote(x_out.at[1, c], x_got.at[0, c], (x_send, x_recv), (0, c), right)
        back.start()
        ahead.start()
        x_copies[c] = [back, ahead]
        if c == 2:
            for copy in lines:
                copy.wait_recv()
            row_sum[0] = force[2, :, SIDE - 1, :] + row_got[0]
            row_sum[1] = force[2, :, SIDE + tall, :] + row_got[1]
            rim_out[0] = row_sum[:, pl.ds(0, HALF), :]
            rim_out[1] = row_sum[:, pl.ds(HALF + wide, HALF), :]
            ends = [
                remote(rim_out.at[0], rim_got.at[1], (e_send, e_recv), 2, left),
                remote(rim_out.at[1], rim_got.at[0], (e_send, e_recv), 3, right),
            ]
            for copy in ends:
                copy.start()
        if c == 0:
            for copy in inner[0]:
                copy.wait_recv()
            for part in range(2):
                inside = pl.ds(part * SIDE, SIDE)
                outside = pl.ds(SIDE + part * SIDE, SIDE)
                u_out[0, inside, :] = force[0, HALF, outside, :] + z_got[part, 0, HALF]
                u_out[1, inside, :] = (
                    force[0, HALF + wide - 1, outside, :] + z_got[part, 0, HALF + wide - 1]
                )
            layers = [
                remote(u_out.at[0], u_got.at[1], (e_send, e_recv), 4, left),
                remote(u_out.at[1], u_got.at[0], (e_send, e_recv), 5, right),
            ]
            for copy in layers:
                copy.start()
    for c in order:
        if c != 0:
            for copy in inner[c]:
                copy.wait_recv()
        for part in range(2):
            inside = pl.ds(part * SIDE, SIDE)
            outside = pl.ds(SIDE + part * SIDE, SIDE)
            velocity[c, :, inside, :] = (
                field[c, own, outside, :] + force[c, own, outside, :] + z_got[part, c, own]
            )
    for c in order:
        for copy in x_copies[c]:
            copy.wait_recv()
        velocity[c, pl.ds(0, HALF)] += x_got[0, c]
        velocity[c, pl.ds(wide - HALF, HALF)] += x_got[1, c]
        if c == 0:
            for copy in layers:
                copy.wait_recv()
            body = pl.ds(SIDE, tall)
            edge_u[0] = field[0, HALF - 1, body, :] + x_out[0, 0, HALF - 1] + u_got[0]
            edge_u[1] = field[0, HALF + wide, body, :] + x_out[1, 0, 0] + u_got[1]
        if c == 2:
            for copy in ends:
                copy.wait_recv()
            edge_w[0] = field[2, own, SIDE - 1, :] + row_sum[0, own, :]
            edge_w[1] = field[2, own, SIDE + tall, :] + row_sum[1, own, :]
            edge_w[:, pl.ds(0, HALF), :] += rim_got[0]
            edge_w[:, pl.ds(wide - HALF, HALF), :] += rim_got[1]
    edges = lines + ends + layers
    wall = velocity.shape[3]
    lane = lax.broadcasted_iota(jnp.int32, (1, 1, wall), 2)
    normal = velocity[1]
    upper = jnp.where(lane == wall - 1, 0.0, pltpu.roll(normal, wall - 1, 2))
    lower = jnp.where(lane == 0, 0.0, pltpu.roll(normal, 1, 2))
    divergence = upper - lower
    stream = velocity[0]
    divergence += jnp.concatenate([stream[1:], edge_u[1:2]], axis=0) - jnp.concatenate(
        [edge_u[0:1], stream[:-1]], axis=0
    )
    span = velocity[2]
    row = lax.broadcasted_iota(jnp.int32, (1, tall, 1), 1)
    after = jnp.where(row == tall - 1, edge_w[1][:, None, :], pltpu.roll(span, tall - 1, 1))
    before = jnp.where(row == 0, edge_w[0][:, None, :], pltpu.roll(span, 1, 1))
    divergence = (divergence + (after - before)) * 0.5
    for half in range(wide // 8):
        blocks = exchanged([divergence[half * 8 + i] for i in range(8)], (16, 32, 64))
        for j in range(nz):
            cut[j, :, pl.ds(half * 128, 128)] = blocks[j]

    def cut_copy(d):
        to = lax.rem(gz + d, nz)
        return pltpu.make_async_remote_copy(
            src_ref=cut.at[to],
            dst_ref=planes.at[gz],
            send_sem=c_send.at[to],
            recv_sem=c_recv.at[gz],
            device_id=(gx, to),
            device_id_type=MESH,
        )

    def cut_from(d):
        origin = lax.rem(gz + d, nz)
        return pltpu.make_async_remote_copy(
            src_ref=cut.at[origin],
            dst_ref=planes.at[origin],
            send_sem=c_send.at[origin],
            recv_sem=c_recv.at[origin],
            device_id=(gx, origin),
            device_id_type=MESH,
        )

    def start(make):
        def go(d, carry):
            make(d).start()
            return carry

        return go

    def wait_recv(make):
        def go(d, carry):
            make(d).wait_recv()
            return carry

        return go

    def wait_send(make):
        def go(d, carry):
            make(d).wait_send()
            return carry

        return go

    lax.fori_loop(1, nz, start(cut_copy), 0)
    planes[gz] = cut[gz]
    lax.fori_loop(1, nz, wait_recv(cut_from), 0)
    high, low = parts(planes[...].reshape(nz * tall, 2 * 128))
    modes[...] = pair((table_z[0], table_z[1]), (high, low), 0).reshape(modes.shape)

    deep = nx // 8
    deep_at, along_at = lax.div(gx, 8), lax.rem(gx, 8)

    def partner(t):
        k, j = lax.div(t, deep), lax.rem(t, deep)
        odd = lax.rem(k, 2)
        step = 4 - odd + lax.div(k, 2) * (1 - 2 * odd)
        return lax.rem(deep_at + j + 1, deep) * 8 + lax.rem(along_at + step, 8)

    def mode_copy(t):
        to = partner(t)
        return pltpu.make_async_remote_copy(
            src_ref=modes.at[:, to],
            dst_ref=rows.at[gx],
            send_sem=m_send.at[to],
            recv_sem=m_recv.at[gx],
            device_id=(to, gz),
            device_id_type=MESH,
        )

    def mode_from(t):
        origin = partner(t)
        return pltpu.make_async_remote_copy(
            src_ref=modes.at[:, origin],
            dst_ref=rows.at[origin],
            send_sem=m_send.at[origin],
            recv_sem=m_recv.at[origin],
            device_id=(origin, gz),
            device_id_type=MESH,
        )

    lax.fori_loop(0, nx - 1, start(mode_copy), 0)
    rows[gx] = modes[:, gx]
    lax.fori_loop(0, nx - 1, wait_recv(mode_from), 0)
    for c in order:
        for copy in rims[c] + inner[c] + x_copies[c]:
            copy.wait_send()
    for copy in edges:
        copy.wait_send()
    lax.fori_loop(1, nz, wait_send(cut_copy), 0)
    lax.fori_loop(0, nx - 1, wait_send(mode_copy), 0)


def finish_kernel(scale, velocity_in, rows, table_x, velocity, source, held, sems):
    through = pltpu.make_async_copy(velocity_in, velocity, sems.at[0])
    through.start()
    columns = []
    for h in range(rows.shape[0] // 16):
        for half in range(2):
            blocks = exchanged(
                [rows[h * 16 + b, :, :, half * 128 : half * 128 + 128] for b in range(16)],
                (1, 2, 4, 8),
            )
            columns.append(
                jnp.concatenate([block[0] for block in blocks] + [block[1] for block in blocks])
            )
    high, low = parts(jnp.concatenate(columns, axis=1))
    lines = high.shape[0] // 2
    copies = [through]
    for q in range(table_x.shape[1]):
        value = pair((high, low), (table_x[0, q], table_x[1, q]), 0)
        real = value[:lines, :128] + value[lines:, 128:]
        imag = value[lines:, :128] - value[:lines, 128:]
        out = pl.ds(q * 128, 128)
        held[0, :, :, out] = (real * scale).reshape(held.shape[1], held.shape[2], 128)
        held[1, :, :, out] = (imag * scale).reshape(held.shape[1], held.shape[2], 128)
        copy = pltpu.make_async_copy(
            held.at[:, :, :, out], source.at[:, :, :, out], sems.at[1 + q]
        )
        copy.start()
        copies.append(copy)
    for copy in copies:
        copy.wait()


def split_table(table):
    high = table.astype(jnp.bfloat16)
    return np.stack([high, (table - high.astype(np.float64)).astype(jnp.bfloat16)])


def transform_tables(length_x, length_z):
    counter = np.arange(length_z)
    angle = counter[:, None] * counter[None, :] % length_z * (2 * math.pi / length_z)
    table_z = np.concatenate([np.cos(angle), -np.sin(angle)])
    h, half, i, b = np.meshgrid(
        np.arange(length_x // 256), np.arange(2), np.arange(8), np.arange(16), indexing="ij"
    )
    place = (16 * (16 * h + b) + 8 * half + i).reshape(-1)
    mode = np.arange(length_x)
    angle = place[:, None] * mode[None, :] % length_x * (2 * math.pi / length_x)
    both = np.stack([np.cos(angle), np.sin(angle)], axis=1)
    both = both.reshape(length_x, 2, length_x // 128, 128).transpose(2, 0, 1, 3)
    return split_table(table_z), split_table(both.reshape(length_x // 128, length_x, 256))


def spectrum(force, field, tile, nx, nz):
    _, wide, tall, wall = tile
    length_x, length_z = wide * nx, tall * nz
    table_z, table_x = transform_tables(length_x, length_z)
    vector = pl.BlockSpec(memory_space=pltpu.VMEM)
    dma = pltpu.SemaphoreType.DMA
    each = wall // nz
    deep = field.shape[1]
    modes = length_z // nx
    velocity, rows = pl.pallas_call(
        functools.partial(spectrum_kernel, nx, nz),
        out_shape=(
            jax.ShapeDtypeStruct(tile, jnp.float32),
            jax.ShapeDtypeStruct((nx, 2, modes, wide * each), jnp.float32),
        ),
        in_specs=[vector] * 3,
        out_specs=(vector, vector),
        scratch_shapes=[
            pltpu.VMEM((2, 3, deep, SIDE, wall), jnp.float32),
            pltpu.VMEM((2, 3, HALF, tall, wall), jnp.float32),
            pltpu.VMEM((2, 3, HALF, tall, wall), jnp.float32),
            pltpu.VMEM((2, tall, wall), jnp.float32),
            pltpu.VMEM((2, tall, wall), jnp.float32),
            pltpu.VMEM((2, deep, wall), jnp.float32),
            pltpu.VMEM((2, deep, wall), jnp.float32),
            pltpu.VMEM((2, deep, wall), jnp.float32),
            pltpu.VMEM((2, 2, HALF, wall), jnp.float32),
            pltpu.VMEM((2, 2, HALF, wall), jnp.float32),
            pltpu.VMEM((2, tall, wall), jnp.float32),
            pltpu.VMEM((2, wide, wall), jnp.float32),
            pltpu.VMEM((nz, tall, wide * each), jnp.float32),
            pltpu.VMEM((nz, tall, wide * each), jnp.float32),
            pltpu.VMEM((2, nx, modes, wide * each), jnp.float32),
            dma((2, 3, 3)), dma((2, 3, 3)), dma((2, 3)), dma((2, 3)), dma((6,)), dma((6,)),
            dma((nz,)), dma((nz,)), dma((nx,)), dma((nx,)),
        ],
        compiler_params=pltpu.CompilerParams(
            collective_id=1, has_side_effects=True, vmem_limit_bytes=28 << 20
        ),
        name="spectrum",
    )(force, field, jnp.asarray(table_z))
    shape = (2, each, modes, length_x)
    return pl.pallas_call(
        functools.partial(finish_kernel, 1.0 / math.sqrt(length_x * length_z)),
        out_shape=(
            jax.ShapeDtypeStruct(tile, jnp.float32),
            jax.ShapeDtypeStruct(shape, jnp.float32),
        ),
        in_specs=[vector] * 3,
        out_specs=(pl.BlockSpec(memory_space=pltpu.HBM), pl.BlockSpec(memory_space=pltpu.HBM)),
        scratch_shapes=[
            pltpu.VMEM(shape, jnp.float32),
            dma((1 + length_x // 128,)),
        ],
        compiler_params=pltpu.CompilerParams(vmem_limit_bytes=16 << 20),
        name="finish",
    )(velocity, rows, jnp.asarray(table_x))


def on_device(
    nx, nz, flow_state, slot_ids, corners, marker_cells, marker_frac, particle_velocity,
    particle_spin,
):
    extended, cross, tap, cells, fracs = predict(flow_state, marker_cells, marker_frac, nx, nz)
    force = spread_forces(
        nx,
        nz,
        extended,
        cross,
        tap,
        slot_ids,
        corners,
        cells,
        fracs,
        particle_velocity,
        particle_spin,
    )
    return spectrum(force, extended, (3,) + flow_state.shape[1:], nx, nz)


def solution(mesh):
    both = ("gx", "gz")
    placed = (
        P(None, "gx", "gz", None),
        P(both),
        P(None, both),
        P(None, both, None),
        P(None, both, None),
        P(),
        P(),
    )
    return jax.shard_map(
        functools.partial(on_device, mesh.shape["gx"], mesh.shape["gz"]),
        mesh=mesh,
        in_specs=placed,
        out_specs=(P(None, "gx", "gz", None), P(None, "gz", "gx", None)),
        check_vma=False,
    )
```

```python
import functools
import math

import jax
import jax.numpy as jnp
import numpy as np
from jax import lax
from jax.experimental import pallas as pl
from jax.experimental.pallas import tpu as pltpu
from jax.sharding import PartitionSpec as P

BOX = 24
HALF = 12
BAND = 32
SIDE = 16
MESH = pl.DeviceIdType.MESH


time_step = 0.1
viscosity = 0.2
drive_force = 1.0


def remote(source, target, sems, slot, to):
    return pltpu.make_async_remote_copy(
        src_ref=source,
        dst_ref=target,
        send_sem=sems[0].at[slot],
        recv_sem=sems[1].at[slot],
        device_id=to,
        device_id_type=MESH,
    )


def around(nx, nz):
    gx, gz = lax.axis_index("gx"), lax.axis_index("gz")
    return (
        (lax.rem(gx + nx - 1, nx), gz),
        (lax.rem(gx + 1, nx), gz),
        (gx, lax.rem(gz + nz - 1, nz)),
        (gx, lax.rem(gz + 1, nz)),
    )


def parts(value):
    high = value.astype(jnp.bfloat16)
    return high, (value - high.astype(jnp.float32)).astype(jnp.bfloat16)


def tap_weights(length, first, taps):
    offset = lax.broadcasted_iota(jnp.int32, (length, first.shape[-1]), 0) - first
    weight = jnp.where(offset == 3, taps[3], 0.0)
    for t in (2, 1, 0):
        weight = jnp.where(offset == t, taps[t], weight)
    return weight


def fill_taps(fracs, tap):
    angle = fracs[...] * (0.5 * math.pi)
    cosine, sine = jnp.cos(angle), jnp.sin(angle)
    tap[0] = 0.25 * (1.0 - sine)
    tap[1] = 0.25 * (1.0 + cosine)
    tap[2] = 0.25 * (1.0 + sine)
    tap[3] = 0.25 * (1.0 - cosine)


def cross_weights(cells, fracs, tap, cross):
    fill_taps(fracs, tap)
    markers = fracs.shape[2]

    def one_slot(s, carry):
        cell = cells[:, pl.ds(s, 1), :].reshape(3, markers)
        taps = [tap[t, :, pl.ds(s, 1), :].reshape(3, markers) for t in range(4)]
        weight_x = tap_weights(BOX, cell[0:1] - 1, [w[0:1] for w in taps])
        weight_y = tap_weights(BAND, cell[1:2] - 1, [w[1:2] for w in taps])
        for i in range(BOX):
            high, low = parts(weight_x[i : i + 1] * weight_y)
            cross[s, 0, pl.ds(i * BAND, BAND), :] = high
            cross[s, 1, pl.ds(i * BAND, BAND), :] = low
        return carry

    lax.fori_loop(0, cells.shape[1], one_slot, 0)


def front_kernel(
    nx, nz, flow_in, cells_in, fracs_in, field, cross, tap, cells, fracs, flow, edge_x, edge_z_out, edge_z,
    f_sem, e_send, e_recv, x_send, x_recv, z_send, z_recv, r_send, r_recv,
):
    _, wide, tall, wall = flow.shape
    left, right, below, above = around(nx, nz)
    barrier = pltpu.get_barrier_semaphore()
    for near in (left, right, below, above):
        pl.semaphore_signal(barrier, inc=1, device_id=near, device_id_type=MESH)
    loads = [pltpu.make_async_copy(flow_in.at[c], flow.at[c], f_sem.at[c]) for c in range(4)]
    lists = [
        pltpu.make_async_copy(cells_in, cells, f_sem.at[4]),
        pltpu.make_async_copy(fracs_in, fracs, f_sem.at[5]),
    ]
    for load in loads + lists:
        load.start()
    pl.semaphore_wait(barrier, 4)
    for load in loads:
        load.wait()
    edge_z_out[0] = flow[:, :, 0, :]
    edge_z_out[1] = flow[:, :, tall - 1, :]
    edges = [
        remote(flow.at[:, 0], edge_x.at[1], (e_send, e_recv), 0, left),
        remote(flow.at[:, wide - 1], edge_x.at[0], (e_send, e_recv), 1, right),
        remote(edge_z_out.at[0], edge_z.at[1], (e_send, e_recv), 2, below),
        remote(edge_z_out.at[1], edge_z.at[0], (e_send, e_recv), 3, above),
    ]
    for copy in edges:
        copy.start()
    spread = time_step * viscosity
    carry_by = 0.5 * time_step
    lane = lax.broadcasted_iota(jnp.int32, (tall, wall), 1)
    row = lax.broadcasted_iota(jnp.int32, (tall, wall), 0)
    first_y, last_y = lane == 0, lane == wall - 1
    first_z, last_z = row == 0, row == tall - 1

    def layer(x, back, ahead):
        here = [flow[c, x] for c in range(4)]
        moves = [carry_by * here[d] for d in range(3)]
        for c in range(3):
            f = here[c]
            total = f * (1.0 - 6.0 * spread)
            y_plus = jnp.where(last_y, 0.0, pltpu.roll(f, wall - 1, 1))
            y_minus = jnp.where(first_y, 0.0, pltpu.roll(f, 1, 1))
            z_plus = jnp.where(last_z, 0.0, pltpu.roll(f, tall - 1, 0))
            z_minus = jnp.where(first_z, 0.0, pltpu.roll(f, 1, 0))
            for plus, minus, move in (
                (ahead[c], back[c], moves[0]),
                (y_plus, y_minus, moves[1]),
                (z_plus, z_minus, moves[2]),
            ):
                total += plus * (spread - move) + minus * (spread + move)
            p = here[3]
            if c == 0:
                total += time_step * drive_force - carry_by * (ahead[3] - back[3])
            if c == 1:
                p_plus = jnp.where(last_y, p, pltpu.roll(p, wall - 1, 1))
                p_minus = jnp.where(first_y, p, pltpu.roll(p, 1, 1))
                total -= carry_by * (p_plus - p_minus)
            if c == 2:
                p_plus = jnp.where(last_z, 0.0, pltpu.roll(p, tall - 1, 0))
                p_minus = jnp.where(first_z, 0.0, pltpu.roll(p, 1, 0))
                total -= carry_by * (p_plus - p_minus)
            field[c, HALF + x, pl.ds(SIDE, tall), :] = total

    def inside(x, carry):
        layer(x, [flow[c, x - 1] for c in range(4)], [flow[c, x + 1] for c in range(4)])
        return carry

    lax.fori_loop(1, wide - 1, inside, 0)
    rim = HALF - 1
    half = SIDE // 2
    spans = (
        {0: (1, rim), 1: (0, 1), 2: (0, HALF), 3: (0, HALF)},
        {0: (0, rim), 1: (rim, 1), 2: (0, HALF), 3: (0, HALF)},
    )
    lines = {0: (half, SIDE), 1: (half, SIDE), 2: (0, half), 3: (tall - half, half)}
    x_copies, z_copies = {}, []

    def send(c, piece):
        for side in range(2):
            first, count = spans[side][piece]
            at, height = lines[piece]
            source, target = ((HALF, HALF + wide), (wide, 0))[side]
            rows = pl.ds(SIDE + at, height)
            copy = remote(
                field.at[c, pl.ds(source + first, count), rows],
                field.at[c, pl.ds(target + first, count), rows],
                (x_send, x_recv), (side, c, piece), (left, right)[side],
            )
            copy.start()
            x_copies[c, piece, side] = copy

    def forward(c, piece, side):
        first, count = spans[side][piece]
        columns = pl.ds((HALF + wide, 0)[side] + first, count)
        at, height = lines[piece]
        slot = min(piece, 2)
        if piece != 3:
            count = min(at + height, HALF) - at
            copy = remote(
                field.at[c, columns, pl.ds(SIDE + at, count)],
                field.at[c, columns, pl.ds(SIDE + tall + at, count)],
                (r_send, r_recv), (0, c, side, slot), below,
            )
            copy.start()
            z_copies.append(copy)
        if piece != 2:
            start = max(at, tall - HALF)
            count = at + height - start
            copy = remote(
                field.at[c, columns, pl.ds(SIDE + start, count)],
                field.at[c, columns, pl.ds(SIDE + start - tall, count)],
                (r_send, r_recv), (1, c, side, slot), above,
            )
            copy.start()
            z_copies.append(copy)

    for c in range(3):
        send(c, 0)
    for copy in edges:
        copy.wait_recv()
    layer(0, [edge_x[0, c] for c in range(4)], [flow[c, 1] for c in range(4)])
    layer(
        wide - 1, [flow[c, wide - 2] for c in range(4)], [edge_x[1, c] for c in range(4)]
    )
    own = pl.ds(HALF, wide)
    for c in range(3):
        for side, z, sign in ((0, 0, 1.0), (1, tall - 1, -1.0)):
            move = carry_by * edge_z_out[side, 2]
            add = edge_z[side, c] * (spread + sign * move)
            if c == 2:
                add += sign * carry_by * edge_z[side, 3]
            field[c, own, SIDE + z, :] += add
        for piece in (2, 3, 1):
            send(c, piece)
    for c in range(3):
        down = remote(
            field.at[c, own, pl.ds(SIDE, HALF)],
            field.at[c, own, pl.ds(SIDE + tall, HALF)],
            (z_send, z_recv), (0, c), below,
        )
        up = remote(
            field.at[c, own, pl.ds(SIDE + tall - HALF, HALF)],
            field.at[c, own, pl.ds(SIDE - HALF, HALF)],
            (z_send, z_recv), (1, c), above,
        )
        down.start()
        up.start()
        z_copies.extend((down, up))
    blank = jnp.zeros(field.shape[:2] + (SIDE - HALF, wall), jnp.float32)
    field[:, :, pl.ds(0, SIDE - HALF), :] = blank
    field[:, :, pl.ds(SIDE + tall + HALF, SIDE - HALF), :] = blank
    for load in lists:
        load.wait()
    cross_weights(cells, fracs, tap, cross)
    for c, piece in [(c, 0) for c in range(3)] + [(c, p) for c in range(3) for p in (2, 3, 1)]:
        for side in range(2):
            x_copies[c, piece, side].wait_recv()
            forward(c, piece, side)
    for copy in z_copies:
        copy.wait_recv()
    for copy in edges + z_copies + list(x_copies.values()):
        copy.wait_send()


def predict(flow, cells, fracs, nx, nz):
    _, wide, tall, wall = flow.shape
    _, slots, markers = cells.shape
    vector = pl.BlockSpec(memory_space=pltpu.VMEM)
    dma = pltpu.SemaphoreType.DMA
    return pl.pallas_call(
        functools.partial(front_kernel, nx, nz),
        out_shape=(
            jax.ShapeDtypeStruct(
                (3, wide + 2 * HALF, tall + 2 * SIDE, wall), jnp.float32
            ),
            jax.ShapeDtypeStruct((slots, 2, BOX * BAND, markers), jnp.bfloat16),
            jax.ShapeDtypeStruct((4,) + cells.shape, jnp.float32),
            jax.ShapeDtypeStruct(cells.shape, jnp.int32),
            jax.ShapeDtypeStruct(cells.shape, jnp.float32),
        ),
        in_specs=[pl.BlockSpec(memory_space=pltpu.HBM)] * 3,
        out_specs=(vector,) * 5,
        scratch_shapes=[
            pltpu.VMEM(flow.shape, jnp.float32),
            pltpu.VMEM((2, 4, tall, wall), jnp.float32),
            pltpu.VMEM((2, 4, wide, wall), jnp.float32),
            pltpu.VMEM((2, 4, wide, wall), jnp.float32),
            dma((6,)), dma((4,)), dma((4,)), dma((2, 3, 4)), dma((2, 3, 4)), dma((2, 3)),
            dma((2, 3)), dma((2, 3, 2, 3)), dma((2, 3, 2, 3)),
        ],
        compiler_params=pltpu.CompilerParams(
            collective_id=0, has_side_effects=True, vmem_limit_bytes=12 << 20
        ),
        name="front",
    )(*(pltpu.with_memory_space_constraint(each, pltpu.HBM) for each in (flow, cells, fracs)))


def dot(a, b, across):
    return lax.dot_general(
        a, b, (((1,), (across,)), ((), ())), preferred_element_type=jnp.float32
    )


def pair(a, b, across):
    rows = a[0].shape[0]
    both = dot(jnp.concatenate(a), b[0], across)
    return both[:rows] + both[rows:] + dot(a[0], b[1], across)


def marker_kernel(
    nx, nz, ids, corners, moving, turning, cells, fracs, tap, field, cross, force
):
    force[...] = jnp.zeros_like(force)
    markers = fracs.shape[2]
    wall = field.shape[3]
    wide, tall = field.shape[1] - 2 * HALF, field.shape[2] - 2 * SIDE
    first_x = lax.axis_index("gx") * wide - HALF
    first_z = lax.axis_index("gz") * tall - SIDE
    many = wall // BAND
    lane = lax.broadcasted_iota(jnp.int32, (1, 1, wall), 2)

    def one_slot(s, carry):
        if True:
            n = lax.max(ids[s], 0)
            living = jnp.where(ids[s] >= 0, 1.0, 0.0)
            x0 = lax.rem(corners[0, s] - first_x + wide * nx, wide * nx)
            y0 = corners[1, s]
            z0 = lax.rem(corners[2, s] - first_z + tall * nz, tall * nz)
            zb = pl.multiple_of((z0 // 8) * 8, 8)
            cell = cells[:, pl.ds(s, 1), :].reshape(3, markers)
            frac = fracs[:, pl.ds(s, 1), :].reshape(3, markers)
            taps = [tap[t, :, pl.ds(s, 1), :].reshape(3, markers) for t in range(4)]

            weight_z = tap_weights(BAND, cell[2:3] - 1 + (z0 - zb), [w[2:3] for w in taps])
            columns = []
            for q in range(BOX // many):
                packed = None
                for r in range(many):
                    piece = field[:, x0 + (q * many + r), pl.ds(zb, BAND), :]
                    piece = pltpu.roll(piece, lax.rem(wall + r * BAND - y0, wall), 2)
                    packed = piece if r == 0 else jnp.where(lane < r * BAND, packed, piece)
                columns.append(packed.reshape(3 * BAND, wall))
            window = parts(jnp.concatenate(columns, axis=1))
            value = pair(window, (cross[s, 0], cross[s, 1]), 0).reshape(3, BAND, markers)
            sampled = jnp.sum(value * weight_z[None], axis=1)
            lever = cell.astype(jnp.float32) + frac - float(HALF)
            spin = [turning[c, n] for c in range(3)]
            loads = []
            for c in range(3):
                a, b = (c + 1) % 3, (c + 2) % 3
                target = moving[c, n] + (spin[a] * lever[b : b + 1] - spin[b] * lever[a : a + 1])
                loads.append((living * (target - sampled[c : c + 1])) * weight_z)
            load = parts(jnp.concatenate(loads))
            value = pair(load, (cross[s, 0], cross[s, 1]), 1).reshape(3, BAND, BOX * BAND)
            inside = (lane >= y0) & (lane < y0 + BOX)
            for i in range(BOX):
                q, r = i // many, i % many
                piece = value[:, :, q * wall : (q + 1) * wall]
                piece = pltpu.roll(piece, lax.rem(wall + y0 - r * BAND, wall), 2)
                force[:, x0 + i, pl.ds(zb, BAND), :] += jnp.where(inside, piece, 0.0)

        return carry

    def four_slots(h, carry):
        for k in range(4):
            one_slot(4 * h + k, carry)
        return carry

    lax.fori_loop(0, ids.shape[0] // 4, four_slots, 0)


def spread_forces(nx, nz, extended, cross, tap, slot_ids, corners, cells, fracs, moving, turning):
    scalar = pl.BlockSpec(memory_space=pltpu.SMEM)
    vector = pl.BlockSpec(memory_space=pltpu.VMEM)
    scalars = [
        pltpu.with_memory_space_constraint(each, pltpu.HBM)
        for each in (slot_ids, corners, moving, turning)
    ]
    return pl.pallas_call(
        functools.partial(marker_kernel, nx, nz),
        out_shape=jax.ShapeDtypeStruct(extended.shape, jnp.float32),
        in_specs=[scalar] * 4 + [vector] * 5,
        out_specs=vector,
        compiler_params=pltpu.CompilerParams(vmem_limit_bytes=16 << 20),
        name="markers",
    )(*scalars, cells, fracs, tap, extended, cross)


def exchanged(rows, lane_bits):
    lane = lax.broadcasted_iota(jnp.int32, rows[0].shape, rows[0].ndim - 1)
    axis = rows[0].ndim - 1
    for bit, shift in enumerate(lane_bits):
        low = (lane & shift) == 0
        step = 1 << bit
        out = list(rows)
        for m in range(len(rows)):
            if m & step == 0:
                a, b = rows[m], rows[m + step]
                out[m] = jnp.where(low, a, pltpu.roll(b, shift, axis))
                out[m + step] = jnp.where(low, pltpu.roll(a, 128 - shift, axis), b)
        rows = out
    return rows


def spectrum_kernel(
    nx, nz, force, field, table_z, velocity, rows,
    z_got, x_out, x_got, u_out, u_got, row_out, row_got, row_sum, rim_out, rim_got, edge_u,
    edge_w, cut, planes, modes,
    z_send, z_recv, x_send, x_recv, e_send, e_recv, c_send, c_recv, m_send, m_recv,
):
    gx, gz = lax.axis_index("gx"), lax.axis_index("gz")
    left, right, below, above = around(nx, nz)
    barrier = pltpu.get_barrier_semaphore()

    def greet_z(d, carry):
        pl.semaphore_signal(
            barrier, inc=1, device_id=(gx, lax.rem(gz + d, nz)), device_id_type=MESH
        )
        return carry

    def greet_x(d, carry):
        pl.semaphore_signal(
            barrier, inc=1, device_id=(lax.rem(gx + d, nx), gz), device_id_type=MESH
        )
        return carry

    lax.fori_loop(1, nx, greet_x, 0)
    lax.fori_loop(1, nz, greet_z, 0)
    wide, tall = velocity.shape[1], velocity.shape[2]
    blank = jnp.zeros(z_got.shape[1:3] + (SIDE - HALF, z_got.shape[4]), jnp.float32)
    z_got[0, :, :, pl.ds(HALF, SIDE - HALF), :] = blank
    z_got[1, :, :, pl.ds(0, SIDE - HALF), :] = blank
    row_out[0] = force[2, :, SIDE, :]
    row_out[1] = force[2, :, SIDE + tall - 1, :]
    pl.semaphore_wait(barrier, nx + nz - 2)

    order = (0, 2, 1)
    own = pl.ds(HALF, wide)
    pieces = (pl.ds(0, HALF), pl.ds(HALF + wide, HALF), own)

    def fold_z(c, piece):
        columns = pieces[piece]
        down = remote(
            force.at[c, columns, pl.ds(SIDE - HALF, HALF), :],
            z_got.at[1, c, columns, pl.ds(SIDE - HALF, HALF), :],
            (z_send, z_recv), (1, c, piece), below,
        )
        up = remote(
            force.at[c, columns, pl.ds(SIDE + tall, HALF), :],
            z_got.at[0, c, columns, pl.ds(0, HALF), :],
            (z_send, z_recv), (0, c, piece), above,
        )
        down.start()
        up.start()
        return [down, up]

    rims, inner = {}, {}
    rims[0] = fold_z(0, 0) + fold_z(0, 1)
    lines = [
        remote(row_out.at[0], row_got.at[1], (e_send, e_recv), 0, below),
        remote(row_out.at[1], row_got.at[0], (e_send, e_recv), 1, above),
    ]
    x_copies = {}

    def fold_x(c, source, columns, piece, start, count):
        lines_at = pl.ds(start, count)
        for side in range(2):
            copy = remote(
                source(side, c, columns[side], start, count),
                x_got.at[1 - side, c, :, lines_at, :],
                (x_send, x_recv), (1 - side, c, piece), (left, right)[side],
            )
            copy.start()
            x_copies.setdefault(c, []).append(copy)

    def from_force(side, c, columns, start, count):
        return force.at[c, columns, pl.ds(SIDE + start, count), :]

    def from_sums(side, c, columns, start, count):
        return x_out.at[side, c, :, pl.ds(start, count), :]

    for c in order:
        fold_x(c, from_force, pieces, 0, HALF, tall - 2 * HALF)
    for c in order:
        for copy in rims[c]:
            copy.wait_recv()
        if c == 0:
            rims[2] = fold_z(2, 0) + fold_z(2, 1)
            for copy in lines:
                copy.start()
            inner[0] = fold_z(0, 2)
        if c == 2:
            rims[1] = fold_z(1, 0) + fold_z(1, 1)
            inner[2] = fold_z(2, 2)
            inner[1] = fold_z(1, 2)
        for part in range(2):
            inside = pl.ds(part * SIDE, SIDE)
            outside = pl.ds(SIDE + part * SIDE, SIDE)
            for side in range(2):
                x_out[side, c, :, inside, :] = (
                    force[c, pieces[side], outside, :] + z_got[part, c, pieces[side]]
                )
        fold_x(c, from_sums, pieces, 1, 0, HALF)
        fold_x(c, from_sums, pieces, 2, tall - HALF, HALF)
        if c == 2:
            for copy in lines:
                copy.wait_recv()
            row_sum[0] = force[2, :, SIDE - 1, :] + row_got[0]
            row_sum[1] = force[2, :, SIDE + tall, :] + row_got[1]
            rim_out[0] = row_sum[:, pl.ds(0, HALF), :]
            rim_out[1] = row_sum[:, pl.ds(HALF + wide, HALF), :]
            ends = [
                remote(rim_out.at[0], rim_got.at[1], (e_send, e_recv), 2, left),
                remote(rim_out.at[1], rim_got.at[0], (e_send, e_recv), 3, right),
            ]
            for copy in ends:
                copy.start()
        if c == 0:
            for copy in inner[0]:
                copy.wait_recv()
            for part in range(2):
                inside = pl.ds(part * SIDE, SIDE)
                outside = pl.ds(SIDE + part * SIDE, SIDE)
                u_out[0, inside, :] = force[0, HALF, outside, :] + z_got[part, 0, HALF]
                u_out[1, inside, :] = (
                    force[0, HALF + wide - 1, outside, :] + z_got[part, 0, HALF + wide - 1]
                )
            layers = [
                remote(u_out.at[0], u_got.at[1], (e_send, e_recv), 4, left),
                remote(u_out.at[1], u_got.at[0], (e_send, e_recv), 5, right),
            ]
            for copy in layers:
                copy.start()
    for c in order:
        if c != 0:
            for copy in inner[c]:
                copy.wait_recv()
        for part in range(2):
            inside = pl.ds(part * SIDE, SIDE)
            outside = pl.ds(SIDE + part * SIDE, SIDE)
            velocity[c, :, inside, :] = (
                field[c, own, outside, :] + force[c, own, outside, :] + z_got[part, c, own]
            )
    for c in order:
        if c == 1:
            stream, span = velocity[0], velocity[2]
            divergence = jnp.concatenate([stream[1:], edge_u[1:2]], axis=0) - jnp.concatenate(
                [edge_u[0:1], stream[:-1]], axis=0
            )
            row = lax.broadcasted_iota(jnp.int32, (1, tall, 1), 1)
            after = jnp.where(
                row == tall - 1, edge_w[1][:, None, :], pltpu.roll(span, tall - 1, 1)
            )
            before = jnp.where(row == 0, edge_w[0][:, None, :], pltpu.roll(span, 1, 1))
            divergence += after - before
        for copy in x_copies[c]:
            copy.wait_recv()
        velocity[c, pl.ds(0, HALF)] += x_got[0, c]
        velocity[c, pl.ds(wide - HALF, HALF)] += x_got[1, c]
        if c == 0:
            for copy in layers:
                copy.wait_recv()
            body = pl.ds(SIDE, tall)
            edge_u[0] = field[0, HALF - 1, body, :] + x_out[0, 0, HALF - 1] + u_got[0]
            edge_u[1] = field[0, HALF + wide, body, :] + x_out[1, 0, 0] + u_got[1]
        if c == 2:
            for copy in ends:
                copy.wait_recv()
            edge_w[0] = field[2, own, SIDE - 1, :] + row_sum[0, own, :]
            edge_w[1] = field[2, own, SIDE + tall, :] + row_sum[1, own, :]
            edge_w[:, pl.ds(0, HALF), :] += rim_got[0]
            edge_w[:, pl.ds(wide - HALF, HALF), :] += rim_got[1]
    edges = lines + ends + layers
    wall = velocity.shape[3]
    lane = lax.broadcasted_iota(jnp.int32, (1, 1, wall), 2)
    normal = velocity[1]
    upper = jnp.where(lane == wall - 1, 0.0, pltpu.roll(normal, wall - 1, 2))
    lower = jnp.where(lane == 0, 0.0, pltpu.roll(normal, 1, 2))
    divergence = (divergence + (upper - lower)) * 0.5
    for half in range(wide // 8):
        blocks = exchanged([divergence[half * 8 + i] for i in range(8)], (16, 32, 64))
        for j in range(nz):
            cut[j, :, pl.ds(half * 128, 128)] = blocks[j]

    def cut_copy(d):
        to = lax.rem(gz + d, nz)
        return pltpu.make_async_remote_copy(
            src_ref=cut.at[to],
            dst_ref=planes.at[gz],
            send_sem=c_send.at[to],
            recv_sem=c_recv.at[gz],
            device_id=(gx, to),
            device_id_type=MESH,
        )

    def cut_from(d):
        origin = lax.rem(gz + d, nz)
        return pltpu.make_async_remote_copy(
            src_ref=cut.at[origin],
            dst_ref=planes.at[origin],
            send_sem=c_send.at[origin],
            recv_sem=c_recv.at[origin],
            device_id=(gx, origin),
            device_id_type=MESH,
        )

    def start(make):
        def go(d, carry):
            make(d).start()
            return carry

        return go

    def wait_recv(make):
        def go(d, carry):
            make(d).wait_recv()
            return carry

        return go

    def wait_send(make):
        def go(d, carry):
            make(d).wait_send()
            return carry

        return go

    lax.fori_loop(1, nz, start(cut_copy), 0)
    planes[gz] = cut[gz]
    lax.fori_loop(1, nz, wait_recv(cut_from), 0)
    high, low = parts(planes[...].reshape(nz * tall, 2 * 128))
    modes[...] = pair((table_z[0], table_z[1]), (high, low), 0).reshape(modes.shape)

    deep = nx // 8
    deep_at, along_at = lax.div(gx, 8), lax.rem(gx, 8)

    def partner(t):
        k, j = lax.div(t, deep), lax.rem(t, deep)
        odd = lax.rem(k, 2)
        step = 4 - odd + lax.div(k, 2) * (1 - 2 * odd)
        return lax.rem(deep_at + j + 1, deep) * 8 + lax.rem(along_at + step, 8)

    def mode_copy(t):
        to = partner(t)
        return pltpu.make_async_remote_copy(
            src_ref=modes.at[:, to],
            dst_ref=rows.at[gx],
            send_sem=m_send.at[to],
            recv_sem=m_recv.at[gx],
            device_id=(to, gz),
            device_id_type=MESH,
        )

    def mode_from(t):
        origin = partner(t)
        return pltpu.make_async_remote_copy(
            src_ref=modes.at[:, origin],
            dst_ref=rows.at[origin],
            send_sem=m_send.at[origin],
            recv_sem=m_recv.at[origin],
            device_id=(origin, gz),
            device_id_type=MESH,
        )

    lax.fori_loop(0, nx - 1, start(mode_copy), 0)
    rows[gx] = modes[:, gx]
    lax.fori_loop(0, nx - 1, wait_recv(mode_from), 0)
    for c in order:
        for copy in rims[c] + inner[c] + x_copies[c]:
            copy.wait_send()
    for copy in edges:
        copy.wait_send()
    lax.fori_loop(1, nz, wait_send(cut_copy), 0)
    lax.fori_loop(0, nx - 1, wait_send(mode_copy), 0)


def finish_kernel(scale, velocity_in, rows, table_x, velocity, source, held, sems):
    through = pltpu.make_async_copy(velocity_in, velocity, sems.at[0])
    through.start()
    columns = []
    for h in range(rows.shape[0] // 16):
        for half in range(2):
            blocks = exchanged(
                [rows[h * 16 + b, :, :, half * 128 : half * 128 + 128] for b in range(16)],
                (1, 2, 4, 8),
            )
            columns.append(
                jnp.concatenate([block[0] for block in blocks] + [block[1] for block in blocks])
            )
    high, low = parts(jnp.concatenate(columns, axis=1))
    lines = high.shape[0] // 2
    copies = [through]
    for q in range(table_x.shape[1]):
        value = pair((high, low), (table_x[0, q], table_x[1, q]), 0)
        real = value[:lines, :128] + value[lines:, 128:]
        imag = value[lines:, :128] - value[:lines, 128:]
        out = pl.ds(q * 128, 128)
        held[0, :, :, out] = (real * scale).reshape(held.shape[1], held.shape[2], 128)
        held[1, :, :, out] = (imag * scale).reshape(held.shape[1], held.shape[2], 128)
        copy = pltpu.make_async_copy(
            held.at[:, :, :, out], source.at[:, :, :, out], sems.at[1 + q]
        )
        copy.start()
        copies.append(copy)
    for copy in copies:
        copy.wait()


def split_table(table):
    high = table.astype(jnp.bfloat16)
    return np.stack([high, (table - high.astype(np.float64)).astype(jnp.bfloat16)])


def transform_tables(length_x, length_z):
    counter = np.arange(length_z)
    angle = counter[:, None] * counter[None, :] % length_z * (2 * math.pi / length_z)
    table_z = np.concatenate([np.cos(angle), -np.sin(angle)])
    h, half, i, b = np.meshgrid(
        np.arange(length_x // 256), np.arange(2), np.arange(8), np.arange(16), indexing="ij"
    )
    place = (16 * (16 * h + b) + 8 * half + i).reshape(-1)
    mode = np.arange(length_x)
    angle = place[:, None] * mode[None, :] % length_x * (2 * math.pi / length_x)
    both = np.stack([np.cos(angle), np.sin(angle)], axis=1)
    both = both.reshape(length_x, 2, length_x // 128, 128).transpose(2, 0, 1, 3)
    return split_table(table_z), split_table(both.reshape(length_x // 128, length_x, 256))


def spectrum(force, field, tile, nx, nz):
    _, wide, tall, wall = tile
    length_x, length_z = wide * nx, tall * nz
    table_z, table_x = transform_tables(length_x, length_z)
    vector = pl.BlockSpec(memory_space=pltpu.VMEM)
    dma = pltpu.SemaphoreType.DMA
    each = wall // nz
    deep = field.shape[1]
    modes = length_z // nx
    velocity, rows = pl.pallas_call(
        functools.partial(spectrum_kernel, nx, nz),
        out_shape=(
            jax.ShapeDtypeStruct(tile, jnp.float32),
            jax.ShapeDtypeStruct((nx, 2, modes, wide * each), jnp.float32),
        ),
        in_specs=[vector] * 3,
        out_specs=(vector, vector),
        scratch_shapes=[
            pltpu.VMEM((2, 3, deep, SIDE, wall), jnp.float32),
            pltpu.VMEM((2, 3, HALF, tall, wall), jnp.float32),
            pltpu.VMEM((2, 3, HALF, tall, wall), jnp.float32),
            pltpu.VMEM((2, tall, wall), jnp.float32),
            pltpu.VMEM((2, tall, wall), jnp.float32),
            pltpu.VMEM((2, deep, wall), jnp.float32),
            pltpu.VMEM((2, deep, wall), jnp.float32),
            pltpu.VMEM((2, deep, wall), jnp.float32),
            pltpu.VMEM((2, 2, HALF, wall), jnp.float32),
            pltpu.VMEM((2, 2, HALF, wall), jnp.float32),
            pltpu.VMEM((2, tall, wall), jnp.float32),
            pltpu.VMEM((2, wide, wall), jnp.float32),
            pltpu.VMEM((nz, tall, wide * each), jnp.float32),
            pltpu.VMEM((nz, tall, wide * each), jnp.float32),
            pltpu.VMEM((2, nx, modes, wide * each), jnp.float32),
            dma((2, 3, 3)), dma((2, 3, 3)), dma((2, 3, 3)), dma((2, 3, 3)), dma((6,)), dma((6,)),
            dma((nz,)), dma((nz,)), dma((nx,)), dma((nx,)),
        ],
        compiler_params=pltpu.CompilerParams(
            collective_id=1, has_side_effects=True, vmem_limit_bytes=28 << 20
        ),
        name="spectrum",
    )(force, field, jnp.asarray(table_z))
    shape = (2, each, modes, length_x)
    return pl.pallas_call(
        functools.partial(finish_kernel, 1.0 / math.sqrt(length_x * length_z)),
        out_shape=(
            jax.ShapeDtypeStruct(tile, jnp.float32),
            jax.ShapeDtypeStruct(shape, jnp.float32),
        ),
        in_specs=[vector] * 3,
        out_specs=(pl.BlockSpec(memory_space=pltpu.HBM), pl.BlockSpec(memory_space=pltpu.HBM)),
        scratch_shapes=[
            pltpu.VMEM(shape, jnp.float32),
            dma((1 + length_x // 128,)),
        ],
        compiler_params=pltpu.CompilerParams(vmem_limit_bytes=16 << 20),
        name="finish",
    )(velocity, rows, jnp.asarray(table_x))


def on_device(
    nx, nz, flow_state, slot_ids, corners, marker_cells, marker_frac, particle_velocity,
    particle_spin,
):
    extended, cross, tap, cells, fracs = predict(flow_state, marker_cells, marker_frac, nx, nz)
    force = spread_forces(
        nx,
        nz,
        extended,
        cross,
        tap,
        slot_ids,
        corners,
        cells,
        fracs,
        particle_velocity,
        particle_spin,
    )
    return spectrum(force, extended, (3,) + flow_state.shape[1:], nx, nz)


def solution(mesh):
    both = ("gx", "gz")
    placed = (
        P(None, "gx", "gz", None),
        P(both),
        P(None, both),
        P(None, both, None),
        P(None, both, None),
        P(),
        P(),
    )
    return jax.shard_map(
        functools.partial(on_device, mesh.shape["gx"], mesh.shape["gz"]),
        mesh=mesh,
        in_specs=placed,
        out_specs=(P(None, "gx", "gz", None), P(None, "gz", "gx", None)),
        check_vma=False,
    )
```

```python
import functools
import math

import jax
import jax.numpy as jnp
import numpy as np
from jax import lax
from jax.experimental import pallas as pl
from jax.experimental.pallas import tpu as pltpu
from jax.sharding import PartitionSpec as P

BOX = 24
HALF = 12
BAND = 32
SIDE = 16
MESH = pl.DeviceIdType.MESH


time_step = 0.1
viscosity = 0.2
drive_force = 1.0


def remote(source, target, sems, slot, to):
    return pltpu.make_async_remote_copy(
        src_ref=source,
        dst_ref=target,
        send_sem=sems[0].at[slot],
        recv_sem=sems[1].at[slot],
        device_id=to,
        device_id_type=MESH,
    )


def around(nx, nz):
    gx, gz = lax.axis_index("gx"), lax.axis_index("gz")
    return (
        (lax.rem(gx + nx - 1, nx), gz),
        (lax.rem(gx + 1, nx), gz),
        (gx, lax.rem(gz + nz - 1, nz)),
        (gx, lax.rem(gz + 1, nz)),
    )


def parts(value):
    high = value.astype(jnp.bfloat16)
    return high, (value - high.astype(jnp.float32)).astype(jnp.bfloat16)


def tap_weights(length, first, taps):
    offset = lax.broadcasted_iota(jnp.int32, (length, first.shape[-1]), 0) - first
    weight = jnp.where(offset == 3, taps[3], 0.0)
    for t in (2, 1, 0):
        weight = jnp.where(offset == t, taps[t], weight)
    return weight


def fill_taps(fracs, tap):
    angle = fracs[...] * (0.5 * math.pi)
    cosine, sine = jnp.cos(angle), jnp.sin(angle)
    tap[0] = 0.25 * (1.0 - sine)
    tap[1] = 0.25 * (1.0 + cosine)
    tap[2] = 0.25 * (1.0 + sine)
    tap[3] = 0.25 * (1.0 - cosine)


def cross_weights(cells, fracs, tap, cross):
    fill_taps(fracs, tap)
    markers = fracs.shape[2]

    def one_slot(s, carry):
        cell = cells[:, pl.ds(s, 1), :].reshape(3, markers)
        taps = [tap[t, :, pl.ds(s, 1), :].reshape(3, markers) for t in range(4)]
        weight_x = tap_weights(BOX, cell[0:1] - 1, [w[0:1] for w in taps])
        weight_y = tap_weights(BAND, cell[1:2] - 1, [w[1:2] for w in taps])
        for i in range(BOX):
            high, low = parts(weight_x[i : i + 1] * weight_y)
            cross[s, 0, pl.ds(i * BAND, BAND), :] = high
            cross[s, 1, pl.ds(i * BAND, BAND), :] = low
        return carry

    lax.fori_loop(0, cells.shape[1], one_slot, 0)


def front_kernel(
    nx, nz, flow_in, cells_in, fracs_in, field, cross, tap, cells, fracs, flow, edge_x, edge_z_out, edge_z,
    f_sem, e_send, e_recv, x_send, x_recv, z_send, z_recv, r_send, r_recv,
):
    _, wide, tall, wall = flow.shape
    left, right, below, above = around(nx, nz)
    barrier = pltpu.get_barrier_semaphore()
    for near in (left, right, below, above):
        pl.semaphore_signal(barrier, inc=1, device_id=near, device_id_type=MESH)
    loads = [pltpu.make_async_copy(flow_in.at[c], flow.at[c], f_sem.at[c]) for c in range(4)]
    lists = [
        pltpu.make_async_copy(cells_in, cells, f_sem.at[4]),
        pltpu.make_async_copy(fracs_in, fracs, f_sem.at[5]),
    ]
    for load in loads + lists:
        load.start()
    pl.semaphore_wait(barrier, 4)
    for load in loads:
        load.wait()
    edge_z_out[0] = flow[:, :, 0, :]
    edge_z_out[1] = flow[:, :, tall - 1, :]
    edges = [
        remote(flow.at[:, 0], edge_x.at[1], (e_send, e_recv), 0, left),
        remote(flow.at[:, wide - 1], edge_x.at[0], (e_send, e_recv), 1, right),
        remote(edge_z_out.at[0], edge_z.at[1], (e_send, e_recv), 2, below),
        remote(edge_z_out.at[1], edge_z.at[0], (e_send, e_recv), 3, above),
    ]
    for copy in edges:
        copy.start()
    spread = time_step * viscosity
    carry_by = 0.5 * time_step
    lane = lax.broadcasted_iota(jnp.int32, (tall, wall), 1)
    row = lax.broadcasted_iota(jnp.int32, (tall, wall), 0)
    first_y, last_y = lane == 0, lane == wall - 1
    first_z, last_z = row == 0, row == tall - 1

    def layer(x, back, ahead):
        here = [flow[c, x] for c in range(4)]
        moves = [carry_by * here[d] for d in range(3)]
        for c in range(3):
            f = here[c]
            total = f * (1.0 - 6.0 * spread)
            y_plus = jnp.where(last_y, 0.0, pltpu.roll(f, wall - 1, 1))
            y_minus = jnp.where(first_y, 0.0, pltpu.roll(f, 1, 1))
            z_plus = jnp.where(last_z, 0.0, pltpu.roll(f, tall - 1, 0))
            z_minus = jnp.where(first_z, 0.0, pltpu.roll(f, 1, 0))
            for plus, minus, move in (
                (ahead[c], back[c], moves[0]),
                (y_plus, y_minus, moves[1]),
                (z_plus, z_minus, moves[2]),
            ):
                total += plus * (spread - move) + minus * (spread + move)
            p = here[3]
            if c == 0:
                total += time_step * drive_force - carry_by * (ahead[3] - back[3])
            if c == 1:
                p_plus = jnp.where(last_y, p, pltpu.roll(p, wall - 1, 1))
                p_minus = jnp.where(first_y, p, pltpu.roll(p, 1, 1))
                total -= carry_by * (p_plus - p_minus)
            if c == 2:
                p_plus = jnp.where(last_z, 0.0, pltpu.roll(p, tall - 1, 0))
                p_minus = jnp.where(first_z, 0.0, pltpu.roll(p, 1, 0))
                total -= carry_by * (p_plus - p_minus)
            field[c, HALF + x, pl.ds(SIDE, tall), :] = total

    def inside(x, carry):
        layer(x, [flow[c, x - 1] for c in range(4)], [flow[c, x + 1] for c in range(4)])
        return carry

    lax.fori_loop(1, wide - 1, inside, 0)
    rim = HALF - 1
    half = SIDE // 2
    spans = (
        {0: (1, rim), 1: (0, 1), 2: (0, HALF), 3: (0, HALF)},
        {0: (0, rim), 1: (rim, 1), 2: (0, HALF), 3: (0, HALF)},
    )
    lines = {0: (half, SIDE), 1: (half, SIDE), 2: (0, half), 3: (tall - half, half)}
    x_copies, z_copies = {}, []

    def send(c, piece):
        for side in range(2):
            first, count = spans[side][piece]
            at, height = lines[piece]
            source, target = ((HALF, HALF + wide), (wide, 0))[side]
            rows = pl.ds(SIDE + at, height)
            copy = remote(
                field.at[c, pl.ds(source + first, count), rows],
                field.at[c, pl.ds(target + first, count), rows],
                (x_send, x_recv), (side, c, piece), (left, right)[side],
            )
            copy.start()
            x_copies[c, piece, side] = copy

    def forward(c, piece, side):
        first, count = spans[side][piece]
        columns = pl.ds((HALF + wide, 0)[side] + first, count)
        at, height = lines[piece]
        slot = min(piece, 2)
        if piece != 3:
            count = min(at + height, HALF) - at
            copy = remote(
                field.at[c, columns, pl.ds(SIDE + at, count)],
                field.at[c, columns, pl.ds(SIDE + tall + at, count)],
                (r_send, r_recv), (0, c, side, slot), below,
            )
            copy.start()
            z_copies.append(copy)
        if piece != 2:
            start = max(at, tall - HALF)
            count = at + height - start
            copy = remote(
                field.at[c, columns, pl.ds(SIDE + start, count)],
                field.at[c, columns, pl.ds(SIDE + start - tall, count)],
                (r_send, r_recv), (1, c, side, slot), above,
            )
            copy.start()
            z_copies.append(copy)

    for c in range(3):
        send(c, 0)
    for copy in edges:
        copy.wait_recv()
    layer(0, [edge_x[0, c] for c in range(4)], [flow[c, 1] for c in range(4)])
    layer(
        wide - 1, [flow[c, wide - 2] for c in range(4)], [edge_x[1, c] for c in range(4)]
    )
    own = pl.ds(HALF, wide)
    for c in range(3):
        for side, z, sign in ((0, 0, 1.0), (1, tall - 1, -1.0)):
            move = carry_by * edge_z_out[side, 2]
            add = edge_z[side, c] * (spread + sign * move)
            if c == 2:
                add += sign * carry_by * edge_z[side, 3]
            field[c, own, SIDE + z, :] += add
        for piece in (2, 3, 1):
            send(c, piece)
    for c in range(3):
        down = remote(
            field.at[c, own, pl.ds(SIDE, HALF)],
            field.at[c, own, pl.ds(SIDE + tall, HALF)],
            (z_send, z_recv), (0, c), below,
        )
        up = remote(
            field.at[c, own, pl.ds(SIDE + tall - HALF, HALF)],
            field.at[c, own, pl.ds(SIDE - HALF, HALF)],
            (z_send, z_recv), (1, c), above,
        )
        down.start()
        up.start()
        z_copies.extend((down, up))
    blank = jnp.zeros(field.shape[:2] + (SIDE - HALF, wall), jnp.float32)
    field[:, :, pl.ds(0, SIDE - HALF), :] = blank
    field[:, :, pl.ds(SIDE + tall + HALF, SIDE - HALF), :] = blank
    for load in lists:
        load.wait()
    cross_weights(cells, fracs, tap, cross)
    for c, piece in [(c, 0) for c in range(3)] + [(c, p) for c in range(3) for p in (2, 3, 1)]:
        for side in range(2):
            x_copies[c, piece, side].wait_recv()
            forward(c, piece, side)
    for copy in z_copies:
        copy.wait_recv()
    for copy in edges + z_copies + list(x_copies.values()):
        copy.wait_send()


def predict(flow, cells, fracs, nx, nz):
    _, wide, tall, wall = flow.shape
    _, slots, markers = cells.shape
    vector = pl.BlockSpec(memory_space=pltpu.VMEM)
    dma = pltpu.SemaphoreType.DMA
    return pl.pallas_call(
        functools.partial(front_kernel, nx, nz),
        out_shape=(
            jax.ShapeDtypeStruct(
                (3, wide + 2 * HALF, tall + 2 * SIDE, wall), jnp.float32
            ),
            jax.ShapeDtypeStruct((slots, 2, BOX * BAND, markers), jnp.bfloat16),
            jax.ShapeDtypeStruct((4,) + cells.shape, jnp.float32),
            jax.ShapeDtypeStruct(cells.shape, jnp.int32),
            jax.ShapeDtypeStruct(cells.shape, jnp.float32),
        ),
        in_specs=[pl.BlockSpec(memory_space=pltpu.HBM)] * 3,
        out_specs=(vector,) * 5,
        scratch_shapes=[
            pltpu.VMEM(flow.shape, jnp.float32),
            pltpu.VMEM((2, 4, tall, wall), jnp.float32),
            pltpu.VMEM((2, 4, wide, wall), jnp.float32),
            pltpu.VMEM((2, 4, wide, wall), jnp.float32),
            dma((6,)), dma((4,)), dma((4,)), dma((2, 3, 4)), dma((2, 3, 4)), dma((2, 3)),
            dma((2, 3)), dma((2, 3, 2, 3)), dma((2, 3, 2, 3)),
        ],
        compiler_params=pltpu.CompilerParams(
            collective_id=0, has_side_effects=True, vmem_limit_bytes=12 << 20
        ),
        name="front",
    )(*(pltpu.with_memory_space_constraint(each, pltpu.HBM) for each in (flow, cells, fracs)))


def dot(a, b, across):
    return lax.dot_general(
        a, b, (((1,), (across,)), ((), ())), preferred_element_type=jnp.float32
    )


def pair(a, b, across):
    rows = a[0].shape[0]
    both = dot(jnp.concatenate(a), b[0], across)
    return both[:rows] + both[rows:] + dot(a[0], b[1], across)


def marker_kernel(
    nx, nz, ids, corners, moving, turning, cells, fracs, tap, field, cross, force
):
    force[...] = jnp.zeros_like(force)
    markers = fracs.shape[2]
    wall = field.shape[3]
    wide, tall = field.shape[1] - 2 * HALF, field.shape[2] - 2 * SIDE
    first_x = lax.axis_index("gx") * wide - HALF
    first_z = lax.axis_index("gz") * tall - SIDE
    many = wall // BAND
    lane = lax.broadcasted_iota(jnp.int32, (1, 1, wall), 2)

    def one_slot(s, carry):
        if True:
            n = lax.max(ids[s], 0)
            living = jnp.where(ids[s] >= 0, 1.0, 0.0)
            x0 = lax.rem(corners[0, s] - first_x + wide * nx, wide * nx)
            y0 = corners[1, s]
            z0 = lax.rem(corners[2, s] - first_z + tall * nz, tall * nz)
            zb = pl.multiple_of((z0 // 8) * 8, 8)
            cell = cells[:, pl.ds(s, 1), :].reshape(3, markers)
            frac = fracs[:, pl.ds(s, 1), :].reshape(3, markers)
            taps = [tap[t, :, pl.ds(s, 1), :].reshape(3, markers) for t in range(4)]

            weight_z = tap_weights(BAND, cell[2:3] - 1 + (z0 - zb), [w[2:3] for w in taps])
            columns = []
            for q in range(BOX // many):
                packed = None
                for r in range(many):
                    piece = field[:, x0 + (q * many + r), pl.ds(zb, BAND), :]
                    piece = pltpu.roll(piece, lax.rem(wall + r * BAND - y0, wall), 2)
                    packed = piece if r == 0 else jnp.where(lane < r * BAND, packed, piece)
                columns.append(packed.reshape(3 * BAND, wall))
            window = parts(jnp.concatenate(columns, axis=1))
            value = pair(window, (cross[s, 0], cross[s, 1]), 0).reshape(3, BAND, markers)
            sampled = jnp.sum(value * weight_z[None], axis=1)
            lever = cell.astype(jnp.float32) + frac - float(HALF)
            spin = [turning[c, n] for c in range(3)]
            loads = []
            for c in range(3):
                a, b = (c + 1) % 3, (c + 2) % 3
                target = moving[c, n] + (spin[a] * lever[b : b + 1] - spin[b] * lever[a : a + 1])
                loads.append((living * (target - sampled[c : c + 1])) * weight_z)
            load = parts(jnp.concatenate(loads))
            value = pair(load, (cross[s, 0], cross[s, 1]), 1).reshape(3, BAND, BOX * BAND)
            inside = (lane >= y0) & (lane < y0 + BOX)
            for i in range(BOX):
                q, r = i // many, i % many
                piece = value[:, :, q * wall : (q + 1) * wall]
                piece = pltpu.roll(piece, lax.rem(wall + y0 - r * BAND, wall), 2)
                force[:, x0 + i, pl.ds(zb, BAND), :] += jnp.where(inside, piece, 0.0)

        return carry

    def eight_slots(h, carry):
        for k in range(8):
            one_slot(8 * h + k, carry)
        return carry

    lax.fori_loop(0, ids.shape[0] // 8, eight_slots, 0)


def spread_forces(nx, nz, extended, cross, tap, slot_ids, corners, cells, fracs, moving, turning):
    scalar = pl.BlockSpec(memory_space=pltpu.SMEM)
    vector = pl.BlockSpec(memory_space=pltpu.VMEM)
    scalars = [
        pltpu.with_memory_space_constraint(each, pltpu.HBM)
        for each in (slot_ids, corners, moving, turning)
    ]
    return pl.pallas_call(
        functools.partial(marker_kernel, nx, nz),
        out_shape=jax.ShapeDtypeStruct(extended.shape, jnp.float32),
        in_specs=[scalar] * 4 + [vector] * 5,
        out_specs=vector,
        compiler_params=pltpu.CompilerParams(vmem_limit_bytes=16 << 20),
        name="markers",
    )(*scalars, cells, fracs, tap, extended, cross)


def exchanged(rows, lane_bits):
    lane = lax.broadcasted_iota(jnp.int32, rows[0].shape, rows[0].ndim - 1)
    axis = rows[0].ndim - 1
    for bit, shift in enumerate(lane_bits):
        low = (lane & shift) == 0
        step = 1 << bit
        out = list(rows)
        for m in range(len(rows)):
            if m & step == 0:
                a, b = rows[m], rows[m + step]
                out[m] = jnp.where(low, a, pltpu.roll(b, shift, axis))
                out[m + step] = jnp.where(low, pltpu.roll(a, 128 - shift, axis), b)
        rows = out
    return rows


def spectrum_kernel(
    nx, nz, force, field, table_z, velocity, rows,
    z_got, x_out, x_got, u_out, u_got, row_out, row_got, row_sum, rim_out, rim_got, edge_u,
    edge_w, cut, planes, modes,
    z_send, z_recv, x_send, x_recv, e_send, e_recv, c_send, c_recv, m_send, m_recv,
):
    gx, gz = lax.axis_index("gx"), lax.axis_index("gz")
    left, right, below, above = around(nx, nz)
    barrier = pltpu.get_barrier_semaphore()

    def greet_z(d, carry):
        pl.semaphore_signal(
            barrier, inc=1, device_id=(gx, lax.rem(gz + d, nz)), device_id_type=MESH
        )
        return carry

    def greet_x(d, carry):
        pl.semaphore_signal(
            barrier, inc=1, device_id=(lax.rem(gx + d, nx), gz), device_id_type=MESH
        )
        return carry

    lax.fori_loop(1, nx, greet_x, 0)
    lax.fori_loop(1, nz, greet_z, 0)
    wide, tall = velocity.shape[1], velocity.shape[2]
    blank = jnp.zeros(z_got.shape[1:3] + (SIDE - HALF, z_got.shape[4]), jnp.float32)
    z_got[0, :, :, pl.ds(HALF, SIDE - HALF), :] = blank
    z_got[1, :, :, pl.ds(0, SIDE - HALF), :] = blank
    row_out[0] = force[2, :, SIDE, :]
    row_out[1] = force[2, :, SIDE + tall - 1, :]
    pl.semaphore_wait(barrier, nx + nz - 2)

    order = (0, 2, 1)
    own = pl.ds(HALF, wide)
    pieces = (pl.ds(0, HALF), pl.ds(HALF + wide, HALF), own)

    def fold_z(c, piece):
        columns = pieces[piece]
        down = remote(
            force.at[c, columns, pl.ds(SIDE - HALF, HALF), :],
            z_got.at[1, c, columns, pl.ds(SIDE - HALF, HALF), :],
            (z_send, z_recv), (1, c, piece), below,
        )
        up = remote(
            force.at[c, columns, pl.ds(SIDE + tall, HALF), :],
            z_got.at[0, c, columns, pl.ds(0, HALF), :],
            (z_send, z_recv), (0, c, piece), above,
        )
        down.start()
        up.start()
        return [down, up]

    rims, inner = {}, {}
    rims[0] = fold_z(0, 0) + fold_z(0, 1)
    lines = [
        remote(row_out.at[0], row_got.at[1], (e_send, e_recv), 0, below),
        remote(row_out.at[1], row_got.at[0], (e_send, e_recv), 1, above),
    ]
    x_copies = {}

    def fold_x(c, source, columns, piece, start, count):
        lines_at = pl.ds(start, count)
        for side in range(2):
            copy = remote(
                source(side, c, columns[side], start, count),
                x_got.at[1 - side, c, :, lines_at, :],
                (x_send, x_recv), (1 - side, c, piece), (left, right)[side],
            )
            copy.start()
            x_copies.setdefault(c, []).append(copy)

    def from_force(side, c, columns, start, count):
        return force.at[c, columns, pl.ds(SIDE + start, count), :]

    def from_sums(side, c, columns, start, count):
        return x_out.at[side, c, :, pl.ds(start, count), :]

    for c in order:
        fold_x(c, from_force, pieces, 0, HALF, tall - 2 * HALF)
    for c in order:
        for copy in rims[c]:
            copy.wait_recv()
        if c == 0:
            rims[2] = fold_z(2, 0) + fold_z(2, 1)
            for copy in lines:
                copy.start()
            inner[0] = fold_z(0, 2)
        if c == 2:
            rims[1] = fold_z(1, 0) + fold_z(1, 1)
            inner[2] = fold_z(2, 2)
            inner[1] = fold_z(1, 2)
        for part in range(2):
            inside = pl.ds(part * SIDE, SIDE)
            outside = pl.ds(SIDE + part * SIDE, SIDE)
            for side in range(2):
                x_out[side, c, :, inside, :] = (
                    force[c, pieces[side], outside, :] + z_got[part, c, pieces[side]]
                )
        fold_x(c, from_sums, pieces, 1, 0, HALF)
        fold_x(c, from_sums, pieces, 2, tall - HALF, HALF)
        if c == 2:
            for copy in lines:
                copy.wait_recv()
            row_sum[0] = force[2, :, SIDE - 1, :] + row_got[0]
            row_sum[1] = force[2, :, SIDE + tall, :] + row_got[1]
            rim_out[0] = row_sum[:, pl.ds(0, HALF), :]
            rim_out[1] = row_sum[:, pl.ds(HALF + wide, HALF), :]
            ends = [
                remote(rim_out.at[0], rim_got.at[1], (e_send, e_recv), 2, left),
                remote(rim_out.at[1], rim_got.at[0], (e_send, e_recv), 3, right),
            ]
            for copy in ends:
                copy.start()
        if c == 0:
            for copy in inner[0]:
                copy.wait_recv()
            for part in range(2):
                inside = pl.ds(part * SIDE, SIDE)
                outside = pl.ds(SIDE + part * SIDE, SIDE)
                u_out[0, inside, :] = force[0, HALF, outside, :] + z_got[part, 0, HALF]
                u_out[1, inside, :] = (
                    force[0, HALF + wide - 1, outside, :] + z_got[part, 0, HALF + wide - 1]
                )
            layers = [
                remote(u_out.at[0], u_got.at[1], (e_send, e_recv), 4, left),
                remote(u_out.at[1], u_got.at[0], (e_send, e_recv), 5, right),
            ]
            for copy in layers:
                copy.start()
    for c in order:
        if c != 0:
            for copy in inner[c]:
                copy.wait_recv()
        for part in range(2):
            inside = pl.ds(part * SIDE, SIDE)
            outside = pl.ds(SIDE + part * SIDE, SIDE)
            velocity[c, :, inside, :] = (
                field[c, own, outside, :] + force[c, own, outside, :] + z_got[part, c, own]
            )
    for c in order:
        if c == 1:
            stream, span = velocity[0], velocity[2]
            divergence = jnp.concatenate([stream[1:], edge_u[1:2]], axis=0) - jnp.concatenate(
                [edge_u[0:1], stream[:-1]], axis=0
            )
            row = lax.broadcasted_iota(jnp.int32, (1, tall, 1), 1)
            after = jnp.where(
                row == tall - 1, edge_w[1][:, None, :], pltpu.roll(span, tall - 1, 1)
            )
            before = jnp.where(row == 0, edge_w[0][:, None, :], pltpu.roll(span, 1, 1))
            divergence += after - before
        for copy in x_copies[c]:
            copy.wait_recv()
        velocity[c, pl.ds(0, HALF)] += x_got[0, c]
        velocity[c, pl.ds(wide - HALF, HALF)] += x_got[1, c]
        if c == 0:
            for copy in layers:
                copy.wait_recv()
            body = pl.ds(SIDE, tall)
            edge_u[0] = field[0, HALF - 1, body, :] + x_out[0, 0, HALF - 1] + u_got[0]
            edge_u[1] = field[0, HALF + wide, body, :] + x_out[1, 0, 0] + u_got[1]
        if c == 2:
            for copy in ends:
                copy.wait_recv()
            edge_w[0] = field[2, own, SIDE - 1, :] + row_sum[0, own, :]
            edge_w[1] = field[2, own, SIDE + tall, :] + row_sum[1, own, :]
            edge_w[:, pl.ds(0, HALF), :] += rim_got[0]
            edge_w[:, pl.ds(wide - HALF, HALF), :] += rim_got[1]
    edges = lines + ends + layers
    wall = velocity.shape[3]
    lane = lax.broadcasted_iota(jnp.int32, (1, 1, wall), 2)
    normal = velocity[1]
    upper = jnp.where(lane == wall - 1, 0.0, pltpu.roll(normal, wall - 1, 2))
    lower = jnp.where(lane == 0, 0.0, pltpu.roll(normal, 1, 2))
    divergence = (divergence + (upper - lower)) * 0.5
    for half in range(wide // 8):
        blocks = exchanged([divergence[half * 8 + i] for i in range(8)], (16, 32, 64))
        for j in range(nz):
            cut[j, :, pl.ds(half * 128, 128)] = blocks[j]

    def cut_copy(d):
        to = lax.rem(gz + d, nz)
        return pltpu.make_async_remote_copy(
            src_ref=cut.at[to],
            dst_ref=planes.at[gz],
            send_sem=c_send.at[to],
            recv_sem=c_recv.at[gz],
            device_id=(gx, to),
            device_id_type=MESH,
        )

    def cut_from(d):
        origin = lax.rem(gz + d, nz)
        return pltpu.make_async_remote_copy(
            src_ref=cut.at[origin],
            dst_ref=planes.at[origin],
            send_sem=c_send.at[origin],
            recv_sem=c_recv.at[origin],
            device_id=(gx, origin),
            device_id_type=MESH,
        )

    def start(make):
        def go(d, carry):
            make(d).start()
            return carry

        return go

    def wait_recv(make):
        def go(d, carry):
            make(d).wait_recv()
            return carry

        return go

    def wait_send(make):
        def go(d, carry):
            make(d).wait_send()
            return carry

        return go

    lax.fori_loop(1, nz, start(cut_copy), 0)
    planes[gz] = cut[gz]
    lax.fori_loop(1, nz, wait_recv(cut_from), 0)
    high, low = parts(planes[...].reshape(nz * tall, 2 * 128))
    modes[...] = pair((table_z[0], table_z[1]), (high, low), 0).reshape(modes.shape)

    deep = nx // 8
    deep_at, along_at = lax.div(gx, 8), lax.rem(gx, 8)

    def partner(t):
        k, j = lax.div(t, deep), lax.rem(t, deep)
        odd = lax.rem(k, 2)
        step = 4 - odd + lax.div(k, 2) * (1 - 2 * odd)
        return lax.rem(deep_at + j + 1, deep) * 8 + lax.rem(along_at + step, 8)

    def mode_copy(t):
        to = partner(t)
        return pltpu.make_async_remote_copy(
            src_ref=modes.at[:, to],
            dst_ref=rows.at[gx],
            send_sem=m_send.at[to],
            recv_sem=m_recv.at[gx],
            device_id=(to, gz),
            device_id_type=MESH,
        )

    def mode_from(t):
        origin = partner(t)
        return pltpu.make_async_remote_copy(
            src_ref=modes.at[:, origin],
            dst_ref=rows.at[origin],
            send_sem=m_send.at[origin],
            recv_sem=m_recv.at[origin],
            device_id=(origin, gz),
            device_id_type=MESH,
        )

    lax.fori_loop(0, nx - 1, start(mode_copy), 0)
    rows[gx] = modes[:, gx]
    lax.fori_loop(0, nx - 1, wait_recv(mode_from), 0)
    for c in order:
        for copy in rims[c] + inner[c] + x_copies[c]:
            copy.wait_send()
    for copy in edges:
        copy.wait_send()
    lax.fori_loop(1, nz, wait_send(cut_copy), 0)
    lax.fori_loop(0, nx - 1, wait_send(mode_copy), 0)


def finish_kernel(scale, velocity_in, rows, table_x, velocity, source, held, sems):
    through = pltpu.make_async_copy(velocity_in, velocity, sems.at[0])
    through.start()
    columns = []
    for h in range(rows.shape[0] // 16):
        for half in range(2):
            blocks = exchanged(
                [rows[h * 16 + b, :, :, half * 128 : half * 128 + 128] for b in range(16)],
                (1, 2, 4, 8),
            )
            columns.append(
                jnp.concatenate([block[0] for block in blocks] + [block[1] for block in blocks])
            )
    high, low = parts(jnp.concatenate(columns, axis=1))
    lines = high.shape[0] // 2
    copies = [through]
    for q in range(table_x.shape[1]):
        value = pair((high, low), (table_x[0, q], table_x[1, q]), 0)
        real = value[:lines, :128] + value[lines:, 128:]
        imag = value[lines:, :128] - value[:lines, 128:]
        out = pl.ds(q * 128, 128)
        held[0, :, :, out] = (real * scale).reshape(held.shape[1], held.shape[2], 128)
        held[1, :, :, out] = (imag * scale).reshape(held.shape[1], held.shape[2], 128)
        copy = pltpu.make_async_copy(
            held.at[:, :, :, out], source.at[:, :, :, out], sems.at[1 + q]
        )
        copy.start()
        copies.append(copy)
    for copy in copies:
        copy.wait()


def split_table(table):
    high = table.astype(jnp.bfloat16)
    return np.stack([high, (table - high.astype(np.float64)).astype(jnp.bfloat16)])


def transform_tables(length_x, length_z):
    counter = np.arange(length_z)
    angle = counter[:, None] * counter[None, :] % length_z * (2 * math.pi / length_z)
    table_z = np.concatenate([np.cos(angle), -np.sin(angle)])
    h, half, i, b = np.meshgrid(
        np.arange(length_x // 256), np.arange(2), np.arange(8), np.arange(16), indexing="ij"
    )
    place = (16 * (16 * h + b) + 8 * half + i).reshape(-1)
    mode = np.arange(length_x)
    angle = place[:, None] * mode[None, :] % length_x * (2 * math.pi / length_x)
    both = np.stack([np.cos(angle), np.sin(angle)], axis=1)
    both = both.reshape(length_x, 2, length_x // 128, 128).transpose(2, 0, 1, 3)
    return split_table(table_z), split_table(both.reshape(length_x // 128, length_x, 256))


def spectrum(force, field, tile, nx, nz):
    _, wide, tall, wall = tile
    length_x, length_z = wide * nx, tall * nz
    table_z, table_x = transform_tables(length_x, length_z)
    vector = pl.BlockSpec(memory_space=pltpu.VMEM)
    dma = pltpu.SemaphoreType.DMA
    each = wall // nz
    deep = field.shape[1]
    modes = length_z // nx
    velocity, rows = pl.pallas_call(
        functools.partial(spectrum_kernel, nx, nz),
        out_shape=(
            jax.ShapeDtypeStruct(tile, jnp.float32),
            jax.ShapeDtypeStruct((nx, 2, modes, wide * each), jnp.float32),
        ),
        in_specs=[vector] * 3,
        out_specs=(vector, vector),
        scratch_shapes=[
            pltpu.VMEM((2, 3, deep, SIDE, wall), jnp.float32),
            pltpu.VMEM((2, 3, HALF, tall, wall), jnp.float32),
            pltpu.VMEM((2, 3, HALF, tall, wall), jnp.float32),
            pltpu.VMEM((2, tall, wall), jnp.float32),
            pltpu.VMEM((2, tall, wall), jnp.float32),
            pltpu.VMEM((2, deep, wall), jnp.float32),
            pltpu.VMEM((2, deep, wall), jnp.float32),
            pltpu.VMEM((2, deep, wall), jnp.float32),
            pltpu.VMEM((2, 2, HALF, wall), jnp.float32),
            pltpu.VMEM((2, 2, HALF, wall), jnp.float32),
            pltpu.VMEM((2, tall, wall), jnp.float32),
            pltpu.VMEM((2, wide, wall), jnp.float32),
            pltpu.VMEM((nz, tall, wide * each), jnp.float32),
            pltpu.VMEM((nz, tall, wide * each), jnp.float32),
            pltpu.VMEM((2, nx, modes, wide * each), jnp.float32),
            dma((2, 3, 3)), dma((2, 3, 3)), dma((2, 3, 3)), dma((2, 3, 3)), dma((6,)), dma((6,)),
            dma((nz,)), dma((nz,)), dma((nx,)), dma((nx,)),
        ],
        compiler_params=pltpu.CompilerParams(
            collective_id=1, has_side_effects=True, vmem_limit_bytes=28 << 20
        ),
        name="spectrum",
    )(force, field, jnp.asarray(table_z))
    shape = (2, each, modes, length_x)
    return pl.pallas_call(
        functools.partial(finish_kernel, 1.0 / math.sqrt(length_x * length_z)),
        out_shape=(
            jax.ShapeDtypeStruct(tile, jnp.float32),
            jax.ShapeDtypeStruct(shape, jnp.float32),
        ),
        in_specs=[vector] * 3,
        out_specs=(pl.BlockSpec(memory_space=pltpu.HBM), pl.BlockSpec(memory_space=pltpu.HBM)),
        scratch_shapes=[
            pltpu.VMEM(shape, jnp.float32),
            dma((1 + length_x // 128,)),
        ],
        compiler_params=pltpu.CompilerParams(vmem_limit_bytes=16 << 20),
        name="finish",
    )(velocity, rows, jnp.asarray(table_x))


def on_device(
    nx, nz, flow_state, slot_ids, corners, marker_cells, marker_frac, particle_velocity,
    particle_spin,
):
    extended, cross, tap, cells, fracs = predict(flow_state, marker_cells, marker_frac, nx, nz)
    force = spread_forces(
        nx,
        nz,
        extended,
        cross,
        tap,
        slot_ids,
        corners,
        cells,
        fracs,
        particle_velocity,
        particle_spin,
    )
    return spectrum(force, extended, (3,) + flow_state.shape[1:], nx, nz)


def solution(mesh):
    both = ("gx", "gz")
    placed = (
        P(None, "gx", "gz", None),
        P(both),
        P(None, both),
        P(None, both, None),
        P(None, both, None),
        P(),
        P(),
    )
    return jax.shard_map(
        functools.partial(on_device, mesh.shape["gx"], mesh.shape["gz"]),
        mesh=mesh,
        in_specs=placed,
        out_specs=(P(None, "gx", "gz", None), P(None, "gz", "gx", None)),
        check_vma=False,
    )
```
